8 devices in a mesh: data: 8 (over z, y, x, core).
Axes of the slice: x: 2, y: 2, z: 1, core: 2. Of those that a mesh axis runs over, the one named last changes fastest.
Arguments:
- act_in: bfloat16 [32768, 768], P('data')
- grad_out: bfloat16 [32768, 768], P('data')
- w_up: bfloat16 [2, 768, 3072], replicated
- w_down: bfloat16 [2, 3072, 768], replicated
- master_up: float32 [2, 768, 3072], P(None, 'data')
- master_down: float32 [2, 3072, 768], P(None, 'data')
- exp_avg_up: float32 [2, 768, 3072], P(None, 'data')
- exp_avg_down: float32 [2, 3072, 768], P(None, 'data')
- exp_sq_up: float32 [2, 768, 3072], P(None, 'data')
- exp_sq_down: float32 [2, 3072, 768], P(None, 'data')
- learn_rate: float32 [], replicated
- clip_norm: float32 [], replicated
Outputs:
- output 1: bfloat16 [2, 768, 3072], replicated
- output 2: bfloat16 [2, 3072, 768], replicated
- output 3: float32 [2, 768, 3072], P(None, 'data')
- output 4: float32 [2, 3072, 768], P(None, 'data')
- output 5: float32 [2, 768, 3072], P(None, 'data')
- output 6: float32 [2, 3072, 768], P(None, 'data')
- output 7: float32 [2, 768, 3072], P(None, 'data')
- output 8: float32 [2, 3072, 768], P(None, 'data')
- output 9: float32 [], replicated
All inputs are finite; a program needn't handle non-finite values.
Results may differ from the reference program's by a relative error of at most 0.00406.
Values are sent between devices in bfloat16 or wider.
A program may use at most 1 GiB of HBM per device.

```python
import jax
import jax.numpy as jnp
from jax import lax

D = 768
FF = 3072
TOKENS_DEV = 4096
GROUP = 8
STEP = 10

BETA_ONE = 0.9
BETA_TWO = 0.95
ADAM_EPS = 1e-8
NORM_EPS = 1e-6
INV_SQRT_TWO = 0.7071067811865476
INV_SQRT_TWO_PI = 0.3989422804014327


def gelu_parts(pre_act):
    normal_cdf = 0.5 * (1.0 + lax.erf(pre_act * INV_SQRT_TWO))
    normal_pdf = jnp.exp(-0.5 * pre_act * pre_act) * INV_SQRT_TWO_PI
    return pre_act * normal_cdf, normal_cdf + pre_act * normal_pdf


def block_grads(act_blk, out_blk, w_up, w_down):
    z_one = jnp.dot(act_blk, w_up[0], preferred_element_type=jnp.float32)
    gelu_one, slope_one = gelu_parts(z_one)
    act_one = gelu_one.astype(jnp.bfloat16)
    hidden = jnp.dot(act_one, w_down[0], preferred_element_type=jnp.float32).astype(jnp.bfloat16)
    z_three = jnp.dot(hidden, w_up[1], preferred_element_type=jnp.float32)
    gelu_three, slope_three = gelu_parts(z_three)
    act_three = gelu_three.astype(jnp.bfloat16)
    g_four = jnp.dot(act_three.T, out_blk, preferred_element_type=jnp.float32)
    dz_three = (jnp.dot(out_blk, w_down[1].T, preferred_element_type=jnp.float32) * slope_three).astype(jnp.bfloat16)
    g_three = jnp.dot(hidden.T, dz_three, preferred_element_type=jnp.float32)
    d_hidden = jnp.dot(dz_three, w_up[1].T, preferred_element_type=jnp.float32).astype(jnp.bfloat16)
    g_two = jnp.dot(act_one.T, d_hidden, preferred_element_type=jnp.float32)
    dz_one = (jnp.dot(d_hidden, w_down[0].T, preferred_element_type=jnp.float32) * slope_one).astype(jnp.bfloat16)
    g_one = jnp.dot(act_blk.T, dz_one, preferred_element_type=jnp.float32)
    return jnp.stack([g_one, g_three]), jnp.stack([g_two, g_four])


def full_grads(act_in, grad_out, w_up, w_down):
    act_blocks = act_in.reshape(GROUP, TOKENS_DEV, D)
    out_blocks = grad_out.reshape(GROUP, TOKENS_DEV, D)

    def add_block(carry_sums, blocks):
        grad_up, grad_down = block_grads(blocks[0], blocks[1], w_up, w_down)
        return (carry_sums[0] + grad_up, carry_sums[1] + grad_down), None

    start_sums = (jnp.zeros((2, D, FF), jnp.float32), jnp.zeros((2, FF, D), jnp.float32))
    final_sums = lax.scan(add_block, start_sums, (act_blocks, out_blocks))[0]
    return final_sums[0] / GROUP, final_sums[1] / GROUP


def lamb_update(master, exp_avg, exp_sq, grad, clip_scale, learn_rate):
    bias_one = 1.0 - BETA_ONE ** STEP
    bias_two = 1.0 - BETA_TWO ** STEP
    avg_new = BETA_ONE * exp_avg + (1.0 - BETA_ONE) * clip_scale * grad
    sq_new = BETA_TWO * exp_sq + (1.0 - BETA_TWO) * (clip_scale * clip_scale) * (grad * grad)
    direction = (avg_new / bias_one) / (jnp.sqrt(sq_new / bias_two) + ADAM_EPS)
    master_norm = jnp.sqrt(jnp.sum(master * master, axis=(1, 2), keepdims=True))
    dir_norm = jnp.sqrt(jnp.sum(direction * direction, axis=(1, 2), keepdims=True))
    master_new = master - learn_rate * (master_norm / dir_norm) * direction
    return master_new, avg_new, sq_new


def row_profile(key, row_count, spread):
    walk = jnp.cumsum(jax.random.normal(key, (row_count,), jnp.float32)) / (row_count ** 0.5)
    return jnp.exp(spread * (walk - jnp.mean(walk)))


def setup_inputs(seed: int = 0) -> dict:
    keys = jax.random.split(jax.random.key(seed), 24)
    row_total = TOKENS_DEV * GROUP
    init_scale = D ** -0.5
    out_scale = (GROUP / TOKENS_DEV) ** 0.5
    act_in = jax.random.normal(keys[0], (row_total, D), jnp.float32).astype(jnp.bfloat16)
    grad_out = (jax.random.normal(keys[1], (row_total, D), jnp.float32) * out_scale).astype(jnp.bfloat16)
    prof_up = jnp.stack([row_profile(keys[2], D, 0.7), row_profile(keys[3], D, 0.7)])[:, :, None]
    prof_down = jnp.stack([row_profile(keys[4], FF, 0.7), row_profile(keys[5], FF, 0.7)])[:, :, None]
    base_up = jax.random.normal(keys[6], (2, D, FF), jnp.float32) * init_scale * prof_up
    base_down = jax.random.normal(keys[7], (2, FF, D), jnp.float32) * init_scale * prof_down
    w_up = base_up.astype(jnp.bfloat16)
    w_down = base_down.astype(jnp.bfloat16)
    master_up = base_up + 0.02 * init_scale * prof_up * jax.random.normal(keys[8], (2, D, FF), jnp.float32)
    master_down = base_down + 0.02 * init_scale * prof_down * jax.random.normal(keys[9], (2, FF, D), jnp.float32)
    grad_up, grad_down = full_grads(act_in, grad_out, w_up, w_down)
    grad_norm = jnp.sqrt(jnp.sum(grad_up * grad_up) + jnp.sum(grad_down * grad_down))
    clip_norm = jax.random.uniform(keys[10], (), jnp.float32, 0.3, 0.7) * grad_norm
    clip_scale = clip_norm / (grad_norm + NORM_EPS)
    step_up = clip_scale * jnp.sqrt(jnp.mean(grad_up * grad_up, axis=(1, 2), keepdims=True))
    step_down = clip_scale * jnp.sqrt(jnp.mean(grad_down * grad_down, axis=(1, 2), keepdims=True))
    exp_avg_up = 0.1 * step_up * jax.random.normal(keys[11], (2, D, FF), jnp.float32)
    exp_avg_down = 0.1 * step_down * jax.random.normal(keys[12], (2, FF, D), jnp.float32)
    sq_prof_up = jnp.stack([row_profile(keys[13], D, 1.5), row_profile(keys[14], D, 1.5)])[:, :, None]
    sq_prof_down = jnp.stack([row_profile(keys[15], FF, 1.5), row_profile(keys[16], FF, 1.5)])[:, :, None]
    exp_sq_up = 0.05 * step_up * step_up * sq_prof_up * jax.random.uniform(keys[17], (2, D, FF), jnp.float32, 0.5, 1.5)
    exp_sq_down = 0.05 * step_down * step_down * sq_prof_down * jax.random.uniform(keys[18], (2, FF, D), jnp.float32, 0.5, 1.5)
    learn_rate = jax.random.uniform(keys[19], (), jnp.float32, 0.08, 0.16)
    return {"act_in": act_in, "grad_out": grad_out, "w_up": w_up, "w_down": w_down, "master_up": master_up, "master_down": master_down, "exp_avg_up": exp_avg_up, "exp_avg_down": exp_avg_down, "exp_sq_up": exp_sq_up, "exp_sq_down": exp_sq_down, "learn_rate": learn_rate, "clip_norm": clip_norm}


def reference(act_in, grad_out, w_up, w_down, master_up, master_down, exp_avg_up, exp_avg_down, exp_sq_up, exp_sq_down, learn_rate, clip_norm):
    grad_up, grad_down = full_grads(act_in, grad_out, w_up, w_down)
    grad_norm = jnp.sqrt(jnp.sum(grad_up * grad_up) + jnp.sum(grad_down * grad_down))
    clip_scale = jnp.minimum(1.0, clip_norm / (grad_norm + NORM_EPS))
    master_up_out, avg_up, sq_up = lamb_update(master_up, exp_avg_up, exp_sq_up, grad_up, clip_scale, learn_rate)
    master_down_out, avg_down, sq_down = lamb_update(master_down, exp_avg_down, exp_sq_down, grad_down, clip_scale, learn_rate)
    return (master_up_out.astype(jnp.bfloat16), master_down_out.astype(jnp.bfloat16), master_up_out, master_down_out, avg_up, avg_down, sq_up, sq_down, grad_norm)
```

```python
import functools

import jax
import jax.numpy as jnp
from jax import lax
from jax.experimental import pallas as pl
from jax.experimental.pallas import tpu as pltpu
from jax.sharding import PartitionSpec as P

STEP = 10
BETA_ONE = 0.9
BETA_TWO = 0.95
ADAM_EPS = 1e-8
NORM_EPS = 1e-6
INV_SQRT_TWO = 0.7071067811865476
INV_SQRT_TWO_PI = 0.3989422804014327


def gelu_parts(pre_act):
    normal_cdf = 0.5 * (1.0 + lax.erf(pre_act * INV_SQRT_TWO))
    normal_pdf = jnp.exp(-0.5 * pre_act * pre_act) * INV_SQRT_TWO_PI
    return pre_act * normal_cdf, normal_cdf + pre_act * normal_pdf


def local_grads(act_in, grad_out, w_up, w_down):
    z_one = jnp.einsum("td,df->tf", act_in, w_up[0], preferred_element_type=jnp.float32)
    gelu_one, slope_one = gelu_parts(z_one)
    act_one = gelu_one.astype(jnp.bfloat16)
    hidden = jnp.einsum("tf,fd->td", act_one, w_down[0], preferred_element_type=jnp.float32).astype(jnp.bfloat16)
    z_three = jnp.einsum("td,df->tf", hidden, w_up[1], preferred_element_type=jnp.float32)
    gelu_three, slope_three = gelu_parts(z_three)
    act_three = gelu_three.astype(jnp.bfloat16)
    g_four = jnp.einsum("tf,td->fd", act_three, grad_out, preferred_element_type=jnp.float32)
    dz_three = (jnp.einsum("td,fd->tf", grad_out, w_down[1], preferred_element_type=jnp.float32) * slope_three).astype(jnp.bfloat16)
    g_three = jnp.einsum("td,tf->df", hidden, dz_three, preferred_element_type=jnp.float32)
    d_hidden = jnp.einsum("tf,df->td", dz_three, w_up[1], preferred_element_type=jnp.float32).astype(jnp.bfloat16)
    g_two = jnp.einsum("tf,td->fd", act_one, d_hidden, preferred_element_type=jnp.float32)
    dz_one = (jnp.einsum("td,fd->tf", d_hidden, w_down[0], preferred_element_type=jnp.float32) * slope_one).astype(jnp.bfloat16)
    g_one = jnp.einsum("td,tf->df", act_in, dz_one, preferred_element_type=jnp.float32)
    return g_one, g_two, g_three, g_four


MESH = pl.DeviceIdType.MESH
VMEM_LIMIT = 66 * 1024 * 1024 - 2 * 1024 * 1024


def coords():
    me = lax.axis_index("data")
    core, col, row = me % 2, (me // 2) % 2, me // 4
    return me, me + 1 - 2 * core, me + 2 - 4 * col, me + 4 - 8 * row


def remote(src, dst, send_sem, recv_sem, device):
    return pltpu.make_async_remote_copy(src_ref=src, dst_ref=dst, send_sem=send_sem, recv_sem=recv_sem, device_id=(device,), device_id_type=MESH)


def meet_all(me, group_size):
    barrier = pltpu.get_barrier_semaphore()
    for step in range(1, group_size):
        pl.semaphore_signal(barrier, inc=1, device_id=((me + step) % group_size,), device_id_type=MESH)
    pl.semaphore_wait(barrier, group_size - 1)


def exchange_start(me, group_size, slots, send_sem, recv_sem):
    copies = []
    for step in range(1, group_size):
        copies.append(remote(slots.at[me], slots.at[me], send_sem.at[step], recv_sem.at[step], (me + step) % group_size))
        copies[-1].start()
    return copies


def stat_sum_kernel(group_size, tile_ref, out_ref, slots, send_sem, recv_sem):
    me = lax.axis_index("data")
    slots[me] = tile_ref[...]
    meet_all(me, group_size)
    for copy in exchange_start(me, group_size, slots, send_sem, recv_sem):
        copy.wait()
    total = slots[0]
    for index in range(1, group_size):
        total = total + slots[index]
    out_ref[...] = total


def stat_sum(tile, group_size):
    return pl.pallas_call(
        functools.partial(stat_sum_kernel, group_size),
        out_shape=jax.ShapeDtypeStruct((8, 128), jnp.float32),
        in_specs=[pl.BlockSpec(memory_space=pltpu.VMEM)],
        out_specs=pl.BlockSpec(memory_space=pltpu.VMEM),
        scratch_shapes=[pltpu.VMEM((group_size, 8, 128), jnp.float32), pltpu.SemaphoreType.DMA((group_size,)), pltpu.SemaphoreType.DMA((group_size,))],
        compiler_params=pltpu.CompilerParams(collective_id=0, has_side_effects=True),
        name="stat_sum",
    )(tile)


def moments_kernel(clip_ref, g_up, g_down, m_up, m_down, v_up, v_down, m_up_out, m_down_out, v_up_out, v_down_out, u_up, u_down, stats):
    bias_one = 1.0 - BETA_ONE ** STEP
    bias_two = 1.0 - BETA_TWO ** STEP
    scale = clip_ref[0]
    row_id = lax.broadcasted_iota(jnp.int32, (8, 128), 0)
    sums = jnp.zeros((8, 128), jnp.float32)
    for family, (g, m, v, m_out, v_out, u) in enumerate([(g_up, m_up, v_up, m_up_out, v_up_out, u_up), (g_down, m_down, v_down, m_down_out, v_down_out, u_down)]):
        for layer in range(2):
            grad = g[layer]
            avg_new = BETA_ONE * m[layer] + (1.0 - BETA_ONE) * scale * grad
            sq_new = BETA_TWO * v[layer] + (1.0 - BETA_TWO) * (scale * scale) * (grad * grad)
            direction = (avg_new / bias_one) / (jnp.sqrt(sq_new / bias_two) + ADAM_EPS)
            m_out[layer] = avg_new
            v_out[layer] = sq_new
            u[layer] = direction
            sums = sums + jnp.where(row_id == 4 + 2 * family + layer, jnp.sum(direction * direction), 0.0)

    @pl.when(pl.program_id(0) == 0)
    def _():
        stats[...] = jnp.zeros_like(stats)

    stats[...] += sums


def moments(clip_scale, g_up, g_down, m_up, m_down, v_up, v_down, steps=4):
    up, down = g_up.shape, g_down.shape
    up_spec = pl.BlockSpec((2, up[1] // steps, up[2]), lambda i: (0, i, 0))
    down_spec = pl.BlockSpec((2, down[1] // steps, down[2]), lambda i: (0, i, 0))
    pair = [up_spec, down_spec]
    up_shape, down_shape = jax.ShapeDtypeStruct(up, jnp.float32), jax.ShapeDtypeStruct(down, jnp.float32)
    return pl.pallas_call(
        moments_kernel,
        grid=(steps,),
        out_shape=[up_shape, down_shape] * 3 + [jax.ShapeDtypeStruct((8, 128), jnp.float32)],
        in_specs=[pl.BlockSpec(memory_space=pltpu.SMEM)] + pair * 3,
        out_specs=pair * 3 + [pl.BlockSpec((8, 128), lambda i: (0, 0))],
        compiler_params=pltpu.CompilerParams(dimension_semantics=("arbitrary",), vmem_limit_bytes=40 * 1024 * 1024),
        name="moments",
    )(clip_scale.reshape(1), g_up, g_down, m_up, m_down, v_up, v_down)


PIECES = ((0, 0), (0, 1), (1, 0), (1, 1))


def update_kernel(group_size, rate_ref, stats_ref, u_up, u_down, p_up, p_down, all_up, all_down, p_up_out, p_down_out,
                  slots, w_up, w_down, stat_send, stat_recv, send_sem, recv_sem, local_sem):
    me, partner, near_x, near_y = coords()
    slots[me] = stats_ref[...]
    meet_all(me, group_size)
    for copy in exchange_start(me, group_size, slots, stat_send, stat_recv):
        copy.wait()
    total = slots[0]
    for index in range(1, group_size):
        total = total + slots[index]
    ratio = jnp.sqrt(total[0:4]) / jnp.sqrt(total[4:8])
    rate = rate_ref[0]
    params = ((u_up, p_up, p_up_out, w_up, all_up), (u_down, p_down, p_down_out, w_down, all_down))

    def place(piece, owner):
        family, layer = PIECES[piece]
        full = params[family][4]
        rows = params[family][3].shape[1]
        return full.at[layer, pl.ds(pl.multiple_of(owner * rows, rows), rows), :]

    sends = []
    count = [0]

    def forward(src, piece, owner, device, rel):
        copy = remote(src, place(piece, owner), send_sem.at[count[0]], recv_sem.at[rel, piece], device)
        count[0] += 1
        copy.start()
        sends.append(copy)

    def arrival(piece, rel, owner):
        spot = place(piece, owner)
        remote(spot, spot, send_sem.at[0], recv_sem.at[rel, piece], me).wait_recv()
        return spot

    own = {}
    local = []
    for piece in (0, 2, 1, 3):
        family, layer = PIECES[piece]
        u, p, p_out, w, full = params[family]
        index = 2 * family + layer
        new = p[layer] - rate * ratio[index:index + 1, 0:1] * u[layer]
        p_out[layer] = new
        w[layer] = new.astype(jnp.bfloat16)
        own[piece] = w.at[layer]
        if family == 0:
            forward(own[piece], piece, me, near_x, 2)
        else:
            forward(own[piece], piece, me, near_y, 4)
        forward(own[piece], piece, me, partner, 1)
        copy = pltpu.make_async_copy(own[piece], place(piece, me), local_sem.at[piece])
        copy.start()
        local.append(copy)
    for piece in (2, 3):
        forward(own[piece], piece, me, near_x, 2)
    for piece in (0, 1):
        forward(own[piece], piece, me, near_y, 4)
    diag = near_x + near_y - me
    for k in range(2):
        spot = arrival(k, 2, near_x)
        forward(spot, k, near_x, near_y, 6)
        forward(spot, k, near_x, partner, 3)
        spot = arrival(2 + k, 4, near_y)
        forward(spot, 2 + k, near_y, near_x, 6)
        forward(spot, 2 + k, near_y, partner, 5)
    for k in range(2):
        spot = arrival(2 + k, 2, near_x)
        forward(spot, 2 + k, near_x, partner, 3)
        spot = arrival(k, 4, near_y)
        forward(spot, k, near_y, partner, 5)
    for k in range(2):
        for piece in (2 + k, k):
            spot = arrival(piece, 6, diag)
            forward(spot, piece, diag, partner, 7)
    for rel, owner in ((1, partner), (3, near_x + partner - me), (5, near_y + partner - me), (7, diag + partner - me)):
        for piece in range(4):
            arrival(piece, rel, owner)
    for copy in sends:
        copy.wait_send()
    for copy in local:
        copy.wait()


def update_and_gather(group_size, learn_rate, stats, u_up, u_down, p_up, p_down):
    up, down = p_up.shape, p_down.shape
    vmem = pl.BlockSpec(memory_space=pltpu.VMEM)
    hbm = pl.BlockSpec(memory_space=pl.ANY)
    return pl.pallas_call(
        functools.partial(update_kernel, group_size),
        out_shape=[
            jax.ShapeDtypeStruct((up[0], up[1] * group_size, up[2]), jnp.bfloat16),
            jax.ShapeDtypeStruct((down[0], down[1] * group_size, down[2]), jnp.bfloat16),
            jax.ShapeDtypeStruct(up, jnp.float32),
            jax.ShapeDtypeStruct(down, jnp.float32),
        ],
        in_specs=[pl.BlockSpec(memory_space=pltpu.SMEM)] + [vmem] * 5,
        out_specs=[hbm, hbm, vmem, vmem],
        scratch_shapes=[
            pltpu.VMEM((group_size, 8, 128), jnp.float32),
            pltpu.VMEM(up, jnp.bfloat16),
            pltpu.VMEM(down, jnp.bfloat16),
            pltpu.SemaphoreType.DMA((group_size,)),
            pltpu.SemaphoreType.DMA((group_size,)),
            pltpu.SemaphoreType.DMA((32,)),
            pltpu.SemaphoreType.DMA((group_size, 4)),
            pltpu.SemaphoreType.DMA((4,)),
        ],
        compiler_params=pltpu.CompilerParams(collective_id=1, has_side_effects=True, vmem_limit_bytes=40 * 1024 * 1024),
        name="update_and_gather",
    )(learn_rate.reshape(1), stats, u_up, u_down, p_up, p_down)


def sum_squares(stacked):
    return jnp.sum(stacked * stacked, axis=(1, 2))


def solution(mesh):
    group_size = mesh.shape["data"]
    batch_rows = P("data", None)
    state_rows = P(None, "data", None)
    replicated = P()

    def reduce_rows(grad):
        return lax.psum_scatter(grad, "data", scatter_dimension=0, tiled=True) / group_size

    def device_step(act_in, grad_out, w_up, w_down, master_up, master_down, exp_avg_up, exp_avg_down, exp_sq_up, exp_sq_down, learn_rate, clip_norm):
        g_one, g_two, g_three, g_four = local_grads(act_in, grad_out, w_up, w_down)
        shard_four = reduce_rows(g_four)
        shard_three = reduce_rows(g_three)
        shard_two = reduce_rows(g_two)
        shard_one = reduce_rows(g_one)
        grad_up = jnp.stack([shard_one, shard_three])
        grad_down = jnp.stack([shard_two, shard_four])
        local_sq = jnp.sum(grad_up * grad_up) + jnp.sum(grad_down * grad_down)
        grad_norm = jnp.sqrt(stat_sum(jnp.full((8, 128), local_sq), group_size)[0, 0])
        clip_scale = jnp.minimum(1.0, clip_norm / (grad_norm + NORM_EPS))
        master_sq = jnp.concatenate([sum_squares(master_up), sum_squares(master_down)])
        avg_up, avg_down, sq_up, sq_down, dir_up, dir_down, dir_stats = moments(clip_scale, grad_up, grad_down, exp_avg_up, exp_avg_down, exp_sq_up, exp_sq_down)
        stats = dir_stats + jnp.pad(master_sq, (0, 4))[:, None]
        new_w_up, new_w_down, master_up_out, master_down_out = update_and_gather(group_size, learn_rate, stats, dir_up, dir_down, master_up, master_down)
        return (new_w_up, new_w_down, master_up_out, master_down_out, avg_up, avg_down, sq_up, sq_down, grad_norm)

    return jax.shard_map(device_step, mesh=mesh, in_specs=(batch_rows, batch_rows, replicated, replicated, state_rows, state_rows, state_rows, state_rows, state_rows, state_rows, replicated, replicated), out_specs=(replicated, replicated, state_rows, state_rows, state_rows, state_rows, state_rows, state_rows, replicated), check_vma=False)
```

```python
import functools

import jax
import jax.numpy as jnp
from jax import lax
from jax.experimental import pallas as pl
from jax.experimental.pallas import tpu as pltpu
from jax.sharding import PartitionSpec as P

STEP = 10
BETA_ONE = 0.9
BETA_TWO = 0.95
ADAM_EPS = 1e-8
NORM_EPS = 1e-6
INV_SQRT_TWO = 0.7071067811865476
INV_SQRT_TWO_PI = 0.3989422804014327


def gelu_parts(pre_act):
    normal_cdf = 0.5 * (1.0 + lax.erf(pre_act * INV_SQRT_TWO))
    normal_pdf = jnp.exp(-0.5 * pre_act * pre_act) * INV_SQRT_TWO_PI
    return pre_act * normal_cdf, normal_cdf + pre_act * normal_pdf


MESH = pl.DeviceIdType.MESH


def coords():
    me = lax.axis_index("data")
    core, col, row = me % 2, (me // 2) % 2, me // 4
    return me, me + 1 - 2 * core, me + 2 - 4 * col, me + 4 - 8 * row


def remote(src, dst, send_sem, recv_sem, device):
    return pltpu.make_async_remote_copy(src_ref=src, dst_ref=dst, send_sem=send_sem, recv_sem=recv_sem, device_id=(device,), device_id_type=MESH)


def meet_all(me, group_size):
    barrier = pltpu.get_barrier_semaphore()
    for step in range(1, group_size):
        pl.semaphore_signal(barrier, inc=1, device_id=((me + step) % group_size,), device_id_type=MESH)
    pl.semaphore_wait(barrier, group_size - 1)


def exchange_start(me, group_size, slots, send_sem, recv_sem):
    copies = []
    for step in range(1, group_size):
        copies.append(remote(slots.at[me], slots.at[me], send_sem.at[step], recv_sem.at[step], (me + step) % group_size))
        copies[-1].start()
    return copies


def stat_sum_kernel(group_size, tile_ref, out_ref, slots, send_sem, recv_sem):
    me = lax.axis_index("data")
    slots[me] = tile_ref[...]
    meet_all(me, group_size)
    for copy in exchange_start(me, group_size, slots, send_sem, recv_sem):
        copy.wait()
    total = slots[0]
    for index in range(1, group_size):
        total = total + slots[index]
    out_ref[...] = total


def stat_sum(tile, group_size):
    return pl.pallas_call(
        functools.partial(stat_sum_kernel, group_size),
        out_shape=jax.ShapeDtypeStruct((8, 128), jnp.float32),
        in_specs=[pl.BlockSpec(memory_space=pltpu.VMEM)],
        out_specs=pl.BlockSpec(memory_space=pltpu.VMEM),
        scratch_shapes=[pltpu.VMEM((group_size, 8, 128), jnp.float32), pltpu.SemaphoreType.DMA((group_size,)), pltpu.SemaphoreType.DMA((group_size,))],
        compiler_params=pltpu.CompilerParams(collective_id=0, has_side_effects=True),
        name="stat_sum",
    )(tile)


CHUNKS = 3
LANES = 128
TILE = 256
OWNERS = tuple(chip * 2 + core for core in range(2) for chip in range(4))
FULL_VMEM = 67043328


def dot_nn(lhs, rhs):
    return jnp.dot(lhs, rhs, preferred_element_type=jnp.float32)


def dot_nt(lhs, rhs):
    return lax.dot_general(lhs, rhs, (((1,), (1,)), ((), ())), preferred_element_type=jnp.float32)


def dot_tn(lhs, rhs):
    return lax.dot_general(lhs, rhs, (((0,), (0,)), ((), ())), preferred_element_type=jnp.float32)


def chunk_blocks(chunk, width):
    return [owner * width + chunk * LANES for owner in OWNERS]


def forward_kernel(x_ref, w_up_ref, w_down_ref, a_out, s_out, h_out):
    x = x_ref[...]
    width = w_up_ref.shape[2] // len(OWNERS)
    total = None
    for chunk in range(CHUNKS):
        starts = chunk_blocks(chunk, width)
        w_in = jnp.concatenate([w_up_ref[0, :, s:s + LANES] for s in starts], axis=1)
        gelu, slope = gelu_parts(dot_nn(x, w_in))
        act = gelu.astype(jnp.bfloat16)
        a_out[chunk] = act
        s_out[chunk] = slope
        w_out = jnp.concatenate([w_down_ref[0, s:s + LANES, :] for s in starts], axis=0)
        part = dot_nn(act, w_out)
        total = part if total is None else total + part
    h_out[...] = total.astype(jnp.bfloat16)


def forward_block(act_in, w_up, w_down, tile=512):
    rows, dim = act_in.shape
    ff = w_up.shape[2]
    wide = ff // CHUNKS
    return pl.pallas_call(
        forward_kernel,
        grid=(rows // tile,),
        out_shape=[
            jax.ShapeDtypeStruct((CHUNKS, rows, wide), jnp.bfloat16),
            jax.ShapeDtypeStruct((CHUNKS, rows, wide), jnp.float32),
            jax.ShapeDtypeStruct((rows, dim), jnp.bfloat16),
        ],
        in_specs=[
            pl.BlockSpec((tile, dim), lambda i: (i, 0)),
            pl.BlockSpec((1, dim, ff), lambda i: (0, 0, 0)),
            pl.BlockSpec((1, ff, dim), lambda i: (0, 0, 0)),
        ],
        out_specs=[
            pl.BlockSpec((CHUNKS, tile, wide), lambda i: (0, i, 0)),
            pl.BlockSpec((CHUNKS, tile, wide), lambda i: (0, i, 0)),
            pl.BlockSpec((tile, dim), lambda i: (i, 0)),
        ],
        compiler_params=pltpu.CompilerParams(dimension_semantics=("arbitrary",), vmem_limit_bytes=FULL_VMEM),
        name="forward_block",
    )(act_in, w_up, w_down)


def backward_kernel(group_size, x_hbm, e_hbm, h_hbm, a_hbm, s_hbm, w_up_hbm, w_down_hbm,
                    g1_out, g2_out, g3_out, g4_out, q_hbm,
                    h_v, e_v, wu_v, wd_v, a_v, q_v, s_v, t_d, t_u,
                    d0, d1a, d1b, d2a, d2b, u0, u1a, u1b, u2a, u2b,
                    load_sem, w_sem, q_sem, s_sem, send_sem, recv_sem, free_sem):
    me, partner, near_x, near_y = coords()
    core, col, row = me % 2, (me // 2) % 2, me // 4
    rows, dim = h_v.shape
    half_rows = rows // 2
    wide = wu_v.shape[2]
    width = wide * CHUNKS // len(OWNERS)
    tiles = half_rows // TILE
    slots = s_v.shape[0]

    def at_rows(start, size):
        return pl.ds(pl.multiple_of(start, size), size)

    def half_copy(src, dst, half, sem):
        span = pl.ds(half * half_rows, half_rows)
        return pltpu.make_async_copy(src.at[span], dst.at[span], load_sem.at[sem, half])

    def start_weight(which, chunk, layer):
        for j, start in enumerate(chunk_blocks(chunk, width)):
            if which == 0:
                pltpu.make_async_copy(w_up_hbm.at[layer, :, pl.ds(start, LANES)], wu_v.at[chunk, :, pl.ds(j * LANES, LANES)], w_sem.at[0, chunk]).start()
            else:
                pltpu.make_async_copy(w_down_hbm.at[layer, pl.ds(start, LANES), :], wd_v.at[chunk, pl.ds(j * LANES, LANES), :], w_sem.at[1, chunk]).start()

    def wait_weight(which, chunk):
        ref = (wu_v, wd_v)[which]
        pltpu.make_async_copy(ref.at[chunk], ref.at[chunk], w_sem.at[which, chunk]).wait()

    for half in range(2):
        half_copy(h_hbm, h_v, half, 0).start()
        half_copy(e_hbm, e_v, half, 1).start()
        if half == 0:
            start_weight(0, 0, 1)
            start_weight(1, 0, 1)
    for chunk in range(1, CHUNKS):
        start_weight(0, chunk, 1)
        start_weight(1, chunk, 1)
    meet_all(me, group_size)

    def hop(src, dst, kind, chunk, stage, device):
        return remote(src, dst, send_sem.at[kind, chunk, stage], recv_sem.at[kind, chunk, stage], device)

    def hop0(kind, i):
        if kind == 0:
            return hop(t_d.at[1 - core], d0.at[i], 0, i, 0, partner)
        return hop(t_u.at[:, :, 1 - core], u0.at[i], 1, i, 0, partner)

    def bufs(kind):
        return (d0, d1a, d1b, d2a, d2b) if kind == 0 else (u0, u1a, u1b, u2a, u2b)

    def hop1(kind, i):
        b0, b1a, b1b, _, _ = bufs(kind)
        cut = b1a.shape[3]
        return (hop(b0.at[i, :, 1 - col, :, pl.ds(0, cut)], b1a.at[i], kind, i, 1, near_x),
                hop(b0.at[i, 1 - row, :, :, pl.ds(cut, cut)], b1b.at[i], kind, i, 2, near_y))

    def hop2(kind, i):
        _, b1a, b1b, b2a, b2b = bufs(kind)
        return (hop(b1a.at[i, 1 - row], b2a.at[i], kind, i, 3, near_y),
                hop(b1b.at[i, 1 - col], b2b.at[i], kind, i, 4, near_x))

    def rs0(kind, i):
        hop0(kind, i).start()

    def rs1(kind, i):
        hop0(kind, i).wait()
        b0 = bufs(kind)[0]
        for y in range(2):
            for x in range(2):
                own = t_d[core, y, x] if kind == 0 else t_u[y, x, core]
                b0[i, y, x] = b0[i, y, x] + own
        for copy in hop1(kind, i):
            copy.start()

    def rs2(kind, i):
        b0, b1a, b1b, _, _ = bufs(kind)
        cut = b1a.shape[3]
        first, second = hop1(kind, i)
        out_a, out_b = hop2(kind, i)
        first.wait()
        for y in range(2):
            b1a[i, y] = b1a[i, y] + b0[i, y, col, :, 0:cut]
        out_a.start()
        second.wait()
        for x in range(2):
            b1b[i, x] = b1b[i, x] + b0[i, row, x, :, cut:2 * cut]
        out_b.start()

    def rs3(kind, i, out):
        _, b1a, b1b, b2a, b2b = bufs(kind)
        cut = b1a.shape[3]
        for copy in hop2(kind, i):
            copy.wait()
        left = (b1a[i, row] + b2a[i]) / group_size
        right = (b1b[i, col] + b2b[i]) / group_size
        if kind == 0:
            span = at_rows(i * LANES, LANES)
            out[span, 0:cut] = left
            out[span, cut:2 * cut] = right
        else:
            for j, owner in enumerate(OWNERS):
                part = (left, right)[j // 4]
                lane = (j % 4) * LANES
                out[:, pl.ds(pl.multiple_of(owner * width + i * LANES, LANES), LANES)] = part[:, lane:lane + LANES]

    def give_free(i):
        for device in (partner, near_x, near_y):
            pl.semaphore_signal(free_sem.at[i], inc=1, device_id=(device,), device_id_type=MESH)

    def grad_down(lhs_ref, rhs_ref, half, before_store=None):
        def part(m, carry):
            acc = dot_tn(lhs_ref[:, at_rows(m * (wide // 2), wide // 2)], rhs_ref[at_rows(half * half_rows, half_rows), :])
            if before_store is not None:
                before_store(m)
            acc = acc.reshape(t_d.shape[1:])
            t_d[m] = acc + jnp.where(half == 0, 0.0, t_d[m])
            return carry
        lax.fori_loop(0, 2, part, 0)

    def grad_up(lhs_ref, rhs_ref, half):
        def part(m, carry):
            acc = dot_tn(lhs_ref[at_rows(half * half_rows, half_rows), at_rows(m * (dim // 2), dim // 2)], rhs_ref[...])
            acc = acc.reshape(t_u.shape[1:])
            t_u[m] = acc + jnp.where(half == 0, 0.0, t_u[m])
            return carry
        lax.fori_loop(0, 2, part, 0)

    def q_copy(i, half):
        return pltpu.make_async_copy(q_v, q_hbm.at[i, at_rows(half * half_rows, half_rows), :], q_sem.at[0])

    def second_chunk(i, carry):
        wait_weight(0, i)
        wait_weight(1, i)

        def second_half(half, carry):
            @pl.when(i == 0)
            def _():
                span = at_rows(half * half_rows, half_rows)
                pltpu.make_async_copy(h_hbm.at[span], h_v.at[span], load_sem.at[0, half]).wait()
                pltpu.make_async_copy(e_hbm.at[span], e_v.at[span], load_sem.at[1, half]).wait()

            @pl.when((i > 0) | (half > 0))
            def _():
                q_copy(i, half).wait()

            def second_tile(t, carry):
                span = at_rows(half * half_rows + t * TILE, TILE)
                z = dot_nn(h_v[span, :], wu_v[i])
                p = dot_nt(e_v[span, :], wd_v[i])
                gelu, slope = gelu_parts(z)
                here = at_rows(t * TILE, TILE)
                a_v[here, :] = gelu.astype(jnp.bfloat16)
                q_v[here, :] = (p * slope).astype(jnp.bfloat16)

                @pl.when((t == tiles // 2) & (half == 0) & (i > 0))
                def _():
                    @pl.when(i > 1)
                    def _():
                        rs3(0, i - 2, g4_out)
                        rs3(1, i - 2, g3_out)
                        give_free(i - 2)
                    rs1(0, i - 1)
                    rs1(1, i - 1)
                return carry

            lax.fori_loop(0, tiles, second_tile, 0)
            q_copy(i, half).start()

            @pl.when((half == 1) & (i > 0))
            def _():
                rs2(0, i - 1)
                rs2(1, i - 1)

            grad_down(a_v, e_v, half)

            @pl.when(half == 1)
            def _():
                rs0(0, i)

            grad_up(h_v, q_v, half)

            @pl.when(half == 1)
            def _():
                rs0(1, i)
            return carry

        lax.fori_loop(0, 2, second_half, 0)
        return carry

    lax.fori_loop(0, CHUNKS, second_chunk, 0)

    q_copy(CHUNKS - 1, 1).wait()
    for half in range(2):
        half_copy(x_hbm, e_v, half, 1).start()
    for chunk in range(CHUNKS):
        start_weight(1, chunk, 0)
    r_rows = half_rows // 4
    staging = (a_v, q_v)

    def r_load(slot, t):
        for k in range(CHUNKS):
            pltpu.make_async_copy(q_hbm.at[k, at_rows(t * r_rows, r_rows), :], staging[slot].at[pl.ds(k * r_rows, r_rows), :], load_sem.at[2, slot]).start()

    def a_load(i, half):
        return pltpu.make_async_copy(a_hbm.at[i, pl.ds(half * half_rows, half_rows), :], staging[half], load_sem.at[0, half])

    for slot in range(2):
        r_load(slot, slot)
    r_steps = rows // r_rows // 2

    def r_pair(t, carry):
        for slot in range(2):
            whole = staging[slot].at[pl.ds(0, CHUNKS * r_rows), :]
            pltpu.make_async_copy(whole, whole, load_sem.at[2, slot]).wait()
            acc = dot_nt(staging[slot][0:r_rows, :], wu_v[0])
            for k in range(1, CHUNKS):
                acc = acc + dot_nt(staging[slot][k * r_rows:(k + 1) * r_rows, :], wu_v[k])
            h_v[at_rows((2 * t + slot) * r_rows, r_rows), :] = acc.astype(jnp.bfloat16)

            @pl.when(t < r_steps - 1)
            def _():
                r_load(slot, 2 * t + 2 + slot)

        @pl.when(t == 0)
        def _():
            rs3(0, CHUNKS - 2, g4_out)
            rs3(1, CHUNKS - 2, g3_out)
            give_free(CHUNKS - 2)
            rs1(0, CHUNKS - 1)
            rs1(1, CHUNKS - 1)
        return carry

    lax.fori_loop(0, r_steps, r_pair, 0)
    for half in range(2):
        a_load(0, half).start()

    def s_load(i, t):
        slot = lax.rem(t, slots)
        return pltpu.make_async_copy(s_hbm.at[i, at_rows(t * TILE, TILE), :], s_v.at[slot], s_sem.at[slot])

    for t in range(slots):
        s_load(0, t).start()
    rs2(0, CHUNKS - 1)
    rs2(1, CHUNKS - 1)

    def first_down(i, carry):
        for half in range(2):
            a_load(i, half).wait()

            def settle(m):
                @pl.when((m == 0) & (i > 0))
                def _():
                    rs1(0, i - 1)

            grad_down(staging[half], h_v, half, settle if half == 0 else None)

            @pl.when(i < CHUNKS - 1)
            def _():
                a_load(i + 1, half).start()

            if half == 0:
                @pl.when(i == 2)
                def _():
                    rs2(0, 0)

        @pl.when(i == 1)
        def _():
            rs3(0, CHUNKS - 1, g4_out)
            rs3(1, CHUNKS - 1, g3_out)
            give_free(CHUNKS - 1)

        pl.semaphore_wait(free_sem.at[i], 3)
        rs0(0, i)
        return carry

    lax.fori_loop(0, CHUNKS, first_down, 0)
    for half in range(2):
        half_copy(x_hbm, e_v, half, 1).wait()

    def first_up(i, carry):
        wait_weight(1, i)

        def first_half(half, carry):
            def first_tile(t, carry):
                tt = half * tiles + t
                s_load(i, tt).wait()
                p = dot_nt(h_v[at_rows(tt * TILE, TILE), :], wd_v[i])
                q_v[at_rows(t * TILE, TILE), :] = (p * s_v[lax.rem(tt, slots)]).astype(jnp.bfloat16)

                ahead = tt + slots
                @pl.when(ahead < 2 * tiles)
                def _():
                    s_load(i, ahead).start()

                @pl.when((t == tiles // 2) & (half == 0))
                def _():
                    @pl.when(i == 0)
                    def _():
                        rs1(0, 2)
                        rs2(0, 1)
                        rs3(0, 0, g2_out)

                    @pl.when(i == 1)
                    def _():
                        rs1(1, 0)
                        rs2(0, 2)
                        rs3(0, 1, g2_out)

                    @pl.when(i == 2)
                    def _():
                        rs1(1, 1)
                        rs2(1, 0)
                        rs3(0, 2, g2_out)
                return carry

            lax.fori_loop(0, tiles, first_tile, 0)

            @pl.when((half == 1) & (i < CHUNKS - 1))
            def _():
                for t in range(slots):
                    s_load(i + 1, t).start()

            grad_up(e_v, q_v, half)
            return carry

        lax.fori_loop(0, 2, first_half, 0)
        rs0(1, i)
        return carry

    lax.fori_loop(0, CHUNKS, first_up, 0)
    rs2(1, 1)
    rs1(1, 2)
    rs3(1, 0, g1_out)
    rs3(1, 1, g1_out)
    rs2(1, 2)
    rs3(1, 2, g1_out)


def backward_blocks(group_size, act_in, grad_out, hidden, act_one, slope_one, w_up, w_down):
    rows, dim = act_in.shape
    ff = w_up.shape[2]
    wide = ff // CHUNKS
    up_rows, down_rows = dim // group_size, LANES
    hbm = pl.BlockSpec(memory_space=pl.ANY)
    vmem = pl.BlockSpec(memory_space=pltpu.VMEM)
    f32 = jnp.float32
    bf16 = jnp.bfloat16
    up_grad = jax.ShapeDtypeStruct((up_rows, ff), f32)
    down_grad = jax.ShapeDtypeStruct((ff // group_size, dim), f32)

    def stages(height, cols):
        return [
            pltpu.VMEM((CHUNKS, 2, 2, height, cols), f32),
            pltpu.VMEM((CHUNKS, 2, height, cols // 2), f32),
            pltpu.VMEM((CHUNKS, 2, height, cols // 2), f32),
            pltpu.VMEM((CHUNKS, height, cols // 2), f32),
            pltpu.VMEM((CHUNKS, height, cols // 2), f32),
        ]

    return pl.pallas_call(
        functools.partial(backward_kernel, group_size),
        out_shape=[up_grad, down_grad, up_grad, down_grad, jax.ShapeDtypeStruct((CHUNKS, rows, wide), bf16)],
        in_specs=[hbm] * 7,
        out_specs=[vmem] * 4 + [hbm],
        scratch_shapes=[
            pltpu.VMEM((rows, dim), bf16),
            pltpu.VMEM((rows, dim), bf16),
            pltpu.VMEM((CHUNKS, dim, wide), bf16),
            pltpu.VMEM((CHUNKS, wide, dim), bf16),
            pltpu.VMEM((rows // 2, wide), bf16),
            pltpu.VMEM((rows // 2, wide), bf16),
            pltpu.VMEM((2, TILE, wide), f32),
            pltpu.VMEM((2, 2, 2, down_rows, dim), f32),
            pltpu.VMEM((2, 2, 2, up_rows, wide), f32),
            *stages(down_rows, dim),
            *stages(up_rows, wide),
            pltpu.SemaphoreType.DMA((3, 2)),
            pltpu.SemaphoreType.DMA((2, CHUNKS)),
            pltpu.SemaphoreType.DMA((1,)),
            pltpu.SemaphoreType.DMA((2,)),
            pltpu.SemaphoreType.DMA((2, CHUNKS, 5)),
            pltpu.SemaphoreType.DMA((2, CHUNKS, 5)),
            pltpu.SemaphoreType.REGULAR((CHUNKS,)),
        ],
        compiler_params=pltpu.CompilerParams(collective_id=2, has_side_effects=True, vmem_limit_bytes=FULL_VMEM),
        name="backward_blocks",
    )(act_in, grad_out, hidden, act_one, slope_one, w_up, w_down)[:4]


def moments_kernel(clip_ref, g_up, g_down, m_up, m_down, v_up, v_down, m_up_out, m_down_out, v_up_out, v_down_out, u_up, u_down, stats):
    bias_one = 1.0 - BETA_ONE ** STEP
    bias_two = 1.0 - BETA_TWO ** STEP
    scale = clip_ref[0]
    row_id = lax.broadcasted_iota(jnp.int32, (8, 128), 0)
    sums = jnp.zeros((8, 128), jnp.float32)
    for family, (g, m, v, m_out, v_out, u) in enumerate([(g_up, m_up, v_up, m_up_out, v_up_out, u_up), (g_down, m_down, v_down, m_down_out, v_down_out, u_down)]):
        for layer in range(2):
            grad = g[layer]
            avg_new = BETA_ONE * m[layer] + (1.0 - BETA_ONE) * scale * grad
            sq_new = BETA_TWO * v[layer] + (1.0 - BETA_TWO) * (scale * scale) * (grad * grad)
            direction = (avg_new / bias_one) / (jnp.sqrt(sq_new / bias_two) + ADAM_EPS)
            m_out[layer] = avg_new
            v_out[layer] = sq_new
            u[layer] = direction
            sums = sums + jnp.where(row_id == 4 + 2 * family + layer, jnp.sum(direction * direction), 0.0)

    @pl.when(pl.program_id(0) == 0)
    def _():
        stats[...] = jnp.zeros_like(stats)

    stats[...] += sums


def moments(clip_scale, g_up, g_down, m_up, m_down, v_up, v_down, steps=4):
    up, down = g_up.shape, g_down.shape
    up_spec = pl.BlockSpec((2, up[1] // steps, up[2]), lambda i: (0, i, 0))
    down_spec = pl.BlockSpec((2, down[1] // steps, down[2]), lambda i: (0, i, 0))
    pair = [up_spec, down_spec]
    up_shape, down_shape = jax.ShapeDtypeStruct(up, jnp.float32), jax.ShapeDtypeStruct(down, jnp.float32)
    return pl.pallas_call(
        moments_kernel,
        grid=(steps,),
        out_shape=[up_shape, down_shape] * 3 + [jax.ShapeDtypeStruct((8, 128), jnp.float32)],
        in_specs=[pl.BlockSpec(memory_space=pltpu.SMEM)] + pair * 3,
        out_specs=pair * 3 + [pl.BlockSpec((8, 128), lambda i: (0, 0))],
        compiler_params=pltpu.CompilerParams(dimension_semantics=("arbitrary",), vmem_limit_bytes=40 * 1024 * 1024),
        name="moments",
    )(clip_scale.reshape(1), g_up, g_down, m_up, m_down, v_up, v_down)


PIECES = ((0, 0), (0, 1), (1, 0), (1, 1))


def update_kernel(group_size, rate_ref, stats_ref, u_up, u_down, p_up, p_down, all_up, all_down, p_up_out, p_down_out,
                  slots, w_up, w_down, stat_send, stat_recv, send_sem, recv_sem, local_sem):
    me, partner, near_x, near_y = coords()
    slots[me] = stats_ref[...]
    meet_all(me, group_size)
    for copy in exchange_start(me, group_size, slots, stat_send, stat_recv):
        copy.wait()
    total = slots[0]
    for index in range(1, group_size):
        total = total + slots[index]
    ratio = jnp.sqrt(total[0:4]) / jnp.sqrt(total[4:8])
    rate = rate_ref[0]
    params = ((u_up, p_up, p_up_out, w_up, all_up), (u_down, p_down, p_down_out, w_down, all_down))

    def place(piece, owner):
        family, layer = PIECES[piece]
        full = params[family][4]
        rows = params[family][3].shape[1]
        return full.at[layer, pl.ds(pl.multiple_of(owner * rows, rows), rows), :]

    sends = []
    count = [0]

    def forward(src, piece, owner, device, rel):
        copy = remote(src, place(piece, owner), send_sem.at[count[0]], recv_sem.at[rel, piece], device)
        count[0] += 1
        copy.start()
        sends.append(copy)

    def arrival(piece, rel, owner):
        spot = place(piece, owner)
        remote(spot, spot, send_sem.at[0], recv_sem.at[rel, piece], me).wait_recv()
        return spot

    own = {}
    local = []
    for piece in (0, 2, 1, 3):
        family, layer = PIECES[piece]
        u, p, p_out, w, full = params[family]
        index = 2 * family + layer
        new = p[layer] - rate * ratio[index:index + 1, 0:1] * u[layer]
        p_out[layer] = new
        w[layer] = new.astype(jnp.bfloat16)
        own[piece] = w.at[layer]
        if family == 0:
            forward(own[piece], piece, me, near_x, 2)
        else:
            forward(own[piece], piece, me, near_y, 4)
        forward(own[piece], piece, me, partner, 1)
        copy = pltpu.make_async_copy(own[piece], place(piece, me), local_sem.at[piece])
        copy.start()
        local.append(copy)
    for piece in (2, 3):
        forward(own[piece], piece, me, near_x, 2)
    for piece in (0, 1):
        forward(own[piece], piece, me, near_y, 4)
    diag = near_x + near_y - me
    for k in range(2):
        spot = arrival(k, 2, near_x)
        forward(spot, k, near_x, near_y, 6)
        forward(spot, k, near_x, partner, 3)
        spot = arrival(2 + k, 4, near_y)
        forward(spot, 2 + k, near_y, near_x, 6)
        forward(spot, 2 + k, near_y, partner, 5)
    for k in range(2):
        spot = arrival(2 + k, 2, near_x)
        forward(spot, 2 + k, near_x, partner, 3)
        spot = arrival(k, 4, near_y)
        forward(spot, k, near_y, partner, 5)
    for k in range(2):
        for piece in (2 + k, k):
            spot = arrival(piece, 6, diag)
            forward(spot, piece, diag, partner, 7)
    for rel, owner in ((1, partner), (3, near_x + partner - me), (5, near_y + partner - me), (7, diag + partner - me)):
        for piece in range(4):
            arrival(piece, rel, owner)
    for copy in sends:
        copy.wait_send()
    for copy in local:
        copy.wait()


def update_and_gather(group_size, learn_rate, stats, u_up, u_down, p_up, p_down):
    up, down = p_up.shape, p_down.shape
    vmem = pl.BlockSpec(memory_space=pltpu.VMEM)
    hbm = pl.BlockSpec(memory_space=pl.ANY)
    return pl.pallas_call(
        functools.partial(update_kernel, group_size),
        out_shape=[
            jax.ShapeDtypeStruct((up[0], up[1] * group_size, up[2]), jnp.bfloat16),
            jax.ShapeDtypeStruct((down[0], down[1] * group_size, down[2]), jnp.bfloat16),
            jax.ShapeDtypeStruct(up, jnp.float32),
            jax.ShapeDtypeStruct(down, jnp.float32),
        ],
        in_specs=[pl.BlockSpec(memory_space=pltpu.SMEM)] + [vmem] * 5,
        out_specs=[hbm, hbm, vmem, vmem],
        scratch_shapes=[
            pltpu.VMEM((group_size, 8, 128), jnp.float32),
            pltpu.VMEM(up, jnp.bfloat16),
            pltpu.VMEM(down, jnp.bfloat16),
            pltpu.SemaphoreType.DMA((group_size,)),
            pltpu.SemaphoreType.DMA((group_size,)),
            pltpu.SemaphoreType.DMA((32,)),
            pltpu.SemaphoreType.DMA((group_size, 4)),
            pltpu.SemaphoreType.DMA((4,)),
        ],
        compiler_params=pltpu.CompilerParams(collective_id=1, has_side_effects=True, vmem_limit_bytes=40 * 1024 * 1024),
        name="update_and_gather",
    )(learn_rate.reshape(1), stats, u_up, u_down, p_up, p_down)


def sum_squares(stacked):
    return jnp.sum(stacked * stacked, axis=(1, 2))


def solution(mesh):
    group_size = mesh.shape["data"]
    batch_rows = P("data", None)
    state_rows = P(None, "data", None)
    replicated = P()

    def device_step(act_in, grad_out, w_up, w_down, master_up, master_down, exp_avg_up, exp_avg_down, exp_sq_up, exp_sq_down, learn_rate, clip_norm):
        act_one, slope_one, hidden = forward_block(act_in, w_up, w_down)
        shard_one, shard_two, shard_three, shard_four = backward_blocks(group_size, act_in, grad_out, hidden, act_one, slope_one, w_up, w_down)
        grad_up = jnp.stack([shard_one, shard_three])
        grad_down = jnp.stack([shard_two, shard_four])
        local_sq = jnp.sum(grad_up * grad_up) + jnp.sum(grad_down * grad_down)
        grad_norm = jnp.sqrt(stat_sum(jnp.full((8, 128), local_sq), group_size)[0, 0])
        clip_scale = jnp.minimum(1.0, clip_norm / (grad_norm + NORM_EPS))
        master_sq = jnp.concatenate([sum_squares(master_up), sum_squares(master_down)])
        avg_up, avg_down, sq_up, sq_down, dir_up, dir_down, dir_stats = moments(clip_scale, grad_up, grad_down, exp_avg_up, exp_avg_down, exp_sq_up, exp_sq_down)
        stats = dir_stats + jnp.pad(master_sq, (0, 4))[:, None]
        new_w_up, new_w_down, master_up_out, master_down_out = update_and_gather(group_size, learn_rate, stats, dir_up, dir_down, master_up, master_down)
        return (new_w_up, new_w_down, master_up_out, master_down_out, avg_up, avg_down, sq_up, sq_down, grad_norm)

    return jax.shard_map(device_step, mesh=mesh, in_specs=(batch_rows, batch_rows, replicated, replicated, state_rows, state_rows, state_rows, state_rows, state_rows, state_rows, replicated, replicated), out_specs=(replicated, replicated, state_rows, state_rows, state_rows, state_rows, state_rows, state_rows, replicated), check_vma=False)
```

```python
import functools

import jax
import jax.numpy as jnp
from jax import lax
from jax.experimental import pallas as pl
from jax.experimental.pallas import tpu as pltpu
from jax.sharding import PartitionSpec as P

STEP = 10
BETA_ONE = 0.9
BETA_TWO = 0.95
ADAM_EPS = 1e-8
NORM_EPS = 1e-6
INV_SQRT_TWO = 0.7071067811865476
INV_SQRT_TWO_PI = 0.3989422804014327


def gelu_parts(pre_act):
    normal_cdf = 0.5 * (1.0 + lax.erf(pre_act * INV_SQRT_TWO))
    normal_pdf = jnp.exp(-0.5 * pre_act * pre_act) * INV_SQRT_TWO_PI
    return pre_act * normal_cdf, normal_cdf + pre_act * normal_pdf


MESH = pl.DeviceIdType.MESH


def coords():
    me = lax.axis_index("data")
    core, col, row = me % 2, (me // 2) % 2, me // 4
    return me, me + 1 - 2 * core, me + 2 - 4 * col, me + 4 - 8 * row


def remote(src, dst, send_sem, recv_sem, device):
    return pltpu.make_async_remote_copy(src_ref=src, dst_ref=dst, send_sem=send_sem, recv_sem=recv_sem, device_id=(device,), device_id_type=MESH)


def meet_all(me, group_size):
    barrier = pltpu.get_barrier_semaphore()
    for step in range(1, group_size):
        pl.semaphore_signal(barrier, inc=1, device_id=((me + step) % group_size,), device_id_type=MESH)
    pl.semaphore_wait(barrier, group_size - 1)


def exchange_start(me, group_size, slots, send_sem, recv_sem):
    copies = []
    for step in range(1, group_size):
        copies.append(remote(slots.at[me], slots.at[me], send_sem.at[step], recv_sem.at[step], (me + step) % group_size))
        copies[-1].start()
    return copies


CHUNKS = 3
LANES = 128
TILE = 256
SLOTS = 4
OWNERS = tuple(chip * 2 + core for core in range(2) for chip in range(4))
FULL_VMEM = 67043328


def dot_nn(lhs, rhs):
    return jnp.dot(lhs, rhs, preferred_element_type=jnp.float32)


def dot_nt(lhs, rhs):
    return lax.dot_general(lhs, rhs, (((1,), (1,)), ((), ())), preferred_element_type=jnp.float32)


def dot_tn(lhs, rhs):
    return lax.dot_general(lhs, rhs, (((0,), (0,)), ((), ())), preferred_element_type=jnp.float32)


def chunk_blocks(chunk, width):
    return [owner * width + chunk * LANES for owner in OWNERS]


def forward_kernel(x_ref, w_up_ref, w_down_ref, a_out, s_out, h_out):
    x = x_ref[...]
    width = w_up_ref.shape[2] // len(OWNERS)
    total = None
    for chunk in range(CHUNKS):
        starts = chunk_blocks(chunk, width)
        w_in = jnp.concatenate([w_up_ref[0, :, s:s + LANES] for s in starts], axis=1)
        gelu, slope = gelu_parts(dot_nn(x, w_in))
        act = gelu.astype(jnp.bfloat16)
        a_out[chunk] = act
        s_out[chunk] = slope
        w_out = jnp.concatenate([w_down_ref[0, s:s + LANES, :] for s in starts], axis=0)
        part = dot_nn(act, w_out)
        total = part if total is None else total + part
    h_out[...] = total.astype(jnp.bfloat16)


def forward_block(act_in, w_up, w_down, tile=512):
    rows, dim = act_in.shape
    ff = w_up.shape[2]
    wide = ff // CHUNKS
    return pl.pallas_call(
        forward_kernel,
        grid=(rows // tile,),
        out_shape=[
            jax.ShapeDtypeStruct((CHUNKS, rows, wide), jnp.bfloat16),
            jax.ShapeDtypeStruct((CHUNKS, rows, wide), jnp.float32),
            jax.ShapeDtypeStruct((rows, dim), jnp.bfloat16),
        ],
        in_specs=[
            pl.BlockSpec((tile, dim), lambda i: (i, 0)),
            pl.BlockSpec((1, dim, ff), lambda i: (0, 0, 0)),
            pl.BlockSpec((1, ff, dim), lambda i: (0, 0, 0)),
        ],
        out_specs=[
            pl.BlockSpec((CHUNKS, tile, wide), lambda i: (0, i, 0)),
            pl.BlockSpec((CHUNKS, tile, wide), lambda i: (0, i, 0)),
            pl.BlockSpec((tile, dim), lambda i: (i, 0)),
        ],
        compiler_params=pltpu.CompilerParams(dimension_semantics=("arbitrary",), vmem_limit_bytes=FULL_VMEM),
        name="forward_block",
    )(act_in, w_up, w_down)


def backward_kernel(group_size, x_hbm, e_hbm, h_hbm, a_hbm, s_hbm, w_up_hbm, w_down_hbm,
                    g1_out, g2_out, g3_out, g4_out, norm_out, q_hbm,
                    h_v, e_v, wu_v, wd_v, a_v, q_v, s_v, t_d, t_u,
                    d0, d1a, d1b, d2a, d2b, u0, u1a, u1b, u2a, u2b,
                    sq_v, slots_v, load_sem, w_sem, q_sem, s_sem, send_sem, recv_sem, free_sem, stat_send, stat_recv):
    me, partner, near_x, near_y = coords()
    core, col, row = me % 2, (me // 2) % 2, me // 4
    rows, dim = h_v.shape
    half_rows = rows // 2
    wide = wu_v.shape[2]
    width = wide * CHUNKS // len(OWNERS)
    tiles = half_rows // TILE
    slots = s_v.shape[0]

    def at_rows(start, size):
        return pl.ds(pl.multiple_of(start, size), size)

    def half_copy(src, dst, half, sem):
        span = pl.ds(half * half_rows, half_rows)
        return pltpu.make_async_copy(src.at[span], dst.at[span], load_sem.at[sem, half])

    def start_weight(which, chunk, layer):
        for j, start in enumerate(chunk_blocks(chunk, width)):
            if which == 0:
                pltpu.make_async_copy(w_up_hbm.at[layer, :, pl.ds(start, LANES)], wu_v.at[chunk, :, pl.ds(j * LANES, LANES)], w_sem.at[0, chunk]).start()
            else:
                pltpu.make_async_copy(w_down_hbm.at[layer, pl.ds(start, LANES), :], wd_v.at[chunk, pl.ds(j * LANES, LANES), :], w_sem.at[1, chunk]).start()

    def wait_weight(which, chunk):
        ref = (wu_v, wd_v)[which]
        pltpu.make_async_copy(ref.at[chunk], ref.at[chunk], w_sem.at[which, chunk]).wait()

    half_copy(h_hbm, h_v, 0, 0).start()
    start_weight(0, 0, 1)
    half_copy(e_hbm, e_v, 0, 1).start()
    start_weight(1, 0, 1)
    sq_v[...] = jnp.zeros_like(sq_v)
    meet_all(me, group_size)

    def hop(src, dst, kind, chunk, stage, device):
        return remote(src, dst, send_sem.at[kind, chunk, stage], recv_sem.at[kind, chunk, stage], device)

    def hop0(kind, i):
        if kind == 0:
            return hop(t_d.at[1 - core], d0.at[i], 0, i, 0, partner)
        return hop(t_u.at[:, :, 1 - core], u0.at[i], 1, i, 0, partner)

    def bufs(kind):
        return (d0, d1a, d1b, d2a, d2b) if kind == 0 else (u0, u1a, u1b, u2a, u2b)

    def hop1(kind, i):
        b0, b1a, b1b, _, _ = bufs(kind)
        cut = b1a.shape[3]
        return (hop(b0.at[i, :, 1 - col, :, pl.ds(0, cut)], b1a.at[i], kind, i, 1, near_x),
                hop(b0.at[i, 1 - row, :, :, pl.ds(cut, cut)], b1b.at[i], kind, i, 2, near_y))

    def hop2(kind, i):
        _, b1a, b1b, b2a, b2b = bufs(kind)
        return (hop(b1a.at[i, 1 - row], b2a.at[i], kind, i, 3, near_y),
                hop(b1b.at[i, 1 - col], b2b.at[i], kind, i, 4, near_x))

    def rs0(kind, i):
        hop0(kind, i).start()

    def rs1(kind, i):
        hop0(kind, i).wait()
        b0 = bufs(kind)[0]
        for y in range(2):
            for x in range(2):
                own = t_d[core, y, x] if kind == 0 else t_u[y, x, core]
                b0[i, y, x] = b0[i, y, x] + own
        for copy in hop1(kind, i):
            copy.start()

    def rs2(kind, i):
        b0, b1a, b1b, _, _ = bufs(kind)
        cut = b1a.shape[3]
        first, second = hop1(kind, i)
        out_a, out_b = hop2(kind, i)
        first.wait()
        for y in range(2):
            b1a[i, y] = b1a[i, y] + b0[i, y, col, :, 0:cut]
        out_a.start()
        second.wait()
        for x in range(2):
            b1b[i, x] = b1b[i, x] + b0[i, row, x, :, cut:2 * cut]
        out_b.start()

    def rs3(kind, i, out):
        _, b1a, b1b, b2a, b2b = bufs(kind)
        cut = b1a.shape[3]
        for copy in hop2(kind, i):
            copy.wait()
        left = (b1a[i, row] + b2a[i]) / group_size
        right = (b1b[i, col] + b2b[i]) / group_size
        square = (left * left + right * right).reshape(left.shape[0] // 8, 8, cut).sum(axis=0)
        for lane in range(0, cut, LANES):
            sq_v[...] += square[:, lane:lane + LANES]
        if kind == 0:
            span = at_rows(i * LANES, LANES)
            out[span, 0:cut] = left
            out[span, cut:2 * cut] = right
        else:
            for j, owner in enumerate(OWNERS):
                part = (left, right)[j // 4]
                lane = (j % 4) * LANES
                out[:, pl.ds(pl.multiple_of(owner * width + i * LANES, LANES), LANES)] = part[:, lane:lane + LANES]

    def give_free(i):
        for device in (partner, near_x, near_y):
            pl.semaphore_signal(free_sem.at[i], inc=1, device_id=(device,), device_id_type=MESH)

    def grad_down(lhs_ref, rhs_ref, half, before_store=None):
        def part(m, carry):
            acc = dot_tn(lhs_ref[:, at_rows(m * (wide // 2), wide // 2)], rhs_ref[at_rows(half * half_rows, half_rows), :])
            if before_store is not None:
                before_store(m)
            acc = acc.reshape(t_d.shape[1:])
            t_d[m] = acc + jnp.where(half == 0, 0.0, t_d[m])
            return carry
        lax.fori_loop(0, 2, part, 0)

    def grad_up(lhs_ref, rhs_ref, half):
        def part(m, carry):
            acc = dot_tn(lhs_ref[at_rows(half * half_rows, half_rows), at_rows(m * (dim // 2), dim // 2)], rhs_ref[...])
            acc = acc.reshape(t_u.shape[1:])
            t_u[m] = acc + jnp.where(half == 0, 0.0, t_u[m])
            return carry
        lax.fori_loop(0, 2, part, 0)

    def q_copy(i, half):
        return pltpu.make_async_copy(q_v, q_hbm.at[i, at_rows(half * half_rows, half_rows), :], q_sem.at[0])

    def second_chunk(i, carry):
        wait_weight(0, i)
        wait_weight(1, i)

        @pl.when(i == 0)
        def _():
            half_copy(h_hbm, h_v, 0, 0).wait()
            half_copy(e_hbm, e_v, 0, 1).wait()
            half_copy(h_hbm, h_v, 1, 0).start()
            half_copy(e_hbm, e_v, 1, 1).start()
            for chunk in range(1, CHUNKS):
                start_weight(0, chunk, 1)
                start_weight(1, chunk, 1)

        def second_half(half, carry):
            @pl.when((i == 0) & (half == 1))
            def _():
                half_copy(h_hbm, h_v, 1, 0).wait()
                half_copy(e_hbm, e_v, 1, 1).wait()

            @pl.when((i > 0) | (half > 0))
            def _():
                q_copy(i, half).wait()

            def second_tile(t, carry):
                span = at_rows(half * half_rows + t * TILE, TILE)
                z = dot_nn(h_v[span, :], wu_v[i])
                p = dot_nt(e_v[span, :], wd_v[i])
                gelu, slope = gelu_parts(z)
                here = at_rows(t * TILE, TILE)
                a_v[here, :] = gelu.astype(jnp.bfloat16)
                q_v[here, :] = (p * slope).astype(jnp.bfloat16)

                @pl.when((t == tiles // 2) & (half == 0) & (i > 0))
                def _():
                    @pl.when(i > 1)
                    def _():
                        rs3(0, i - 2, g4_out)
                        rs3(1, i - 2, g3_out)
                        give_free(i - 2)
                    rs1(0, i - 1)
                    rs1(1, i - 1)
                return carry

            lax.fori_loop(0, tiles, second_tile, 0)
            q_copy(i, half).start()

            grad_down(a_v, e_v, half)

            @pl.when(half == 1)
            def _():
                rs0(0, i)

            @pl.when((half == 1) & (i > 0))
            def _():
                rs2(0, i - 1)
                rs2(1, i - 1)

            grad_up(h_v, q_v, half)

            @pl.when(half == 1)
            def _():
                rs0(1, i)
            return carry

        lax.fori_loop(0, 2, second_half, 0)
        return carry

    lax.fori_loop(0, CHUNKS, second_chunk, 0)

    q_copy(CHUNKS - 1, 1).wait()
    for half in range(2):
        half_copy(x_hbm, e_v, half, 1).start()
    for chunk in range(CHUNKS):
        start_weight(1, chunk, 0)
    r_rows = half_rows // 4
    staging = (a_v, q_v)

    def r_load(slot, t):
        for k in range(CHUNKS):
            pltpu.make_async_copy(q_hbm.at[k, at_rows(t * r_rows, r_rows), :], staging[slot].at[pl.ds(k * r_rows, r_rows), :], load_sem.at[2, slot]).start()

    def a_load(i, half):
        return pltpu.make_async_copy(a_hbm.at[i, pl.ds(half * half_rows, half_rows), :], staging[half], load_sem.at[0, half])

    for slot in range(2):
        r_load(slot, slot)
    r_steps = rows // r_rows // 2

    def r_pair(t, carry):
        for slot in range(2):
            whole = staging[slot].at[pl.ds(0, CHUNKS * r_rows), :]
            pltpu.make_async_copy(whole, whole, load_sem.at[2, slot]).wait()
            for part in range(2):
                m = part * (r_rows // 2)
                acc = dot_nt(staging[slot][m:m + r_rows // 2, :], wu_v[0])
                for k in range(1, CHUNKS):
                    acc = acc + dot_nt(staging[slot][k * r_rows + m:k * r_rows + m + r_rows // 2, :], wu_v[k])
                h_v[at_rows((2 * t + slot) * r_rows + m, r_rows // 2), :] = acc.astype(jnp.bfloat16)

            @pl.when(t < r_steps - 1)
            def _():
                r_load(slot, 2 * t + 2 + slot)

        @pl.when(t == 0)
        def _():
            rs3(0, CHUNKS - 2, g4_out)
            rs3(1, CHUNKS - 2, g3_out)
            give_free(CHUNKS - 2)
            rs1(0, CHUNKS - 1)
            rs1(1, CHUNKS - 1)
        return carry

    lax.fori_loop(0, r_steps, r_pair, 0)
    for half in range(2):
        a_load(0, half).start()

    def s_load(i, t):
        slot = lax.rem(t, slots)
        return pltpu.make_async_copy(s_hbm.at[i, at_rows(t * TILE, TILE), :], s_v.at[slot], s_sem.at[slot])

    for t in range(slots):
        s_load(0, t).start()
    rs2(0, CHUNKS - 1)
    rs2(1, CHUNKS - 1)

    def first_down(i, carry):
        for half in range(2):
            a_load(i, half).wait()

            def settle(m):
                @pl.when((m == 0) & (i > 0))
                def _():
                    rs1(0, i - 1)

            grad_down(staging[half], h_v, half, settle if half == 0 else None)

            @pl.when(i < CHUNKS - 1)
            def _():
                a_load(i + 1, half).start()

            if half == 0:
                @pl.when(i == 2)
                def _():
                    rs2(0, 0)

        @pl.when(i == 1)
        def _():
            rs3(0, CHUNKS - 1, g4_out)
            rs3(1, CHUNKS - 1, g3_out)
            give_free(CHUNKS - 1)

        pl.semaphore_wait(free_sem.at[i], 3)
        rs0(0, i)
        return carry

    lax.fori_loop(0, CHUNKS, first_down, 0)
    for half in range(2):
        half_copy(x_hbm, e_v, half, 1).wait()

    def first_up(i, carry):
        wait_weight(1, i)

        def first_half(half, carry):
            def first_tile(t, carry):
                tt = half * tiles + t
                s_load(i, tt).wait()
                p = dot_nt(h_v[at_rows(tt * TILE, TILE), :], wd_v[i])
                q_v[at_rows(t * TILE, TILE), :] = (p * s_v[lax.rem(tt, slots)]).astype(jnp.bfloat16)

                ahead = tt + slots
                @pl.when(ahead < 2 * tiles)
                def _():
                    s_load(i, ahead).start()

                @pl.when((t == tiles // 2) & (half == 0))
                def _():
                    @pl.when(i == 0)
                    def _():
                        rs1(0, 2)
                        rs2(0, 1)
                        rs3(0, 0, g2_out)

                    @pl.when(i == 1)
                    def _():
                        rs1(1, 0)
                        rs2(0, 2)
                        rs3(0, 1, g2_out)

                    @pl.when(i == 2)
                    def _():
                        rs1(1, 1)
                        rs2(1, 0)
                        rs3(0, 2, g2_out)
                return carry

            lax.fori_loop(0, tiles, first_tile, 0)

            @pl.when((half == 1) & (i < CHUNKS - 1))
            def _():
                for t in range(slots):
                    s_load(i + 1, t).start()

            grad_up(e_v, q_v, half)
            return carry

        lax.fori_loop(0, 2, first_half, 0)
        rs0(1, i)
        return carry

    lax.fori_loop(0, CHUNKS, first_up, 0)
    rs2(1, 1)
    rs1(1, 2)
    rs3(1, 0, g1_out)
    rs3(1, 1, g1_out)
    rs2(1, 2)
    rs3(1, 2, g1_out)
    slots_v[me] = sq_v[...]
    for copy in exchange_start(me, group_size, slots_v, stat_send, stat_recv):
        copy.wait()
    total = slots_v[0]
    for index in range(1, group_size):
        total = total + slots_v[index]
    norm_out[...] = jnp.full(norm_out.shape, jnp.sum(total))


def backward_blocks(group_size, act_in, grad_out, hidden, act_one, slope_one, w_up, w_down):
    rows, dim = act_in.shape
    ff = w_up.shape[2]
    wide = ff // CHUNKS
    up_rows, down_rows = dim // group_size, LANES
    hbm = pl.BlockSpec(memory_space=pl.ANY)
    vmem = pl.BlockSpec(memory_space=pltpu.VMEM)
    f32 = jnp.float32
    bf16 = jnp.bfloat16
    up_grad = jax.ShapeDtypeStruct((up_rows, ff), f32)
    down_grad = jax.ShapeDtypeStruct((ff // group_size, dim), f32)

    def stages(height, cols):
        return [
            pltpu.VMEM((CHUNKS, 2, 2, height, cols), f32),
            pltpu.VMEM((CHUNKS, 2, height, cols // 2), f32),
            pltpu.VMEM((CHUNKS, 2, height, cols // 2), f32),
            pltpu.VMEM((CHUNKS, height, cols // 2), f32),
            pltpu.VMEM((CHUNKS, height, cols // 2), f32),
        ]

    return pl.pallas_call(
        functools.partial(backward_kernel, group_size),
        out_shape=[up_grad, down_grad, up_grad, down_grad, jax.ShapeDtypeStruct((8, 128), f32), jax.ShapeDtypeStruct((CHUNKS, rows, wide), bf16)],
        in_specs=[hbm] * 7,
        out_specs=[vmem] * 5 + [hbm],
        scratch_shapes=[
            pltpu.VMEM((rows, dim), bf16),
            pltpu.VMEM((rows, dim), bf16),
            pltpu.VMEM((CHUNKS, dim, wide), bf16),
            pltpu.VMEM((CHUNKS, wide, dim), bf16),
            pltpu.VMEM((rows // 2, wide), bf16),
            pltpu.VMEM((rows // 2, wide), bf16),
            pltpu.VMEM((SLOTS, TILE, wide), f32),
            pltpu.VMEM((2, 2, 2, down_rows, dim), f32),
            pltpu.VMEM((2, 2, 2, up_rows, wide), f32),
            *stages(down_rows, dim),
            *stages(up_rows, wide),
            pltpu.VMEM((8, 128), f32),
            pltpu.VMEM((group_size, 8, 128), f32),
            pltpu.SemaphoreType.DMA((3, 2)),
            pltpu.SemaphoreType.DMA((2, CHUNKS)),
            pltpu.SemaphoreType.DMA((1,)),
            pltpu.SemaphoreType.DMA((SLOTS,)),
            pltpu.SemaphoreType.DMA((2, CHUNKS, 5)),
            pltpu.SemaphoreType.DMA((2, CHUNKS, 5)),
            pltpu.SemaphoreType.REGULAR((CHUNKS,)),
            pltpu.SemaphoreType.DMA((group_size,)),
            pltpu.SemaphoreType.DMA((group_size,)),
        ],
        compiler_params=pltpu.CompilerParams(collective_id=2, has_side_effects=True, vmem_limit_bytes=FULL_VMEM),
        name="backward_blocks",
    )(act_in, grad_out, hidden, act_one, slope_one, w_up, w_down)[:5]


def moments_kernel(clip_ref, norm_ref, g_one, g_two, g_three, g_four, m_up, m_down, v_up, v_down, m_up_out, m_down_out, v_up_out, v_down_out, u_up, u_down, stats):
    bias_one = 1.0 - BETA_ONE ** STEP
    bias_two = 1.0 - BETA_TWO ** STEP
    scale = jnp.minimum(1.0, clip_ref[0] / (jnp.sqrt(norm_ref[0:1, 0:1]) + NORM_EPS))
    row_id = lax.broadcasted_iota(jnp.int32, (8, 128), 0)
    sums = jnp.zeros((8, 128), jnp.float32)
    for family, (grads, m, v, m_out, v_out, u) in enumerate([((g_one, g_three), m_up, v_up, m_up_out, v_up_out, u_up), ((g_two, g_four), m_down, v_down, m_down_out, v_down_out, u_down)]):
        for layer in range(2):
            grad = grads[layer][...]
            avg_new = BETA_ONE * m[layer] + (1.0 - BETA_ONE) * scale * grad
            sq_new = BETA_TWO * v[layer] + (1.0 - BETA_TWO) * (scale * scale) * (grad * grad)
            direction = (avg_new / bias_one) / (jnp.sqrt(sq_new / bias_two) + ADAM_EPS)
            m_out[layer] = avg_new
            v_out[layer] = sq_new
            u[layer] = direction
            sums = sums + jnp.where(row_id == 4 + 2 * family + layer, jnp.sum(direction * direction), 0.0)

    @pl.when(pl.program_id(0) == 0)
    def _():
        stats[...] = jnp.zeros_like(stats)

    stats[...] += sums


def moments(clip_norm, norm_tile, grads, m_up, m_down, v_up, v_down, steps=4):
    up, down = m_up.shape, m_down.shape
    up_spec = pl.BlockSpec((2, up[1] // steps, up[2]), lambda i: (0, i, 0))
    down_spec = pl.BlockSpec((2, down[1] // steps, down[2]), lambda i: (0, i, 0))
    up_grad = pl.BlockSpec((up[1] // steps, up[2]), lambda i: (i, 0))
    down_grad = pl.BlockSpec((down[1] // steps, down[2]), lambda i: (i, 0))
    tile = pl.BlockSpec((8, 128), lambda i: (0, 0))
    pair = [up_spec, down_spec]
    up_shape, down_shape = jax.ShapeDtypeStruct(up, jnp.float32), jax.ShapeDtypeStruct(down, jnp.float32)
    return pl.pallas_call(
        moments_kernel,
        grid=(steps,),
        out_shape=[up_shape, down_shape] * 3 + [jax.ShapeDtypeStruct((8, 128), jnp.float32)],
        in_specs=[pl.BlockSpec(memory_space=pltpu.SMEM), tile] + [up_grad, down_grad] * 2 + pair * 2,
        out_specs=pair * 3 + [tile],
        compiler_params=pltpu.CompilerParams(dimension_semantics=("arbitrary",), vmem_limit_bytes=FULL_VMEM),
        name="moments",
    )(clip_norm.reshape(1), norm_tile, *grads, m_up, m_down, v_up, v_down)


PIECES = ((0, 0), (0, 1), (1, 0), (1, 1))


def update_kernel(group_size, rate_ref, stats_ref, u_up_hbm, u_down_hbm, p_up_hbm, p_down_hbm, all_up, all_down, p_up_out, p_down_out,
                  slots, u_up, u_down, p_up, p_down, w_up, w_down, stat_send, stat_recv, send_sem, recv_sem, local_sem, in_sem, out_sem):
    me, partner, near_x, near_y = coords()
    loads = []
    for src, dst in ((p_up_hbm, p_up), (p_down_hbm, p_down), (u_up_hbm, u_up), (u_down_hbm, u_down)):
        for layer in range(2):
            copy = pltpu.make_async_copy(src.at[layer], dst.at[layer], in_sem.at[len(loads)])
            copy.start()
            loads.append(copy)
    row_id = lax.broadcasted_iota(jnp.int32, (8, 128), 0)
    stats = stats_ref[...]
    for index in range(4):
        loads[index].wait()
        master = (p_up, p_down)[index // 2][index % 2]
        stats = stats + jnp.where(row_id == index, jnp.sum(master * master), 0.0)
    slots[me] = stats
    meet_all(me, group_size)
    for copy in exchange_start(me, group_size, slots, stat_send, stat_recv):
        copy.wait()
    total = slots[0]
    for index in range(1, group_size):
        total = total + slots[index]
    ratio = jnp.sqrt(total[0:4]) / jnp.sqrt(total[4:8])
    rate = rate_ref[0]
    params = ((u_up, p_up, p_up_out, w_up, all_up), (u_down, p_down, p_down_out, w_down, all_down))

    def place(piece, owner):
        family, layer = PIECES[piece]
        full = params[family][4]
        rows = params[family][3].shape[1]
        return full.at[layer, pl.ds(pl.multiple_of(owner * rows, rows), rows), :]

    sends = []
    count = [0]

    def forward(src, piece, owner, device, rel):
        copy = remote(src, place(piece, owner), send_sem.at[count[0]], recv_sem.at[rel, piece], device)
        count[0] += 1
        copy.start()
        sends.append(copy)

    def arrival(piece, rel, owner):
        spot = place(piece, owner)
        remote(spot, spot, send_sem.at[0], recv_sem.at[rel, piece], me).wait_recv()
        return spot

    own = {}
    local = []
    for piece in (0, 2, 1, 3):
        family, layer = PIECES[piece]
        u, p, p_out, w, full = params[family]
        index = 2 * family + layer
        loads[4 + index].wait()
        new = p[layer] - rate * ratio[index:index + 1, 0:1] * u[layer]
        w[layer] = new.astype(jnp.bfloat16)
        own[piece] = w.at[layer]
        if family == 0:
            forward(own[piece], piece, me, near_x, 2)
        else:
            forward(own[piece], piece, me, near_y, 4)
        forward(own[piece], piece, me, partner, 1)
        copy = pltpu.make_async_copy(own[piece], place(piece, me), local_sem.at[piece])
        copy.start()
        local.append(copy)
        p[layer] = new
        copy = pltpu.make_async_copy(p.at[layer], p_out.at[layer], out_sem.at[piece])
        copy.start()
        local.append(copy)
    for piece in (2, 3):
        forward(own[piece], piece, me, near_x, 2)
    for piece in (0, 1):
        forward(own[piece], piece, me, near_y, 4)
    diag = near_x + near_y - me
    for k in range(2):
        spot = arrival(k, 2, near_x)
        forward(spot, k, near_x, near_y, 6)
        forward(spot, k, near_x, partner, 3)
        spot = arrival(2 + k, 4, near_y)
        forward(spot, 2 + k, near_y, near_x, 6)
        forward(spot, 2 + k, near_y, partner, 5)
    for k in range(2):
        spot = arrival(2 + k, 2, near_x)
        forward(spot, 2 + k, near_x, partner, 3)
        spot = arrival(k, 4, near_y)
        forward(spot, k, near_y, partner, 5)
    for k in range(2):
        for piece in (2 + k, k):
            spot = arrival(piece, 6, diag)
            forward(spot, piece, diag, partner, 7)
    for rel, owner in ((1, partner), (3, near_x + partner - me), (5, near_y + partner - me), (7, diag + partner - me)):
        for piece in range(4):
            arrival(piece, rel, owner)
    for copy in sends:
        copy.wait_send()
    for copy in local:
        copy.wait()


def update_and_gather(group_size, learn_rate, stats, u_up, u_down, p_up, p_down):
    up, down = p_up.shape, p_down.shape
    vmem = pl.BlockSpec(memory_space=pltpu.VMEM)
    hbm = pl.BlockSpec(memory_space=pl.ANY)
    return pl.pallas_call(
        functools.partial(update_kernel, group_size),
        out_shape=[
            jax.ShapeDtypeStruct((up[0], up[1] * group_size, up[2]), jnp.bfloat16),
            jax.ShapeDtypeStruct((down[0], down[1] * group_size, down[2]), jnp.bfloat16),
            jax.ShapeDtypeStruct(up, jnp.float32),
            jax.ShapeDtypeStruct(down, jnp.float32),
        ],
        in_specs=[pl.BlockSpec(memory_space=pltpu.SMEM), vmem] + [hbm] * 4,
        out_specs=[hbm] * 4,
        scratch_shapes=[
            pltpu.VMEM((group_size, 8, 128), jnp.float32),
            pltpu.VMEM(up, jnp.float32),
            pltpu.VMEM(down, jnp.float32),
            pltpu.VMEM(up, jnp.float32),
            pltpu.VMEM(down, jnp.float32),
            pltpu.VMEM(up, jnp.bfloat16),
            pltpu.VMEM(down, jnp.bfloat16),
            pltpu.SemaphoreType.DMA((group_size,)),
            pltpu.SemaphoreType.DMA((group_size,)),
            pltpu.SemaphoreType.DMA((32,)),
            pltpu.SemaphoreType.DMA((group_size, 4)),
            pltpu.SemaphoreType.DMA((4,)),
            pltpu.SemaphoreType.DMA((8,)),
            pltpu.SemaphoreType.DMA((4,)),
        ],
        compiler_params=pltpu.CompilerParams(collective_id=1, has_side_effects=True, vmem_limit_bytes=FULL_VMEM),
        name="update_and_gather",
    )(learn_rate.reshape(1), stats, u_up, u_down, p_up, p_down)


def solution(mesh):
    group_size = mesh.shape["data"]
    batch_rows = P("data", None)
    state_rows = P(None, "data", None)
    replicated = P()

    def device_step(act_in, grad_out, w_up, w_down, master_up, master_down, exp_avg_up, exp_avg_down, exp_sq_up, exp_sq_down, learn_rate, clip_norm):
        act_one, slope_one, hidden = forward_block(act_in, w_up, w_down)
        *grads, norm_tile = backward_blocks(group_size, act_in, grad_out, hidden, act_one, slope_one, w_up, w_down)
        grad_norm = jnp.sqrt(norm_tile[0, 0])
        avg_up, avg_down, sq_up, sq_down, dir_up, dir_down, stats = moments(clip_norm, norm_tile, grads, exp_avg_up, exp_avg_down, exp_sq_up, exp_sq_down)
        new_w_up, new_w_down, master_up_out, master_down_out = update_and_gather(group_size, learn_rate, stats, dir_up, dir_down, master_up, master_down)
        return (new_w_up, new_w_down, master_up_out, master_down_out, avg_up, avg_down, sq_up, sq_down, grad_norm)

    return jax.shard_map(device_step, mesh=mesh, in_specs=(batch_rows, batch_rows, replicated, replicated, state_rows, state_rows, state_rows, state_rows, state_rows, state_rows, replicated, replicated), out_specs=(replicated, replicated, state_rows, state_rows, state_rows, state_rows, state_rows, state_rows, replicated), check_vma=False)
```

```python
import functools

import jax
import jax.numpy as jnp
from jax import lax
from jax.experimental import pallas as pl
from jax.experimental.pallas import tpu as pltpu
from jax.sharding import PartitionSpec as P

STEP = 10
BETA_ONE = 0.9
BETA_TWO = 0.95
ADAM_EPS = 1e-8
NORM_EPS = 1e-6
INV_SQRT_TWO = 0.7071067811865476
INV_SQRT_TWO_PI = 0.3989422804014327


def gelu_parts(pre_act):
    normal_cdf = 0.5 * (1.0 + lax.erf(pre_act * INV_SQRT_TWO))
    normal_pdf = jnp.exp(-0.5 * pre_act * pre_act) * INV_SQRT_TWO_PI
    return pre_act * normal_cdf, normal_cdf + pre_act * normal_pdf


MESH = pl.DeviceIdType.MESH


def coords():
    me = lax.axis_index("data")
    core, col, row = me % 2, (me // 2) % 2, me // 4
    return me, me + 1 - 2 * core, me + 2 - 4 * col, me + 4 - 8 * row


def remote(src, dst, send_sem, recv_sem, device):
    return pltpu.make_async_remote_copy(src_ref=src, dst_ref=dst, send_sem=send_sem, recv_sem=recv_sem, device_id=(device,), device_id_type=MESH)


def meet_all(me, group_size):
    barrier = pltpu.get_barrier_semaphore()
    for step in range(1, group_size):
        pl.semaphore_signal(barrier, inc=1, device_id=((me + step) % group_size,), device_id_type=MESH)
    pl.semaphore_wait(barrier, group_size - 1)


def exchange_start(me, group_size, slots, send_sem, recv_sem):
    copies = []
    for step in range(1, group_size):
        copies.append(remote(slots.at[me], slots.at[me], send_sem.at[step], recv_sem.at[step], (me + step) % group_size))
        copies[-1].start()
    return copies


CHUNKS = 3
LANES = 128
TILE = 256
SLOTS = 4
OWNERS = tuple(chip * 2 + core for core in range(2) for chip in range(4))
FULL_VMEM = 67043328


def dot_nn(lhs, rhs):
    return jnp.dot(lhs, rhs, preferred_element_type=jnp.float32)


def dot_nt(lhs, rhs):
    return lax.dot_general(lhs, rhs, (((1,), (1,)), ((), ())), preferred_element_type=jnp.float32)


def dot_tn(lhs, rhs):
    return lax.dot_general(lhs, rhs, (((0,), (0,)), ((), ())), preferred_element_type=jnp.float32)


def chunk_blocks(chunk, width):
    return [owner * width + chunk * LANES for owner in OWNERS]


def forward_kernel(x_ref, w_up_ref, w_down_ref, a_out, s_out, h_out):
    x = x_ref[...]
    width = w_up_ref.shape[2] // len(OWNERS)
    total = None
    for chunk in range(CHUNKS):
        starts = chunk_blocks(chunk, width)
        w_in = jnp.concatenate([w_up_ref[0, :, s:s + LANES] for s in starts], axis=1)
        gelu, slope = gelu_parts(dot_nn(x, w_in))
        act = gelu.astype(jnp.bfloat16)
        a_out[chunk] = act
        s_out[chunk] = slope
        w_out = jnp.concatenate([w_down_ref[0, s:s + LANES, :] for s in starts], axis=0)
        part = dot_nn(act, w_out)
        total = part if total is None else total + part
    h_out[...] = total.astype(jnp.bfloat16)


def forward_block(act_in, w_up, w_down, tile=512):
    rows, dim = act_in.shape
    ff = w_up.shape[2]
    wide = ff // CHUNKS
    return pl.pallas_call(
        forward_kernel,
        grid=(rows // tile,),
        out_shape=[
            jax.ShapeDtypeStruct((CHUNKS, rows, wide), jnp.bfloat16),
            jax.ShapeDtypeStruct((CHUNKS, rows, wide), jnp.float32),
            jax.ShapeDtypeStruct((rows, dim), jnp.bfloat16),
        ],
        in_specs=[
            pl.BlockSpec((tile, dim), lambda i: (i, 0)),
            pl.BlockSpec((1, dim, ff), lambda i: (0, 0, 0)),
            pl.BlockSpec((1, ff, dim), lambda i: (0, 0, 0)),
        ],
        out_specs=[
            pl.BlockSpec((CHUNKS, tile, wide), lambda i: (0, i, 0)),
            pl.BlockSpec((CHUNKS, tile, wide), lambda i: (0, i, 0)),
            pl.BlockSpec((tile, dim), lambda i: (i, 0)),
        ],
        compiler_params=pltpu.CompilerParams(dimension_semantics=("arbitrary",), vmem_limit_bytes=FULL_VMEM),
        name="forward_block",
    )(act_in, w_up, w_down)


def backward_kernel(group_size, x_hbm, e_hbm, h_hbm, a_hbm, s_hbm, w_up_hbm, w_down_hbm,
                    g1_out, g2_out, g3_out, g4_out, norm_out, q_hbm,
                    h_v, e_v, wu_v, wd_v, a_v, q_v, s_v, t_d, t_u,
                    d0, d1a, d1b, d2a, d2b, u0, u1a, u1b, u2a, u2b,
                    sq_v, slots_v, load_sem, w_sem, q_sem, s_sem, send_sem, recv_sem, free_sem, stat_send, stat_recv):
    me, partner, near_x, near_y = coords()
    core, col, row = me % 2, (me // 2) % 2, me // 4
    rows, dim = h_v.shape
    half_rows = rows // 2
    wide = wu_v.shape[2]
    width = wide * CHUNKS // len(OWNERS)
    tiles = half_rows // TILE
    slots = s_v.shape[0]

    def at_rows(start, size):
        return pl.ds(pl.multiple_of(start, size), size)

    def half_copy(src, dst, half, sem):
        span = pl.ds(half * half_rows, half_rows)
        return pltpu.make_async_copy(src.at[span], dst.at[span], load_sem.at[sem, half])

    def start_weight(which, chunk, layer):
        for j, start in enumerate(chunk_blocks(chunk, width)):
            if which == 0:
                pltpu.make_async_copy(w_up_hbm.at[layer, :, pl.ds(start, LANES)], wu_v.at[chunk, :, pl.ds(j * LANES, LANES)], w_sem.at[0, chunk]).start()
            else:
                pltpu.make_async_copy(w_down_hbm.at[layer, pl.ds(start, LANES), :], wd_v.at[chunk, pl.ds(j * LANES, LANES), :], w_sem.at[1, chunk]).start()

    def wait_weight(which, chunk):
        ref = (wu_v, wd_v)[which]
        pltpu.make_async_copy(ref.at[chunk], ref.at[chunk], w_sem.at[which, chunk]).wait()

    half_copy(h_hbm, h_v, 0, 0).start()
    start_weight(0, 0, 1)
    half_copy(e_hbm, e_v, 0, 1).start()
    start_weight(1, 0, 1)
    sq_v[...] = jnp.zeros_like(sq_v)
    meet_all(me, group_size)

    def hop(src, dst, kind, chunk, stage, device):
        return remote(src, dst, send_sem.at[kind, chunk, stage], recv_sem.at[kind, chunk, stage], device)

    def hop0(kind, i):
        if kind == 0:
            return hop(t_d.at[1 - core], d0.at[i], 0, i, 0, partner)
        return hop(t_u.at[:, :, 1 - core], u0.at[i], 1, i, 0, partner)

    def bufs(kind):
        return (d0, d1a, d1b, d2a, d2b) if kind == 0 else (u0, u1a, u1b, u2a, u2b)

    def hop1(kind, i):
        b0, b1a, b1b, _, _ = bufs(kind)
        cut = b1a.shape[3]
        return (hop(b0.at[i, :, 1 - col, :, pl.ds(0, cut)], b1a.at[i], kind, i, 1, near_x),
                hop(b0.at[i, 1 - row, :, :, pl.ds(cut, cut)], b1b.at[i], kind, i, 2, near_y))

    def hop2(kind, i):
        _, b1a, b1b, b2a, b2b = bufs(kind)
        return (hop(b1a.at[i, 1 - row], b2a.at[i], kind, i, 3, near_y),
                hop(b1b.at[i, 1 - col], b2b.at[i], kind, i, 4, near_x))

    def rs0(kind, i):
        hop0(kind, i).start()

    def rs1(kind, i):
        hop0(kind, i).wait()
        b0 = bufs(kind)[0]
        for y in range(2):
            for x in range(2):
                own = t_d[core, y, x] if kind == 0 else t_u[y, x, core]
                b0[i, y, x] = b0[i, y, x] + own
        for copy in hop1(kind, i):
            copy.start()

    def rs2(kind, i):
        b0, b1a, b1b, _, _ = bufs(kind)
        cut = b1a.shape[3]
        first, second = hop1(kind, i)
        out_a, out_b = hop2(kind, i)
        first.wait()
        for y in range(2):
            b1a[i, y] = b1a[i, y] + b0[i, y, col, :, 0:cut]
        out_a.start()
        second.wait()
        for x in range(2):
            b1b[i, x] = b1b[i, x] + b0[i, row, x, :, cut:2 * cut]
        out_b.start()

    def rs3(kind, i, out):
        _, b1a, b1b, b2a, b2b = bufs(kind)
        cut = b1a.shape[3]
        for copy in hop2(kind, i):
            copy.wait()
        left = (b1a[i, row] + b2a[i]) / group_size
        right = (b1b[i, col] + b2b[i]) / group_size
        square = (left * left + right * right).reshape(left.shape[0] // 8, 8, cut).sum(axis=0)
        for lane in range(0, cut, LANES):
            sq_v[...] += square[:, lane:lane + LANES]
        if kind == 0:
            span = at_rows(i * LANES, LANES)
            out[span, 0:cut] = left
            out[span, cut:2 * cut] = right
        else:
            for j, owner in enumerate(OWNERS):
                part = (left, right)[j // 4]
                lane = (j % 4) * LANES
                out[:, pl.ds(pl.multiple_of(owner * width + i * LANES, LANES), LANES)] = part[:, lane:lane + LANES]

    def give_free(i):
        for device in (partner, near_x, near_y):
            pl.semaphore_signal(free_sem.at[i], inc=1, device_id=(device,), device_id_type=MESH)

    def grad_down(lhs_ref, rhs_ref, half):
        def part(m, carry):
            acc = dot_tn(lhs_ref[:, at_rows(m * (wide // 2), wide // 2)], rhs_ref[at_rows(half * half_rows, half_rows), :])
            acc = acc.reshape(t_d.shape[1:])
            t_d[m] = acc + jnp.where(half == 0, 0.0, t_d[m])
            return carry
        lax.fori_loop(0, 2, part, 0)

    def grad_up(lhs_ref, rhs_ref, half):
        def part(m, carry):
            acc = dot_tn(lhs_ref[at_rows(half * half_rows, half_rows), at_rows(m * (dim // 2), dim // 2)], rhs_ref[...])
            acc = acc.reshape(t_u.shape[1:])
            t_u[m] = acc + jnp.where(half == 0, 0.0, t_u[m])
            return carry
        lax.fori_loop(0, 2, part, 0)

    def q_copy(i, half):
        return pltpu.make_async_copy(q_v, q_hbm.at[i, at_rows(half * half_rows, half_rows), :], q_sem.at[0])

    def second_chunk(i, carry):
        wait_weight(0, i)
        wait_weight(1, i)

        @pl.when(i == 0)
        def _():
            half_copy(h_hbm, h_v, 0, 0).wait()
            half_copy(e_hbm, e_v, 0, 1).wait()
            half_copy(h_hbm, h_v, 1, 0).start()
            half_copy(e_hbm, e_v, 1, 1).start()
            for chunk in range(1, CHUNKS):
                start_weight(0, chunk, 1)
                start_weight(1, chunk, 1)

        def second_half(half, carry):
            @pl.when((i == 0) & (half == 1))
            def _():
                half_copy(h_hbm, h_v, 1, 0).wait()
                half_copy(e_hbm, e_v, 1, 1).wait()

            @pl.when((i > 0) | (half > 0))
            def _():
                q_copy(i, half).wait()

            def second_tile(t, carry):
                span = at_rows(half * half_rows + t * TILE, TILE)
                z = dot_nn(h_v[span, :], wu_v[i])
                p = dot_nt(e_v[span, :], wd_v[i])
                gelu, slope = gelu_parts(z)
                here = at_rows(t * TILE, TILE)
                a_v[here, :] = gelu.astype(jnp.bfloat16)
                q_v[here, :] = (p * slope).astype(jnp.bfloat16)

                @pl.when((half == 0) & (i > 1))
                def _():
                    @pl.when(t == 0)
                    def _():
                        rs2(1, i - 2)

                    @pl.when(t == 2)
                    def _():
                        rs3(0, i - 2, g4_out)

                @pl.when((t == tiles // 2) & (half == 0) & (i > 0))
                def _():
                    rs1(0, i - 1)

                @pl.when((t == 3) & (half == 1) & (i > 0))
                def _():
                    rs2(0, i - 1)
                return carry

            lax.fori_loop(0, tiles, second_tile, 0)
            q_copy(i, half).start()

            @pl.when((half == 0) & (i > 1))
            def _():
                rs3(1, i - 2, g3_out)
                give_free(i - 2)

            grad_down(a_v, e_v, half)

            @pl.when(half == 1)
            def _():
                rs0(0, i)

            @pl.when((half == 0) & (i > 0))
            def _():
                rs1(1, i - 1)

            grad_up(h_v, q_v, half)

            @pl.when(half == 1)
            def _():
                rs0(1, i)
            return carry

        lax.fori_loop(0, 2, second_half, 0)
        return carry

    lax.fori_loop(0, CHUNKS, second_chunk, 0)

    q_copy(CHUNKS - 1, 1).wait()
    for half in range(2):
        half_copy(x_hbm, e_v, half, 1).start()
    for chunk in range(CHUNKS):
        start_weight(1, chunk, 0)
    r_rows = half_rows // 4
    staging = (a_v, q_v)

    def r_load(slot, t):
        for k in range(CHUNKS):
            pltpu.make_async_copy(q_hbm.at[k, at_rows(t * r_rows, r_rows), :], staging[slot].at[pl.ds(k * r_rows, r_rows), :], load_sem.at[2, slot]).start()

    def a_load(i, half):
        return pltpu.make_async_copy(a_hbm.at[i, pl.ds(half * half_rows, half_rows), :], staging[half], load_sem.at[0, half])

    for slot in range(2):
        r_load(slot, slot)
    r_steps = rows // r_rows // 2

    def r_pair(t, carry):
        for slot in range(2):
            whole = staging[slot].at[pl.ds(0, CHUNKS * r_rows), :]
            pltpu.make_async_copy(whole, whole, load_sem.at[2, slot]).wait()
            for part in range(2):
                m = part * (r_rows // 2)
                acc = dot_nt(staging[slot][m:m + r_rows // 2, :], wu_v[0])
                for k in range(1, CHUNKS):
                    acc = acc + dot_nt(staging[slot][k * r_rows + m:k * r_rows + m + r_rows // 2, :], wu_v[k])
                h_v[at_rows((2 * t + slot) * r_rows + m, r_rows // 2), :] = acc.astype(jnp.bfloat16)

            @pl.when(t < r_steps - 1)
            def _():
                r_load(slot, 2 * t + 2 + slot)

        @pl.when(t == 0)
        def _():
            rs1(0, CHUNKS - 1)
            rs3(0, CHUNKS - 2, g4_out)

        @pl.when(t == 1)
        def _():
            rs1(1, CHUNKS - 1)
            rs3(1, CHUNKS - 2, g3_out)
            give_free(CHUNKS - 2)
        return carry

    rs2(1, CHUNKS - 2)
    lax.fori_loop(0, r_steps, r_pair, 0)
    for half in range(2):
        a_load(0, half).start()

    def s_load(i, t):
        slot = lax.rem(t, slots)
        return pltpu.make_async_copy(s_hbm.at[i, at_rows(t * TILE, TILE), :], s_v.at[slot], s_sem.at[slot])

    for t in range(slots):
        s_load(0, t).start()
    rs2(0, CHUNKS - 1)

    def first_chunk(i, carry):
        a_load(i, 0).wait()
        grad_down(a_v, h_v, 0)

        @pl.when(i < CHUNKS - 1)
        def _():
            a_load(i + 1, 0).start()

        @pl.when(i == 2)
        def _():
            rs2(1, 0)

        a_load(i, 1).wait()
        grad_down(q_v, h_v, 1)
        pl.semaphore_wait(free_sem.at[i], 3)
        rs0(0, i)
        wait_weight(1, i)

        @pl.when(i == 0)
        def _():
            for half in range(2):
                half_copy(x_hbm, e_v, half, 1).wait()

        def first_half(half, carry):
            def first_tile(t, carry):
                tt = half * tiles + t
                s_load(i, tt).wait()
                p = dot_nt(h_v[at_rows(tt * TILE, TILE), :], wd_v[i])
                q_v[at_rows(t * TILE, TILE), :] = (p * s_v[lax.rem(tt, slots)]).astype(jnp.bfloat16)

                ahead = tt + slots
                @pl.when(ahead < 2 * tiles)
                def _():
                    s_load(i, ahead).start()

                @pl.when((tt == 6) & (i == 0))
                def _():
                    rs3(0, 2, g4_out)

                @pl.when((tt == tiles + 3) & (i == 2))
                def _():
                    rs3(1, 0, g1_out)
                return carry

            @pl.when(half == 0)
            def _():
                @pl.when(i == 0)
                def _():
                    rs2(1, 2)

                @pl.when(i == 1)
                def _():
                    rs2(0, 0)

                @pl.when(i > 0)
                def _():
                    rs1(1, i - 1)

            @pl.when(half == 1)
            def _():
                @pl.when(i == 2)
                def _():
                    rs2(0, 1)

                rs1(0, i)

                @pl.when(i == 0)
                def _():
                    rs3(1, 2, g3_out)
                    give_free(2)

                @pl.when(i == 1)
                def _():
                    rs3(0, 0, g2_out)

            lax.fori_loop(0, tiles, first_tile, 0)

            @pl.when((half == 1) & (i < CHUNKS - 1))
            def _():
                for t in range(slots):
                    s_load(i + 1, t).start()

            grad_up(e_v, q_v, half)
            return carry

        lax.fori_loop(0, 2, first_half, 0)
        rs0(1, i)

        @pl.when(i < CHUNKS - 1)
        def _():
            a_load(i + 1, 1).start()
        return carry

    lax.fori_loop(0, CHUNKS, first_chunk, 0)
    rs2(1, 1)
    rs1(1, 2)
    rs3(0, 1, g2_out)
    rs2(0, 2)
    rs3(1, 1, g1_out)
    rs2(1, 2)
    rs3(0, 2, g2_out)
    rs3(1, 2, g1_out)
    slots_v[me] = sq_v[...]
    for copy in exchange_start(me, group_size, slots_v, stat_send, stat_recv):
        copy.wait()
    total = slots_v[0]
    for index in range(1, group_size):
        total = total + slots_v[index]
    norm_out[...] = jnp.full(norm_out.shape, jnp.sum(total))


def backward_blocks(group_size, act_in, grad_out, hidden, act_one, slope_one, w_up, w_down):
    rows, dim = act_in.shape
    ff = w_up.shape[2]
    wide = ff // CHUNKS
    up_rows, down_rows = dim // group_size, LANES
    hbm = pl.BlockSpec(memory_space=pl.ANY)
    vmem = pl.BlockSpec(memory_space=pltpu.VMEM)
    f32 = jnp.float32
    bf16 = jnp.bfloat16
    up_grad = jax.ShapeDtypeStruct((up_rows, ff), f32)
    down_grad = jax.ShapeDtypeStruct((ff // group_size, dim), f32)

    def stages(height, cols):
        return [
            pltpu.VMEM((CHUNKS, 2, 2, height, cols), f32),
            pltpu.VMEM((CHUNKS, 2, height, cols // 2), f32),
            pltpu.VMEM((CHUNKS, 2, height, cols // 2), f32),
            pltpu.VMEM((CHUNKS, height, cols // 2), f32),
            pltpu.VMEM((CHUNKS, height, cols // 2), f32),
        ]

    return pl.pallas_call(
        functools.partial(backward_kernel, group_size),
        out_shape=[up_grad, down_grad, up_grad, down_grad, jax.ShapeDtypeStruct((8, 128), f32), jax.ShapeDtypeStruct((CHUNKS, rows, wide), bf16)],
        in_specs=[hbm] * 7,
        out_specs=[vmem] * 5 + [hbm],
        scratch_shapes=[
            pltpu.VMEM((rows, dim), bf16),
            pltpu.VMEM((rows, dim), bf16),
            pltpu.VMEM((CHUNKS, dim, wide), bf16),
            pltpu.VMEM((CHUNKS, wide, dim), bf16),
            pltpu.VMEM((rows // 2, wide), bf16),
            pltpu.VMEM((rows // 2, wide), bf16),
            pltpu.VMEM((SLOTS, TILE, wide), f32),
            pltpu.VMEM((2, 2, 2, down_rows, dim), f32),
            pltpu.VMEM((2, 2, 2, up_rows, wide), f32),
            *stages(down_rows, dim),
            *stages(up_rows, wide),
            pltpu.VMEM((8, 128), f32),
            pltpu.VMEM((group_size, 8, 128), f32),
            pltpu.SemaphoreType.DMA((3, 2)),
            pltpu.SemaphoreType.DMA((2, CHUNKS)),
            pltpu.SemaphoreType.DMA((1,)),
            pltpu.SemaphoreType.DMA((SLOTS,)),
            pltpu.SemaphoreType.DMA((2, CHUNKS, 5)),
            pltpu.SemaphoreType.DMA((2, CHUNKS, 5)),
            pltpu.SemaphoreType.REGULAR((CHUNKS,)),
            pltpu.SemaphoreType.DMA((group_size,)),
            pltpu.SemaphoreType.DMA((group_size,)),
        ],
        compiler_params=pltpu.CompilerParams(collective_id=2, has_side_effects=True, vmem_limit_bytes=FULL_VMEM),
        name="backward_blocks",
    )(act_in, grad_out, hidden, act_one, slope_one, w_up, w_down)[:5]


def moments_kernel(clip_ref, norm_ref, g_one, g_two, g_three, g_four, m_up, m_down, v_up, v_down, m_up_out, m_down_out, v_up_out, v_down_out, u_up, u_down, stats):
    inv_one = 1.0 / (1.0 - BETA_ONE ** STEP)
    inv_two = 1.0 / (1.0 - BETA_TWO ** STEP)
    scale = jnp.minimum(1.0, clip_ref[0] / (jnp.sqrt(norm_ref[0:1, 0:1]) + NORM_EPS))
    row_id = lax.broadcasted_iota(jnp.int32, (8, 128), 0)
    sums = jnp.zeros((8, 128), jnp.float32)
    for family, (grads, m, v, m_out, v_out, u) in enumerate([((g_one, g_three), m_up, v_up, m_up_out, v_up_out, u_up), ((g_two, g_four), m_down, v_down, m_down_out, v_down_out, u_down)]):
        for layer in range(2):
            grad = grads[layer][...]
            avg_new = BETA_ONE * m[layer] + (1.0 - BETA_ONE) * scale * grad
            sq_new = BETA_TWO * v[layer] + (1.0 - BETA_TWO) * (scale * scale) * (grad * grad)
            direction = (avg_new * inv_one) / (jnp.sqrt(sq_new * inv_two) + ADAM_EPS)
            m_out[layer] = avg_new
            v_out[layer] = sq_new
            u[layer] = direction
            sums = sums + jnp.where(row_id == 4 + 2 * family + layer, jnp.sum(direction * direction), 0.0)

    @pl.when(pl.program_id(0) == 0)
    def _():
        stats[...] = jnp.zeros_like(stats)

    stats[...] += sums


def moments(clip_norm, norm_tile, grads, m_up, m_down, v_up, v_down, steps=6):
    up, down = m_up.shape, m_down.shape
    up_spec = pl.BlockSpec((2, up[1] // steps, up[2]), lambda i: (0, i, 0))
    down_spec = pl.BlockSpec((2, down[1] // steps, down[2]), lambda i: (0, i, 0))
    up_grad = pl.BlockSpec((up[1] // steps, up[2]), lambda i: (i, 0))
    down_grad = pl.BlockSpec((down[1] // steps, down[2]), lambda i: (i, 0))
    tile = pl.BlockSpec((8, 128), lambda i: (0, 0))
    pair = [up_spec, down_spec]
    up_shape, down_shape = jax.ShapeDtypeStruct(up, jnp.float32), jax.ShapeDtypeStruct(down, jnp.float32)
    return pl.pallas_call(
        moments_kernel,
        grid=(steps,),
        out_shape=[up_shape, down_shape] * 3 + [jax.ShapeDtypeStruct((8, 128), jnp.float32)],
        in_specs=[pl.BlockSpec(memory_space=pltpu.SMEM), tile] + [up_grad, down_grad] * 2 + pair * 2,
        out_specs=pair * 3 + [tile],
        compiler_params=pltpu.CompilerParams(dimension_semantics=("arbitrary",), vmem_limit_bytes=FULL_VMEM),
        name="moments",
    )(clip_norm.reshape(1), norm_tile, *grads, m_up, m_down, v_up, v_down)


PIECES = ((0, 0), (0, 1), (1, 0), (1, 1))


def update_kernel(group_size, rate_ref, stats_ref, u_up_hbm, u_down_hbm, p_up_hbm, p_down_hbm, all_up, all_down, p_up_out, p_down_out,
                  slots, u_up, u_down, p_up, p_down, w_up, w_down, stat_send, stat_recv, send_sem, recv_sem, local_sem, in_sem, out_sem):
    me, partner, near_x, near_y = coords()
    loads = []
    for src, dst in ((p_up_hbm, p_up), (p_down_hbm, p_down), (u_up_hbm, u_up), (u_down_hbm, u_down)):
        for layer in range(2):
            copy = pltpu.make_async_copy(src.at[layer], dst.at[layer], in_sem.at[len(loads)])
            copy.start()
            loads.append(copy)
    row_id = lax.broadcasted_iota(jnp.int32, (8, 128), 0)
    stats = stats_ref[...]
    for index in range(4):
        loads[index].wait()
        master = (p_up, p_down)[index // 2][index % 2]
        stats = stats + jnp.where(row_id == index, jnp.sum(master * master), 0.0)
    slots[me] = stats
    meet_all(me, group_size)
    for copy in exchange_start(me, group_size, slots, stat_send, stat_recv):
        copy.wait()
    total = slots[0]
    for index in range(1, group_size):
        total = total + slots[index]
    ratio = jnp.sqrt(total[0:4]) / jnp.sqrt(total[4:8])
    rate = rate_ref[0]
    params = ((u_up, p_up, p_up_out, w_up, all_up), (u_down, p_down, p_down_out, w_down, all_down))

    def place(piece, owner):
        family, layer = PIECES[piece]
        full = params[family][4]
        rows = params[family][3].shape[1]
        return full.at[layer, pl.ds(pl.multiple_of(owner * rows, rows), rows), :]

    sends = []
    count = [0]

    def forward(src, piece, owner, device, rel):
        copy = remote(src, place(piece, owner), send_sem.at[count[0]], recv_sem.at[rel, piece], device)
        count[0] += 1
        copy.start()
        sends.append(copy)

    def arrival(piece, rel, owner):
        spot = place(piece, owner)
        remote(spot, spot, send_sem.at[0], recv_sem.at[rel, piece], me).wait_recv()
        return spot

    own = {}
    local = []
    for piece in (0, 2, 1, 3):
        family, layer = PIECES[piece]
        u, p, p_out, w, full = params[family]
        index = 2 * family + layer
        loads[4 + index].wait()
        new = p[layer] - rate * ratio[index:index + 1, 0:1] * u[layer]
        w[layer] = new.astype(jnp.bfloat16)
        own[piece] = w.at[layer]
        if family == 0:
            forward(own[piece], piece, me, near_x, 2)
        else:
            forward(own[piece], piece, me, near_y, 4)
        forward(own[piece], piece, me, partner, 1)
        copy = pltpu.make_async_copy(own[piece], place(piece, me), local_sem.at[piece])
        copy.start()
        local.append(copy)
        p[layer] = new
        copy = pltpu.make_async_copy(p.at[layer], p_out.at[layer], out_sem.at[piece])
        copy.start()
        local.append(copy)
    for piece in (2, 3):
        forward(own[piece], piece, me, near_x, 2)
    for piece in (0, 1):
        forward(own[piece], piece, me, near_y, 4)
    diag = near_x + near_y - me
    for k in range(2):
        spot = arrival(k, 2, near_x)
        forward(spot, k, near_x, near_y, 6)
        forward(spot, k, near_x, partner, 3)
        spot = arrival(2 + k, 4, near_y)
        forward(spot, 2 + k, near_y, near_x, 6)
        forward(spot, 2 + k, near_y, partner, 5)
    for k in range(2):
        spot = arrival(2 + k, 2, near_x)
        forward(spot, 2 + k, near_x, partner, 3)
        spot = arrival(k, 4, near_y)
        forward(spot, k, near_y, partner, 5)
    for k in range(2):
        for piece in (2 + k, k):
            spot = arrival(piece, 6, diag)
            forward(spot, piece, diag, partner, 7)
    for rel, owner in ((1, partner), (3, near_x + partner - me), (5, near_y + partner - me), (7, diag + partner - me)):
        for piece in range(4):
            arrival(piece, rel, owner)
    for copy in sends:
        copy.wait_send()
    for copy in local:
        copy.wait()


def update_and_gather(group_size, learn_rate, stats, u_up, u_down, p_up, p_down):
    up, down = p_up.shape, p_down.shape
    vmem = pl.BlockSpec(memory_space=pltpu.VMEM)
    hbm = pl.BlockSpec(memory_space=pl.ANY)
    return pl.pallas_call(
        functools.partial(update_kernel, group_size),
        out_shape=[
            pltpu.VMEM((up[0], up[1] * group_size, up[2]), jnp.bfloat16),
            pltpu.VMEM((down[0], down[1] * group_size, down[2]), jnp.bfloat16),
            jax.ShapeDtypeStruct(up, jnp.float32),
            jax.ShapeDtypeStruct(down, jnp.float32),
        ],
        in_specs=[pl.BlockSpec(memory_space=pltpu.SMEM), vmem] + [hbm] * 4,
        out_specs=[vmem] * 2 + [hbm] * 2,
        scratch_shapes=[
            pltpu.VMEM((group_size, 8, 128), jnp.float32),
            pltpu.VMEM(up, jnp.float32),
            pltpu.VMEM(down, jnp.float32),
            pltpu.VMEM(up, jnp.float32),
            pltpu.VMEM(down, jnp.float32),
            pltpu.VMEM(up, jnp.bfloat16),
            pltpu.VMEM(down, jnp.bfloat16),
            pltpu.SemaphoreType.DMA((group_size,)),
            pltpu.SemaphoreType.DMA((group_size,)),
            pltpu.SemaphoreType.DMA((32,)),
            pltpu.SemaphoreType.DMA((group_size, 4)),
            pltpu.SemaphoreType.DMA((4,)),
            pltpu.SemaphoreType.DMA((8,)),
            pltpu.SemaphoreType.DMA((4,)),
        ],
        compiler_params=pltpu.CompilerParams(collective_id=1, has_side_effects=True, vmem_limit_bytes=FULL_VMEM - 2 * group_size * (up[0] * up[1] * up[2] + down[0] * down[1] * down[2]) - 256 * 1024),
        name="update_and_gather",
    )(learn_rate.reshape(1), stats, u_up, u_down, p_up, p_down)


def solution(mesh):
    group_size = mesh.shape["data"]
    batch_rows = P("data", None)
    state_rows = P(None, "data", None)
    replicated = P()

    def device_step(act_in, grad_out, w_up, w_down, master_up, master_down, exp_avg_up, exp_avg_down, exp_sq_up, exp_sq_down, learn_rate, clip_norm):
        act_one, slope_one, hidden = forward_block(act_in, w_up, w_down)
        *grads, norm_tile = backward_blocks(group_size, act_in, grad_out, hidden, act_one, slope_one, w_up, w_down)
        grad_norm = jnp.sqrt(norm_tile[0, 0])
        avg_up, avg_down, sq_up, sq_down, dir_up, dir_down, stats = moments(clip_norm, norm_tile, grads, exp_avg_up, exp_avg_down, exp_sq_up, exp_sq_down)
        new_w_up, new_w_down, master_up_out, master_down_out = update_and_gather(group_size, learn_rate, stats, dir_up, dir_down, master_up, master_down)
        return (new_w_up, new_w_down, master_up_out, master_down_out, avg_up, avg_down, sq_up, sq_down, grad_norm)

    return jax.shard_map(device_step, mesh=mesh, in_specs=(batch_rows, batch_rows, replicated, replicated, state_rows, state_rows, state_rows, state_rows, state_rows, state_rows, replicated, replicated), out_specs=(replicated, replicated, state_rows, state_rows, state_rows, state_rows, state_rows, state_rows, replicated), check_vma=False)
```

```python
import functools

import jax
import jax.numpy as jnp
from jax import lax
from jax.experimental import pallas as pl
from jax.experimental.pallas import tpu as pltpu
from jax.sharding import PartitionSpec as P

STEP = 10
BETA_ONE = 0.9
BETA_TWO = 0.95
ADAM_EPS = 1e-8
NORM_EPS = 1e-6
INV_SQRT_TWO = 0.7071067811865476
INV_SQRT_TWO_PI = 0.3989422804014327


def gelu_parts(pre_act):
    normal_cdf = 0.5 * (1.0 + lax.erf(pre_act * INV_SQRT_TWO))
    normal_pdf = jnp.exp(-0.5 * pre_act * pre_act) * INV_SQRT_TWO_PI
    return pre_act * normal_cdf, normal_cdf + pre_act * normal_pdf


MESH = pl.DeviceIdType.MESH


def coords():
    me = lax.axis_index("data")
    core, col, row = me % 2, (me // 2) % 2, me // 4
    return me, me + 1 - 2 * core, me + 2 - 4 * col, me + 4 - 8 * row


def remote(src, dst, send_sem, recv_sem, device):
    return pltpu.make_async_remote_copy(src_ref=src, dst_ref=dst, send_sem=send_sem, recv_sem=recv_sem, device_id=(device,), device_id_type=MESH)


def meet_all(me, group_size):
    barrier = pltpu.get_barrier_semaphore()
    for step in range(1, group_size):
        pl.semaphore_signal(barrier, inc=1, device_id=((me + step) % group_size,), device_id_type=MESH)
    pl.semaphore_wait(barrier, group_size - 1)


def exchange_start(me, group_size, slots, send_sem, recv_sem):
    copies = []
    for step in range(1, group_size):
        copies.append(remote(slots.at[me], slots.at[me], send_sem.at[step], recv_sem.at[step], (me + step) % group_size))
        copies[-1].start()
    return copies


CHUNKS = 3
LANES = 128
TILE = 256
SLOTS = 4
OWNERS = tuple(chip * 2 + core for core in range(2) for chip in range(4))
FULL_VMEM = 67043328


def dot_nn(lhs, rhs):
    return jnp.dot(lhs, rhs, preferred_element_type=jnp.float32)


def dot_nt(lhs, rhs):
    return lax.dot_general(lhs, rhs, (((1,), (1,)), ((), ())), preferred_element_type=jnp.float32)


def dot_tn(lhs, rhs):
    return lax.dot_general(lhs, rhs, (((0,), (0,)), ((), ())), preferred_element_type=jnp.float32)


def chunk_blocks(chunk, width):
    return [owner * width + chunk * LANES for owner in OWNERS]


def forward_kernel(x_ref, w_up_ref, w_down_ref, a_out, s_out, h_out):
    x = x_ref[...]
    width = w_up_ref.shape[2] // len(OWNERS)
    total = None
    for chunk in range(CHUNKS):
        starts = chunk_blocks(chunk, width)
        w_in = jnp.concatenate([w_up_ref[0, :, s:s + LANES] for s in starts], axis=1)
        gelu, slope = gelu_parts(dot_nn(x, w_in))
        act = gelu.astype(jnp.bfloat16)
        a_out[chunk] = act
        s_out[chunk] = slope
        w_out = jnp.concatenate([w_down_ref[0, s:s + LANES, :] for s in starts], axis=0)
        part = dot_nn(act, w_out)
        total = part if total is None else total + part
    h_out[...] = total.astype(jnp.bfloat16)


def forward_block(act_in, w_up, w_down, tile=512):
    rows, dim = act_in.shape
    ff = w_up.shape[2]
    wide = ff // CHUNKS
    return pl.pallas_call(
        forward_kernel,
        grid=(rows // tile,),
        out_shape=[
            jax.ShapeDtypeStruct((CHUNKS, rows, wide), jnp.bfloat16),
            jax.ShapeDtypeStruct((CHUNKS, rows, wide), jnp.float32),
            jax.ShapeDtypeStruct((rows, dim), jnp.bfloat16),
        ],
        in_specs=[
            pl.BlockSpec((tile, dim), lambda i: (i, 0)),
            pl.BlockSpec((1, dim, ff), lambda i: (0, 0, 0)),
            pl.BlockSpec((1, ff, dim), lambda i: (0, 0, 0)),
        ],
        out_specs=[
            pl.BlockSpec((CHUNKS, tile, wide), lambda i: (0, i, 0)),
            pl.BlockSpec((CHUNKS, tile, wide), lambda i: (0, i, 0)),
            pl.BlockSpec((tile, dim), lambda i: (i, 0)),
        ],
        compiler_params=pltpu.CompilerParams(dimension_semantics=("arbitrary",), vmem_limit_bytes=FULL_VMEM),
        name="forward_block",
    )(act_in, w_up, w_down)


def backward_kernel(group_size, x_hbm, e_hbm, h_hbm, a_hbm, s_hbm, w_up_hbm, w_down_hbm,
                    g1_out, g2_out, g3_out, g4_out, norm_out, q_hbm,
                    h_v, e_v, wu_v, wd_v, a_v, q_v, s_v, t_d, t_u,
                    d0, d1a, d1b, d2a, d2b, u0, u1a, u1b, u2a, u2b,
                    sq_v, slots_v, load_sem, w_sem, q_sem, s_sem, send_sem, recv_sem, free_sem, stat_send, stat_recv):
    me, partner, near_x, near_y = coords()
    core, col, row = me % 2, (me // 2) % 2, me // 4
    rows, dim = h_v.shape
    half_rows = rows // 2
    wide = wu_v.shape[2]
    width = wide * CHUNKS // len(OWNERS)
    tiles = half_rows // TILE
    slots = s_v.shape[0]

    def at_rows(start, size):
        return pl.ds(pl.multiple_of(start, size), size)

    def half_copy(src, dst, half, sem):
        span = pl.ds(half * half_rows, half_rows)
        return pltpu.make_async_copy(src.at[span], dst.at[span], load_sem.at[sem, half])

    def start_weight(which, chunk, layer):
        for j, start in enumerate(chunk_blocks(chunk, width)):
            if which == 0:
                pltpu.make_async_copy(w_up_hbm.at[layer, :, pl.ds(start, LANES)], wu_v.at[chunk, :, pl.ds(j * LANES, LANES)], w_sem.at[0, chunk]).start()
            else:
                pltpu.make_async_copy(w_down_hbm.at[layer, pl.ds(start, LANES), :], wd_v.at[chunk, pl.ds(j * LANES, LANES), :], w_sem.at[1, chunk]).start()

    def wait_weight(which, chunk):
        ref = (wu_v, wd_v)[which]
        pltpu.make_async_copy(ref.at[chunk], ref.at[chunk], w_sem.at[which, chunk]).wait()

    half_copy(h_hbm, h_v, 0, 0).start()
    start_weight(0, 0, 1)
    half_copy(e_hbm, e_v, 0, 1).start()
    start_weight(1, 0, 1)
    sq_v[...] = jnp.zeros_like(sq_v)
    meet_all(me, group_size)

    def hop(src, dst, kind, chunk, stage, device):
        return remote(src, dst, send_sem.at[kind, chunk, stage], recv_sem.at[kind, chunk, stage], device)

    def hop0(kind, i):
        if kind == 0:
            return hop(t_d.at[:, 1 - core], d0.at[i], 0, i, 0, partner)
        return hop(t_u.at[:, :, :, 1 - core], u0.at[i], 1, i, 0, partner)

    def bufs(kind):
        return (d0, d1a, d1b, d2a, d2b) if kind == 0 else (u0, u1a, u1b, u2a, u2b)

    def hop1(kind, i):
        b0, b1a, b1b, _, _ = bufs(kind)
        return (hop(b0.at[i, 0, :, 1 - col], b1a.at[i], kind, i, 1, near_x),
                hop(b0.at[i, 1, 1 - row], b1b.at[i], kind, i, 2, near_y))

    def hop2(kind, i):
        _, b1a, b1b, b2a, b2b = bufs(kind)
        return (hop(b1a.at[i, 1 - row], b2a.at[i], kind, i, 3, near_y),
                hop(b1b.at[i, 1 - col], b2b.at[i], kind, i, 4, near_x))

    def rs0(kind, i):
        hop0(kind, i).start()

    def rs1(kind, i):
        hop0(kind, i).wait()
        b0 = bufs(kind)[0]
        for side in range(2):
            for y in range(2):
                for x in range(2):
                    own = t_d[side, core, y, x] if kind == 0 else t_u[side, y, x, core]
                    b0[i, side, y, x] = b0[i, side, y, x] + own
        for copy in hop1(kind, i):
            copy.start()

    def rs2(kind, i):
        b0, b1a, b1b, _, _ = bufs(kind)
        first, second = hop1(kind, i)
        out_a, out_b = hop2(kind, i)
        first.wait()
        for y in range(2):
            b1a[i, y] = b1a[i, y] + b0[i, 0, y, col]
        out_a.start()
        second.wait()
        for x in range(2):
            b1b[i, x] = b1b[i, x] + b0[i, 1, row, x]
        out_b.start()

    def rs3(kind, i, out):
        _, b1a, b1b, b2a, b2b = bufs(kind)
        cut = b1a.shape[3]
        for copy in hop2(kind, i):
            copy.wait()
        left = (b1a[i, row] + b2a[i]) / group_size
        right = (b1b[i, col] + b2b[i]) / group_size
        square = (left * left + right * right).reshape(left.shape[0] // 8, 8, cut).sum(axis=0)
        for lane in range(0, cut, LANES):
            sq_v[...] += square[:, lane:lane + LANES]
        if kind == 0:
            span = at_rows(i * LANES, LANES)
            out[span, 0:cut] = left
            out[span, cut:2 * cut] = right
        else:
            for j, owner in enumerate(OWNERS):
                part = (left, right)[j // 4]
                lane = (j % 4) * LANES
                out[:, pl.ds(pl.multiple_of(owner * width + i * LANES, LANES), LANES)] = part[:, lane:lane + LANES]

    def give_free(i):
        for device in (partner, near_x, near_y):
            pl.semaphore_signal(free_sem.at[i], inc=1, device_id=(device,), device_id_type=MESH)

    def grad_down(lhs_ref, rhs_ref, half):
        def part(m, carry):
            acc = dot_tn(lhs_ref[:, at_rows(m * (wide // 2), wide // 2)], rhs_ref[at_rows(half * half_rows, half_rows), :])
            cut = dim // 2
            for side in range(2):
                piece = acc[:, side * cut:(side + 1) * cut].reshape(t_d.shape[2:])
                t_d[side, m] = piece + jnp.where(half == 0, 0.0, t_d[side, m])
            return carry
        lax.fori_loop(0, 2, part, 0)

    def grad_up(lhs_ref, rhs_ref, half):
        def part(m, carry):
            acc = dot_tn(lhs_ref[at_rows(half * half_rows, half_rows), at_rows(m * (dim // 2), dim // 2)], rhs_ref[...])
            cut = wide // 2
            for side in range(2):
                piece = acc[:, side * cut:(side + 1) * cut].reshape(t_u.shape[2:])
                t_u[side, m] = piece + jnp.where(half == 0, 0.0, t_u[side, m])
            return carry
        lax.fori_loop(0, 2, part, 0)

    def q_copy(i, half):
        return pltpu.make_async_copy(q_v, q_hbm.at[i, at_rows(half * half_rows, half_rows), :], q_sem.at[0])

    def second_chunk(i, carry):
        wait_weight(0, i)
        wait_weight(1, i)

        @pl.when(i == 0)
        def _():
            half_copy(h_hbm, h_v, 0, 0).wait()
            half_copy(e_hbm, e_v, 0, 1).wait()
            half_copy(h_hbm, h_v, 1, 0).start()
            half_copy(e_hbm, e_v, 1, 1).start()
            for chunk in range(1, CHUNKS):
                start_weight(0, chunk, 1)
                start_weight(1, chunk, 1)

        def second_half(half, carry):
            @pl.when((i == 0) & (half == 1))
            def _():
                half_copy(h_hbm, h_v, 1, 0).wait()
                half_copy(e_hbm, e_v, 1, 1).wait()

            @pl.when((i > 0) | (half > 0))
            def _():
                q_copy(i, half).wait()

            def second_tile(t, carry):
                span = at_rows(half * half_rows + t * TILE, TILE)
                z = dot_nn(h_v[span, :], wu_v[i])
                p = dot_nt(e_v[span, :], wd_v[i])
                gelu, slope = gelu_parts(z)
                here = at_rows(t * TILE, TILE)
                a_v[here, :] = gelu.astype(jnp.bfloat16)
                q_v[here, :] = (p * slope).astype(jnp.bfloat16)

                @pl.when((half == 0) & (i > 1))
                def _():
                    @pl.when(t == 0)
                    def _():
                        rs2(1, i - 2)

                    @pl.when(t == 2)
                    def _():
                        rs3(0, i - 2, g4_out)

                @pl.when((t == tiles // 2) & (half == 0) & (i > 0))
                def _():
                    rs1(0, i - 1)

                @pl.when((t == 3) & (half == 1) & (i > 0))
                def _():
                    rs2(0, i - 1)
                return carry

            lax.fori_loop(0, tiles, second_tile, 0)
            q_copy(i, half).start()

            @pl.when((half == 0) & (i > 1))
            def _():
                rs3(1, i - 2, g3_out)
                give_free(i - 2)

            grad_down(a_v, e_v, half)

            @pl.when(half == 1)
            def _():
                rs0(0, i)

            @pl.when((half == 0) & (i > 0))
            def _():
                rs1(1, i - 1)

            grad_up(h_v, q_v, half)

            @pl.when(half == 1)
            def _():
                rs0(1, i)
            return carry

        lax.fori_loop(0, 2, second_half, 0)
        return carry

    lax.fori_loop(0, CHUNKS, second_chunk, 0)

    q_copy(CHUNKS - 1, 1).wait()
    for half in range(2):
        half_copy(x_hbm, e_v, half, 1).start()
    for chunk in range(CHUNKS):
        start_weight(1, chunk, 0)
    r_rows = half_rows // 4
    staging = (a_v, q_v)

    def r_load(slot, t):
        for k in range(CHUNKS):
            pltpu.make_async_copy(q_hbm.at[k, at_rows(t * r_rows, r_rows), :], staging[slot].at[pl.ds(k * r_rows, r_rows), :], load_sem.at[2, slot]).start()

    def a_load(i, half):
        return pltpu.make_async_copy(a_hbm.at[i, pl.ds(half * half_rows, half_rows), :], staging[half], load_sem.at[0, half])

    for slot in range(2):
        r_load(slot, slot)
    r_steps = rows // r_rows // 2

    def r_pair(t, carry):
        for slot in range(2):
            whole = staging[slot].at[pl.ds(0, CHUNKS * r_rows), :]
            pltpu.make_async_copy(whole, whole, load_sem.at[2, slot]).wait()
            for part in range(2):
                m = part * (r_rows // 2)
                acc = dot_nt(staging[slot][m:m + r_rows // 2, :], wu_v[0])
                for k in range(1, CHUNKS):
                    acc = acc + dot_nt(staging[slot][k * r_rows + m:k * r_rows + m + r_rows // 2, :], wu_v[k])
                h_v[at_rows((2 * t + slot) * r_rows + m, r_rows // 2), :] = acc.astype(jnp.bfloat16)

            @pl.when(t < r_steps - 1)
            def _():
                r_load(slot, 2 * t + 2 + slot)

        @pl.when(t == 0)
        def _():
            rs1(0, CHUNKS - 1)
            rs3(0, CHUNKS - 2, g4_out)

        @pl.when(t == 1)
        def _():
            rs1(1, CHUNKS - 1)
            rs3(1, CHUNKS - 2, g3_out)
            give_free(CHUNKS - 2)
        return carry

    rs2(1, CHUNKS - 2)
    lax.fori_loop(0, r_steps, r_pair, 0)
    for half in range(2):
        a_load(0, half).start()

    def s_load(i, t):
        slot = lax.rem(t, slots)
        return pltpu.make_async_copy(s_hbm.at[i, at_rows(t * TILE, TILE), :], s_v.at[slot], s_sem.at[slot])

    for t in range(slots):
        s_load(0, t).start()
    rs2(0, CHUNKS - 1)

    def first_chunk(i, carry):
        a_load(i, 0).wait()
        grad_down(a_v, h_v, 0)

        @pl.when(i < CHUNKS - 1)
        def _():
            a_load(i + 1, 0).start()

        @pl.when(i == 2)
        def _():
            rs2(1, 0)

        a_load(i, 1).wait()
        grad_down(q_v, h_v, 1)
        pl.semaphore_wait(free_sem.at[i], 3)
        rs0(0, i)
        wait_weight(1, i)

        @pl.when(i == 0)
        def _():
            for half in range(2):
                half_copy(x_hbm, e_v, half, 1).wait()

        def first_half(half, carry):
            def first_tile(t, carry):
                tt = half * tiles + t
                s_load(i, tt).wait()
                p = dot_nt(h_v[at_rows(tt * TILE, TILE), :], wd_v[i])
                q_v[at_rows(t * TILE, TILE), :] = (p * s_v[lax.rem(tt, slots)]).astype(jnp.bfloat16)

                ahead = tt + slots
                @pl.when(ahead < 2 * tiles)
                def _():
                    s_load(i, ahead).start()

                @pl.when((tt == 6) & (i == 0))
                def _():
                    rs3(0, 2, g4_out)

                @pl.when((tt == tiles + 3) & (i == 2))
                def _():
                    rs3(1, 0, g1_out)
                return carry

            @pl.when(half == 0)
            def _():
                @pl.when(i == 0)
                def _():
                    rs2(1, 2)

                @pl.when(i == 1)
                def _():
                    rs2(0, 0)

                @pl.when(i > 0)
                def _():
                    rs1(1, i - 1)

            @pl.when(half == 1)
            def _():
                @pl.when(i == 2)
                def _():
                    rs2(0, 1)

                rs1(0, i)

                @pl.when(i == 0)
                def _():
                    rs3(1, 2, g3_out)
                    give_free(2)

                @pl.when(i == 1)
                def _():
                    rs3(0, 0, g2_out)

            lax.fori_loop(0, tiles, first_tile, 0)

            @pl.when((half == 1) & (i < CHUNKS - 1))
            def _():
                for t in range(slots):
                    s_load(i + 1, t).start()

            grad_up(e_v, q_v, half)
            return carry

        lax.fori_loop(0, 2, first_half, 0)
        rs0(1, i)

        @pl.when(i < CHUNKS - 1)
        def _():
            a_load(i + 1, 1).start()
        return carry

    lax.fori_loop(0, CHUNKS, first_chunk, 0)
    rs2(1, 1)
    rs1(1, 2)
    rs3(0, 1, g2_out)
    rs2(0, 2)
    rs3(1, 1, g1_out)
    rs2(1, 2)
    rs3(0, 2, g2_out)
    rs3(1, 2, g1_out)
    slots_v[me] = sq_v[...]
    for copy in exchange_start(me, group_size, slots_v, stat_send, stat_recv):
        copy.wait()
    total = slots_v[0]
    for index in range(1, group_size):
        total = total + slots_v[index]
    norm_out[...] = jnp.full(norm_out.shape, jnp.sum(total))


def backward_blocks(group_size, act_in, grad_out, hidden, act_one, slope_one, w_up, w_down):
    rows, dim = act_in.shape
    ff = w_up.shape[2]
    wide = ff // CHUNKS
    up_rows, down_rows = dim // group_size, LANES
    hbm = pl.BlockSpec(memory_space=pl.ANY)
    vmem = pl.BlockSpec(memory_space=pltpu.VMEM)
    f32 = jnp.float32
    bf16 = jnp.bfloat16
    up_grad = jax.ShapeDtypeStruct((up_rows, ff), f32)
    down_grad = jax.ShapeDtypeStruct((ff // group_size, dim), f32)

    def stages(height, cols):
        return [
            pltpu.VMEM((CHUNKS, 2, 2, 2, height, cols // 2), f32),
            pltpu.VMEM((CHUNKS, 2, height, cols // 2), f32),
            pltpu.VMEM((CHUNKS, 2, height, cols // 2), f32),
            pltpu.VMEM((CHUNKS, height, cols // 2), f32),
            pltpu.VMEM((CHUNKS, height, cols // 2), f32),
        ]

    return pl.pallas_call(
        functools.partial(backward_kernel, group_size),
        out_shape=[up_grad, down_grad, up_grad, down_grad, jax.ShapeDtypeStruct((8, 128), f32), jax.ShapeDtypeStruct((CHUNKS, rows, wide), bf16)],
        in_specs=[hbm] * 7,
        out_specs=[vmem] * 5 + [hbm],
        scratch_shapes=[
            pltpu.VMEM((rows, dim), bf16),
            pltpu.VMEM((rows, dim), bf16),
            pltpu.VMEM((CHUNKS, dim, wide), bf16),
            pltpu.VMEM((CHUNKS, wide, dim), bf16),
            pltpu.VMEM((rows // 2, wide), bf16),
            pltpu.VMEM((rows // 2, wide), bf16),
            pltpu.VMEM((SLOTS, TILE, wide), f32),
            pltpu.VMEM((2, 2, 2, 2, down_rows, dim // 2), f32),
            pltpu.VMEM((2, 2, 2, 2, up_rows, wide // 2), f32),
            *stages(down_rows, dim),
            *stages(up_rows, wide),
            pltpu.VMEM((8, 128), f32),
            pltpu.VMEM((group_size, 8, 128), f32),
            pltpu.SemaphoreType.DMA((3, 2)),
            pltpu.SemaphoreType.DMA((2, CHUNKS)),
            pltpu.SemaphoreType.DMA((1,)),
            pltpu.SemaphoreType.DMA((SLOTS,)),
            pltpu.SemaphoreType.DMA((2, CHUNKS, 5)),
            pltpu.SemaphoreType.DMA((2, CHUNKS, 5)),
            pltpu.SemaphoreType.REGULAR((CHUNKS,)),
            pltpu.SemaphoreType.DMA((group_size,)),
            pltpu.SemaphoreType.DMA((group_size,)),
        ],
        compiler_params=pltpu.CompilerParams(collective_id=2, has_side_effects=True, vmem_limit_bytes=FULL_VMEM),
        name="backward_blocks",
    )(act_in, grad_out, hidden, act_one, slope_one, w_up, w_down)[:5]


def moments_kernel(clip_ref, norm_ref, g_one, g_two, g_three, g_four, m_up, m_down, v_up, v_down, m_up_out, m_down_out, v_up_out, v_down_out, u_up, u_down, stats):
    inv_one = 1.0 / (1.0 - BETA_ONE ** STEP)
    inv_two = 1.0 / (1.0 - BETA_TWO ** STEP)
    scale = jnp.minimum(1.0, clip_ref[0] / (jnp.sqrt(norm_ref[0:1, 0:1]) + NORM_EPS))
    row_id = lax.broadcasted_iota(jnp.int32, (8, 128), 0)
    sums = jnp.zeros((8, 128), jnp.float32)
    for family, (grads, m, v, m_out, v_out, u) in enumerate([((g_one, g_three), m_up, v_up, m_up_out, v_up_out, u_up), ((g_two, g_four), m_down, v_down, m_down_out, v_down_out, u_down)]):
        for layer in range(2):
            grad = grads[layer][...]
            avg_new = BETA_ONE * m[layer] + (1.0 - BETA_ONE) * scale * grad
            sq_new = BETA_TWO * v[layer] + (1.0 - BETA_TWO) * (scale * scale) * (grad * grad)
            direction = (avg_new * inv_one) / (jnp.sqrt(sq_new * inv_two) + ADAM_EPS)
            m_out[layer] = avg_new
            v_out[layer] = sq_new
            u[layer] = direction
            sums = sums + jnp.where(row_id == 4 + 2 * family + layer, jnp.sum(direction * direction), 0.0)

    @pl.when(pl.program_id(0) == 0)
    def _():
        stats[...] = jnp.zeros_like(stats)

    stats[...] += sums


def moments(clip_norm, norm_tile, grads, m_up, m_down, v_up, v_down, steps=4):
    up, down = m_up.shape, m_down.shape
    up_spec = pl.BlockSpec((2, up[1] // steps, up[2]), lambda i: (0, i, 0))
    down_spec = pl.BlockSpec((2, down[1] // steps, down[2]), lambda i: (0, i, 0))
    up_grad = pl.BlockSpec((up[1] // steps, up[2]), lambda i: (i, 0))
    down_grad = pl.BlockSpec((down[1] // steps, down[2]), lambda i: (i, 0))
    tile = pl.BlockSpec((8, 128), lambda i: (0, 0))
    pair = [up_spec, down_spec]
    up_shape, down_shape = jax.ShapeDtypeStruct(up, jnp.float32), jax.ShapeDtypeStruct(down, jnp.float32)
    return pl.pallas_call(
        moments_kernel,
        grid=(steps,),
        out_shape=[up_shape, down_shape] * 3 + [jax.ShapeDtypeStruct((8, 128), jnp.float32)],
        in_specs=[pl.BlockSpec(memory_space=pltpu.SMEM), tile] + [up_grad, down_grad] * 2 + pair * 2,
        out_specs=pair * 3 + [tile],
        compiler_params=pltpu.CompilerParams(dimension_semantics=("arbitrary",), vmem_limit_bytes=FULL_VMEM),
        name="moments",
    )(clip_norm.reshape(1), norm_tile, *grads, m_up, m_down, v_up, v_down)


PIECES = ((0, 0), (0, 1), (1, 0), (1, 1))


def update_kernel(group_size, rate_ref, stats_ref, u_up_hbm, u_down_hbm, p_up_hbm, p_down_hbm, all_up, all_down, p_up_out, p_down_out,
                  slots, u_up, u_down, p_up, p_down, w_up, w_down, stat_send, stat_recv, send_sem, recv_sem, local_sem, in_sem, out_sem):
    me, partner, near_x, near_y = coords()
    loads = []
    for src, dst in ((p_up_hbm, p_up), (p_down_hbm, p_down), (u_up_hbm, u_up), (u_down_hbm, u_down)):
        for layer in range(2):
            copy = pltpu.make_async_copy(src.at[layer], dst.at[layer], in_sem.at[len(loads)])
            copy.start()
            loads.append(copy)
    meet_all(me, group_size)
    row_id = lax.broadcasted_iota(jnp.int32, (8, 128), 0)
    stats = stats_ref[...]
    for index in range(4):
        loads[index].wait()
        master = (p_up, p_down)[index // 2][index % 2]
        stats = stats + jnp.where(row_id == index, jnp.sum(master * master), 0.0)
    slots[me] = stats
    for copy in exchange_start(me, group_size, slots, stat_send, stat_recv):
        copy.wait()
    total = slots[0]
    for index in range(1, group_size):
        total = total + slots[index]
    ratio = jnp.sqrt(total[0:4]) / jnp.sqrt(total[4:8])
    rate = rate_ref[0]
    params = ((u_up, p_up, p_up_out, w_up, all_up), (u_down, p_down, p_down_out, w_down, all_down))

    def place(piece, owner):
        family, layer = PIECES[piece]
        full = params[family][4]
        rows = params[family][3].shape[1]
        return full.at[layer, pl.ds(pl.multiple_of(owner * rows, rows), rows), :]

    sends = []
    count = [0]

    def forward(src, piece, owner, device, rel):
        copy = remote(src, place(piece, owner), send_sem.at[count[0]], recv_sem.at[rel, piece], device)
        count[0] += 1
        copy.start()
        sends.append(copy)

    def arrival(piece, rel, owner):
        spot = place(piece, owner)
        remote(spot, spot, send_sem.at[0], recv_sem.at[rel, piece], me).wait_recv()
        return spot

    own = {}
    local = []
    for piece in (0, 2, 1, 3):
        family, layer = PIECES[piece]
        u, p, p_out, w, full = params[family]
        index = 2 * family + layer
        loads[4 + index].wait()
        new = p[layer] - rate * ratio[index:index + 1, 0:1] * u[layer]
        w[layer] = new.astype(jnp.bfloat16)
        own[piece] = w.at[layer]
        if family == 0:
            forward(own[piece], piece, me, near_x, 2)
        else:
            forward(own[piece], piece, me, near_y, 4)
        forward(own[piece], piece, me, partner, 1)
        copy = pltpu.make_async_copy(own[piece], place(piece, me), local_sem.at[piece])
        copy.start()
        local.append(copy)
        p[layer] = new
        copy = pltpu.make_async_copy(p.at[layer], p_out.at[layer], out_sem.at[piece])
        copy.start()
        local.append(copy)
    for piece in (2, 3):
        forward(own[piece], piece, me, near_x, 2)
    for piece in (0, 1):
        forward(own[piece], piece, me, near_y, 4)
    diag = near_x + near_y - me
    for k in range(2):
        spot = arrival(k, 2, near_x)
        forward(spot, k, near_x, near_y, 6)
        forward(spot, k, near_x, partner, 3)
        spot = arrival(2 + k, 4, near_y)
        forward(spot, 2 + k, near_y, near_x, 6)
        forward(spot, 2 + k, near_y, partner, 5)
    for k in range(2):
        spot = arrival(2 + k, 2, near_x)
        forward(spot, 2 + k, near_x, partner, 3)
        spot = arrival(k, 4, near_y)
        forward(spot, k, near_y, partner, 5)
    for k in range(2):
        for piece in (2 + k, k):
            spot = arrival(piece, 6, diag)
            forward(spot, piece, diag, partner, 7)
    for rel, owner in ((1, partner), (3, near_x + partner - me), (5, near_y + partner - me), (7, diag + partner - me)):
        for piece in range(4):
            arrival(piece, rel, owner)
    for copy in sends:
        copy.wait_send()
    for copy in local:
        copy.wait()


def update_and_gather(group_size, learn_rate, stats, u_up, u_down, p_up, p_down):
    up, down = p_up.shape, p_down.shape
    vmem = pl.BlockSpec(memory_space=pltpu.VMEM)
    hbm = pl.BlockSpec(memory_space=pl.ANY)
    return pl.pallas_call(
        functools.partial(update_kernel, group_size),
        out_shape=[
            pltpu.VMEM((up[0], up[1] * group_size, up[2]), jnp.bfloat16),
            pltpu.VMEM((down[0], down[1] * group_size, down[2]), jnp.bfloat16),
            jax.ShapeDtypeStruct(up, jnp.float32),
            jax.ShapeDtypeStruct(down, jnp.float32),
        ],
        in_specs=[pl.BlockSpec(memory_space=pltpu.SMEM), vmem] + [hbm] * 4,
        out_specs=[vmem] * 2 + [hbm] * 2,
        scratch_shapes=[
            pltpu.VMEM((group_size, 8, 128), jnp.float32),
            pltpu.VMEM(up, jnp.float32),
            pltpu.VMEM(down, jnp.float32),
            pltpu.VMEM(up, jnp.float32),
            pltpu.VMEM(down, jnp.float32),
            pltpu.VMEM(up, jnp.bfloat16),
            pltpu.VMEM(down, jnp.bfloat16),
            pltpu.SemaphoreType.DMA((group_size,)),
            pltpu.SemaphoreType.DMA((group_size,)),
            pltpu.SemaphoreType.DMA((32,)),
            pltpu.SemaphoreType.DMA((group_size, 4)),
            pltpu.SemaphoreType.DMA((4,)),
            pltpu.SemaphoreType.DMA((8,)),
            pltpu.SemaphoreType.DMA((4,)),
        ],
        compiler_params=pltpu.CompilerParams(collective_id=1, has_side_effects=True, vmem_limit_bytes=FULL_VMEM - 2 * group_size * (up[0] * up[1] * up[2] + down[0] * down[1] * down[2]) - 256 * 1024),
        name="update_and_gather",
    )(learn_rate.reshape(1), stats, u_up, u_down, p_up, p_down)


def solution(mesh):
    group_size = mesh.shape["data"]
    batch_rows = P("data", None)
    state_rows = P(None, "data", None)
    replicated = P()

    def device_step(act_in, grad_out, w_up, w_down, master_up, master_down, exp_avg_up, exp_avg_down, exp_sq_up, exp_sq_down, learn_rate, clip_norm):
        act_one, slope_one, hidden = forward_block(act_in, w_up, w_down)
        *grads, norm_tile = backward_blocks(group_size, act_in, grad_out, hidden, act_one, slope_one, w_up, w_down)
        grad_norm = jnp.sqrt(norm_tile[0, 0])
        avg_up, avg_down, sq_up, sq_down, dir_up, dir_down, stats = moments(clip_norm, norm_tile, grads, exp_avg_up, exp_avg_down, exp_sq_up, exp_sq_down)
        new_w_up, new_w_down, master_up_out, master_down_out = update_and_gather(group_size, learn_rate, stats, dir_up, dir_down, master_up, master_down)
        return (new_w_up, new_w_down, master_up_out, master_down_out, avg_up, avg_down, sq_up, sq_down, grad_norm)

    return jax.shard_map(device_step, mesh=mesh, in_specs=(batch_rows, batch_rows, replicated, replicated, state_rows, state_rows, state_rows, state_rows, state_rows, state_rows, replicated, replicated), out_specs=(replicated, replicated, state_rows, state_rows, state_rows, state_rows, state_rows, state_rows, replicated), check_vma=False)
```

```python
import functools

import jax
import jax.numpy as jnp
from jax import lax
from jax.experimental import pallas as pl
from jax.experimental.pallas import tpu as pltpu
from jax.sharding import PartitionSpec as P

STEP = 10
BETA_ONE = 0.9
BETA_TWO = 0.95
ADAM_EPS = 1e-8
NORM_EPS = 1e-6
INV_SQRT_TWO = 0.7071067811865476
INV_SQRT_TWO_PI = 0.3989422804014327


def gelu_parts(pre_act):
    normal_cdf = 0.5 * (1.0 + lax.erf(pre_act * INV_SQRT_TWO))
    normal_pdf = jnp.exp(-0.5 * pre_act * pre_act) * INV_SQRT_TWO_PI
    return pre_act * normal_cdf, normal_cdf + pre_act * normal_pdf


MESH = pl.DeviceIdType.MESH


def coords():
    me = lax.axis_index("data")
    core, col, row = me % 2, (me // 2) % 2, me // 4
    return me, me + 1 - 2 * core, me + 2 - 4 * col, me + 4 - 8 * row


def remote(src, dst, send_sem, recv_sem, device):
    return pltpu.make_async_remote_copy(src_ref=src, dst_ref=dst, send_sem=send_sem, recv_sem=recv_sem, device_id=(device,), device_id_type=MESH)


def meet_all(me, group_size):
    barrier = pltpu.get_barrier_semaphore()
    for step in range(1, group_size):
        pl.semaphore_signal(barrier, inc=1, device_id=((me + step) % group_size,), device_id_type=MESH)
    pl.semaphore_wait(barrier, group_size - 1)


def exchange_start(me, group_size, slots, send_sem, recv_sem):
    copies = []
    for step in range(1, group_size):
        copies.append(remote(slots.at[me], slots.at[me], send_sem.at[step], recv_sem.at[step], (me + step) % group_size))
        copies[-1].start()
    return copies


CHUNKS = 3
LANES = 128
TILE = 256
SLOTS = 4
OWNERS = tuple(chip * 2 + core for core in range(2) for chip in range(4))
FULL_VMEM = 67043328


def dot_nn(lhs, rhs):
    return jnp.dot(lhs, rhs, preferred_element_type=jnp.float32)


def dot_nt(lhs, rhs):
    return lax.dot_general(lhs, rhs, (((1,), (1,)), ((), ())), preferred_element_type=jnp.float32)


def dot_tn(lhs, rhs):
    return lax.dot_general(lhs, rhs, (((0,), (0,)), ((), ())), preferred_element_type=jnp.float32)


def chunk_blocks(chunk, width):
    return [owner * width + chunk * LANES for owner in OWNERS]


def forward_kernel(x_ref, w_up_ref, w_down_ref, up_block, down_block_one, down_block_two, a_out, s_out, h_out, down_t_one, down_t_two, up_t):
    for block, out in ((down_block_one, down_t_one), (down_block_two, down_t_two)):
        for chunk in range(CHUNKS):
            out[chunk] = block[0, chunk * LANES:(chunk + 1) * LANES, :].T
    for chunk in range(CHUNKS):
        up_t[chunk, 0] = up_block[0, :, chunk * LANES:(chunk + 1) * LANES].T
    x = x_ref[...]
    width = w_up_ref.shape[2] // len(OWNERS)
    total = None
    for chunk in range(CHUNKS):
        starts = chunk_blocks(chunk, width)
        w_in = jnp.concatenate([w_up_ref[0, :, s:s + LANES] for s in starts], axis=1)
        gelu, slope = gelu_parts(dot_nn(x, w_in))
        act = gelu.astype(jnp.bfloat16)
        a_out[chunk] = act
        s_out[chunk] = slope
        w_out = jnp.concatenate([w_down_ref[0, s:s + LANES, :] for s in starts], axis=0)
        part = dot_nn(act, w_out)
        total = part if total is None else total + part
    h_out[...] = total.astype(jnp.bfloat16)


def forward_block(act_in, w_up, w_down, tile=512):
    rows, dim = act_in.shape
    ff = w_up.shape[2]
    wide = ff // CHUNKS
    owners = len(OWNERS)
    width = ff // owners
    assert rows // tile == owners

    def slot(i):
        return (i % 2) * (owners // 2) + i // 2

    return pl.pallas_call(
        forward_kernel,
        grid=(rows // tile,),
        out_shape=[
            jax.ShapeDtypeStruct((CHUNKS, rows, wide), jnp.bfloat16),
            jax.ShapeDtypeStruct((CHUNKS, rows, wide), jnp.float32),
            jax.ShapeDtypeStruct((rows, dim), jnp.bfloat16),
            jax.ShapeDtypeStruct((CHUNKS, dim, wide), jnp.bfloat16),
            jax.ShapeDtypeStruct((CHUNKS, dim, wide), jnp.bfloat16),
            jax.ShapeDtypeStruct((CHUNKS, owners, LANES, dim), jnp.bfloat16),
        ],
        in_specs=[
            pl.BlockSpec((tile, dim), lambda i: (i, 0)),
            pl.BlockSpec((1, dim, ff), lambda i: (0, 0, 0)),
            pl.BlockSpec((1, ff, dim), lambda i: (0, 0, 0)),
            pl.BlockSpec((1, dim, width), lambda i: (1, 0, i)),
            pl.BlockSpec((1, width, dim), lambda i: (0, i, 0)),
            pl.BlockSpec((1, width, dim), lambda i: (1, i, 0)),
        ],
        out_specs=[
            pl.BlockSpec((CHUNKS, tile, wide), lambda i: (0, i, 0)),
            pl.BlockSpec((CHUNKS, tile, wide), lambda i: (0, i, 0)),
            pl.BlockSpec((tile, dim), lambda i: (i, 0)),
            pl.BlockSpec((CHUNKS, dim, LANES), lambda i: (0, 0, slot(i))),
            pl.BlockSpec((CHUNKS, dim, LANES), lambda i: (0, 0, slot(i))),
            pl.BlockSpec((CHUNKS, 1, LANES, dim), lambda i: (0, slot(i), 0, 0)),
        ],
        compiler_params=pltpu.CompilerParams(dimension_semantics=("arbitrary",), vmem_limit_bytes=FULL_VMEM),
        name="forward_block",
    )(act_in, w_up, w_down, w_up, w_down, w_down)


def backward_kernel(group_size, x_hbm, e_hbm, h_hbm, a_hbm, s_hbm, w_up_hbm, down_t_one, down_t_two, up_t,
                    g1_out, g2_out, g3_out, g4_out, norm_out, q_hbm,
                    h_v, e_v, wu_v, wd_v, a_v, q_v, s_v, t_d, t_u,
                    d0, d1a, d1b, d2a, d2b, u0, u1a, u1b, u2a, u2b,
                    sq_v, slots_v, load_sem, w_sem, q_sem, s_sem, send_sem, recv_sem, free_sem, stat_send, stat_recv):
    me, partner, near_x, near_y = coords()
    core, col, row = me % 2, (me // 2) % 2, me // 4
    rows, dim = h_v.shape
    half_rows = rows // 2
    wide = wu_v.shape[2]
    width = wide * CHUNKS // len(OWNERS)
    tiles = half_rows // TILE
    slots = s_v.shape[0]

    def at_rows(start, size):
        return pl.ds(pl.multiple_of(start, size), size)

    def half_copy(src, dst, half, sem):
        span = pl.ds(half * half_rows, half_rows)
        return pltpu.make_async_copy(src.at[span], dst.at[span], load_sem.at[sem, half])

    def start_up(chunk):
        for j, start in enumerate(chunk_blocks(chunk, width)):
            pltpu.make_async_copy(w_up_hbm.at[1, :, pl.ds(start, LANES)], wu_v.at[chunk, :, pl.ds(j * LANES, LANES)], w_sem.at[0, chunk]).start()

    def start_down(src, chunk):
        pltpu.make_async_copy(src.at[chunk], wd_v.at[chunk], w_sem.at[1, chunk]).start()

    def up_t_copy(part):
        span = (pl.ds(0, half_rows), pl.ds(half_rows, CHUNKS * wide - half_rows))[part]
        return pltpu.make_async_copy(up_t.at[span], e_v.at[span], load_sem.at[1, part])

    def wait_weight(which, chunk):
        ref = (wu_v, wd_v)[which]
        pltpu.make_async_copy(ref.at[chunk], ref.at[chunk], w_sem.at[which, chunk]).wait()

    half_copy(h_hbm, h_v, 0, 0).start()
    start_up(0)
    half_copy(e_hbm, e_v, 0, 1).start()
    start_down(down_t_two, 0)
    sq_v[...] = jnp.zeros_like(sq_v)
    meet_all(me, group_size)

    def hop(src, dst, kind, chunk, stage, device):
        return remote(src, dst, send_sem.at[kind, chunk, stage], recv_sem.at[kind, chunk, stage], device)

    def hop0(kind, i):
        if kind == 0:
            return hop(t_d.at[:, 1 - core], d0.at[i], 0, i, 0, partner)
        return hop(t_u.at[:, :, :, 1 - core], u0.at[i], 1, i, 0, partner)

    def bufs(kind):
        return (d0, d1a, d1b, d2a, d2b) if kind == 0 else (u0, u1a, u1b, u2a, u2b)

    def hop1(kind, i):
        b0, b1a, b1b, _, _ = bufs(kind)
        return (hop(b0.at[i, 0, :, 1 - col], b1a.at[i], kind, i, 1, near_x),
                hop(b0.at[i, 1, 1 - row], b1b.at[i], kind, i, 2, near_y))

    def hop2(kind, i):
        _, b1a, b1b, b2a, b2b = bufs(kind)
        return (hop(b1a.at[i, 1 - row], b2a.at[i], kind, i, 3, near_y),
                hop(b1b.at[i, 1 - col], b2b.at[i], kind, i, 4, near_x))

    def rs0(kind, i):
        hop0(kind, i).start()

    def rs1(kind, i):
        hop0(kind, i).wait()
        b0 = bufs(kind)[0]
        for side in range(2):
            for y in range(2):
                for x in range(2):
                    own = t_d[side, core, y, x] if kind == 0 else t_u[side, y, x, core]
                    b0[i, side, y, x] = b0[i, side, y, x] + own
        for copy in hop1(kind, i):
            copy.start()

    def rs2(kind, i):
        b0, b1a, b1b, _, _ = bufs(kind)
        first, second = hop1(kind, i)
        out_a, out_b = hop2(kind, i)
        first.wait()
        for y in range(2):
            b1a[i, y] = b1a[i, y] + b0[i, 0, y, col]
        out_a.start()
        second.wait()
        for x in range(2):
            b1b[i, x] = b1b[i, x] + b0[i, 1, row, x]
        out_b.start()

    def rs3(kind, i, out):
        _, b1a, b1b, b2a, b2b = bufs(kind)
        cut = b1a.shape[3]
        for copy in hop2(kind, i):
            copy.wait()
        left = (b1a[i, row] + b2a[i]) / group_size
        right = (b1b[i, col] + b2b[i]) / group_size
        square = (left * left + right * right).reshape(left.shape[0] // 8, 8, cut).sum(axis=0)
        for lane in range(0, cut, LANES):
            sq_v[...] += square[:, lane:lane + LANES]
        if kind == 0:
            span = at_rows(i * LANES, LANES)
            out[span, 0:cut] = left
            out[span, cut:2 * cut] = right
        else:
            for j, owner in enumerate(OWNERS):
                part = (left, right)[j // 4]
                lane = (j % 4) * LANES
                out[:, pl.ds(pl.multiple_of(owner * width + i * LANES, LANES), LANES)] = part[:, lane:lane + LANES]

    def give_free(i):
        for device in (partner, near_x, near_y):
            pl.semaphore_signal(free_sem.at[i], inc=1, device_id=(device,), device_id_type=MESH)

    def grad_down(lhs_ref, rhs_ref, half):
        def part(m, carry):
            acc = dot_tn(lhs_ref[:, at_rows(m * (wide // 2), wide // 2)], rhs_ref[at_rows(half * half_rows, half_rows), :])
            cut = dim // 2
            for side in range(2):
                piece = acc[:, side * cut:(side + 1) * cut].reshape(t_d.shape[2:])
                t_d[side, m] = piece + jnp.where(half == 0, 0.0, t_d[side, m])
            return carry
        lax.fori_loop(0, 2, part, 0)

    def grad_up(lhs_ref, rhs_ref, half):
        def part(m, carry):
            acc = dot_tn(lhs_ref[at_rows(half * half_rows, half_rows), at_rows(m * (dim // 2), dim // 2)], rhs_ref[...])
            cut = wide // 2
            for side in range(2):
                piece = acc[:, side * cut:(side + 1) * cut].reshape(t_u.shape[2:])
                t_u[side, m] = piece + jnp.where(half == 0, 0.0, t_u[side, m])
            return carry
        lax.fori_loop(0, 2, part, 0)

    def q_copy(i, half):
        return pltpu.make_async_copy(q_v, q_hbm.at[i, at_rows(half * half_rows, half_rows), :], q_sem.at[0])

    def second_chunk(i, carry):
        wait_weight(0, i)
        wait_weight(1, i)

        @pl.when(i == 0)
        def _():
            half_copy(h_hbm, h_v, 0, 0).wait()
            half_copy(e_hbm, e_v, 0, 1).wait()
            half_copy(h_hbm, h_v, 1, 0).start()
            half_copy(e_hbm, e_v, 1, 1).start()
            for chunk in range(1, CHUNKS):
                start_up(chunk)
                start_down(down_t_two, chunk)

        def second_half(half, carry):
            @pl.when((i == 0) & (half == 1))
            def _():
                half_copy(h_hbm, h_v, 1, 0).wait()
                half_copy(e_hbm, e_v, 1, 1).wait()

            @pl.when((i > 0) | (half > 0))
            def _():
                q_copy(i, half).wait()

            def second_tile(t, carry):
                span = at_rows(half * half_rows + t * TILE, TILE)
                z = dot_nn(h_v[span, :], wu_v[i])
                p = dot_nn(e_v[span, :], wd_v[i])
                gelu, slope = gelu_parts(z)
                here = at_rows(t * TILE, TILE)
                a_v[here, :] = gelu.astype(jnp.bfloat16)
                q_v[here, :] = (p * slope).astype(jnp.bfloat16)

                @pl.when((t == 0) & (half == 0) & (i > 1))
                def _():
                    rs3(1, i - 2, g3_out)
                    give_free(i - 2)

                @pl.when((t == 1) & (half == 0) & (i > 0))
                def _():
                    rs1(0, i - 1)

                @pl.when((t == 5) & (half == 0) & (i > 0))
                def _():
                    rs1(1, i - 1)

                @pl.when((t == 0) & (half == 1) & (i > 0))
                def _():
                    rs2(0, i - 1)

                @pl.when((t == 6) & (half == 1) & (i > 0))
                def _():
                    rs2(1, i - 1)
                return carry

            lax.fori_loop(0, tiles, second_tile, 0)
            q_copy(i, half).start()

            grad_down(a_v, e_v, half)

            @pl.when(i == CHUNKS - 1)
            def _():
                @pl.when(half == 0)
                def _():
                    up_t_copy(0).start()

                @pl.when(half == 1)
                def _():
                    up_t_copy(1).start()

            @pl.when(half == 1)
            def _():
                rs0(0, i)

                @pl.when(i > 0)
                def _():
                    rs3(0, i - 1, g4_out)

            grad_up(h_v, q_v, half)

            @pl.when(half == 1)
            def _():
                rs0(1, i)
            return carry

        lax.fori_loop(0, 2, second_half, 0)
        return carry

    lax.fori_loop(0, CHUNKS, second_chunk, 0)

    q_copy(CHUNKS - 1, 1).wait()
    for chunk in range(CHUNKS):
        start_down(down_t_one, chunk)
    r_rows = half_rows // 4
    staging = (a_v, q_v)

    def r_load(slot, t):
        for k in range(CHUNKS):
            pltpu.make_async_copy(q_hbm.at[k, at_rows(t * r_rows, r_rows), :], staging[slot].at[pl.ds(k * r_rows, r_rows), :], load_sem.at[2, slot]).start()

    def a_load(i, half):
        return pltpu.make_async_copy(a_hbm.at[i, pl.ds(half * half_rows, half_rows), :], staging[half], load_sem.at[0, half])

    for slot in range(2):
        r_load(slot, slot)
    r_steps = rows // r_rows // 2

    def r_pair(t, carry):
        for slot in range(2):
            whole = staging[slot].at[pl.ds(0, CHUNKS * r_rows), :]
            pltpu.make_async_copy(whole, whole, load_sem.at[2, slot]).wait()
            for part in range(2):
                m = part * (r_rows // 2)
                acc = dot_nn(staging[slot][m:m + r_rows // 2, :], e_v[0:wide, :])
                for k in range(1, CHUNKS):
                    acc = acc + dot_nn(staging[slot][k * r_rows + m:k * r_rows + m + r_rows // 2, :], e_v[k * wide:(k + 1) * wide, :])
                h_v[at_rows((2 * t + slot) * r_rows + m, r_rows // 2), :] = acc.astype(jnp.bfloat16)

            @pl.when(t < r_steps - 1)
            def _():
                r_load(slot, 2 * t + 2 + slot)

        @pl.when(t == 0)
        def _():
            rs1(0, CHUNKS - 1)
            rs1(1, CHUNKS - 1)

        @pl.when(t == 2)
        def _():
            rs2(0, CHUNKS - 1)
        return carry

    rs3(1, CHUNKS - 2, g3_out)
    give_free(CHUNKS - 2)
    for part in range(2):
        up_t_copy(part).wait()
    lax.fori_loop(0, r_steps, r_pair, 0)
    for half in range(2):
        half_copy(x_hbm, e_v, half, 1).start()
    for half in range(2):
        a_load(0, half).start()

    def s_load(i, t):
        slot = lax.rem(t, slots)
        return pltpu.make_async_copy(s_hbm.at[i, at_rows(t * TILE, TILE), :], s_v.at[slot], s_sem.at[slot])

    for t in range(slots):
        s_load(0, t).start()

    def first_chunk(i, carry):
        @pl.when(i == 1)
        def _():
            rs2(0, 0)

        a_load(i, 0).wait()
        grad_down(a_v, h_v, 0)

        @pl.when(i < CHUNKS - 1)
        def _():
            a_load(i + 1, 0).start()

        @pl.when(i == 0)
        def _():
            rs2(1, 2)

        @pl.when(i == 2)
        def _():
            rs2(0, 1)

        a_load(i, 1).wait()
        grad_down(q_v, h_v, 1)
        pl.semaphore_wait(free_sem.at[i], 3)
        rs0(0, i)
        wait_weight(1, i)

        @pl.when(i == 0)
        def _():
            for half in range(2):
                half_copy(x_hbm, e_v, half, 1).wait()

        def first_half(half, carry):
            def first_tile(t, carry):
                tt = half * tiles + t
                s_load(i, tt).wait()
                p = dot_nn(h_v[at_rows(tt * TILE, TILE), :], wd_v[i])
                q_v[at_rows(t * TILE, TILE), :] = (p * s_v[lax.rem(tt, slots)]).astype(jnp.bfloat16)

                ahead = tt + slots
                @pl.when(ahead < 2 * tiles)
                def _():
                    s_load(i, ahead).start()

                @pl.when((tt == 7) & (i == 0))
                def _():
                    rs3(1, 2, g3_out)
                    give_free(2)

                @pl.when((tt == tiles + 6) & (i == 1))
                def _():
                    rs2(1, 0)
                return carry

            @pl.when(half == 0)
            def _():
                @pl.when(i > 0)
                def _():
                    rs1(1, i - 1)

                @pl.when(i == 0)
                def _():
                    rs3(0, 2, g4_out)

                @pl.when(i == 1)
                def _():
                    rs3(0, 0, g2_out)

                @pl.when(i == 2)
                def _():
                    rs3(1, 0, g1_out)

            lax.fori_loop(0, tiles, first_tile, 0)

            @pl.when((half == 1) & (i < CHUNKS - 1))
            def _():
                for t in range(slots):
                    s_load(i + 1, t).start()

            @pl.when(half == 0)
            def _():
                rs1(0, i)

                @pl.when(i == 2)
                def _():
                    rs3(0, 1, g2_out)

            grad_up(e_v, q_v, half)
            return carry

        lax.fori_loop(0, 2, first_half, 0)
        rs0(1, i)

        @pl.when(i < CHUNKS - 1)
        def _():
            a_load(i + 1, 1).start()
        return carry

    lax.fori_loop(0, CHUNKS, first_chunk, 0)
    rs2(1, 1)
    rs1(1, 2)
    rs2(0, 2)
    rs3(1, 1, g1_out)
    rs2(1, 2)
    rs3(0, 2, g2_out)
    rs3(1, 2, g1_out)
    slots_v[me] = sq_v[...]
    for copy in exchange_start(me, group_size, slots_v, stat_send, stat_recv):
        copy.wait()
    total = slots_v[0]
    for index in range(1, group_size):
        total = total + slots_v[index]
    norm_out[...] = jnp.full(norm_out.shape, jnp.sum(total))


def backward_blocks(group_size, act_in, grad_out, hidden, act_one, slope_one, w_up, down_t_one, down_t_two, up_t):
    rows, dim = act_in.shape
    ff = w_up.shape[2]
    wide = ff // CHUNKS
    up_rows, down_rows = dim // group_size, LANES
    hbm = pl.BlockSpec(memory_space=pl.ANY)
    vmem = pl.BlockSpec(memory_space=pltpu.VMEM)
    f32 = jnp.float32
    bf16 = jnp.bfloat16
    up_grad = jax.ShapeDtypeStruct((up_rows, ff), f32)
    down_grad = jax.ShapeDtypeStruct((ff // group_size, dim), f32)

    def stages(height, cols):
        return [
            pltpu.VMEM((CHUNKS, 2, 2, 2, height, cols // 2), f32),
            pltpu.VMEM((CHUNKS, 2, height, cols // 2), f32),
            pltpu.VMEM((CHUNKS, 2, height, cols // 2), f32),
            pltpu.VMEM((CHUNKS, height, cols // 2), f32),
            pltpu.VMEM((CHUNKS, height, cols // 2), f32),
        ]

    return pl.pallas_call(
        functools.partial(backward_kernel, group_size),
        out_shape=[up_grad, down_grad, up_grad, down_grad, jax.ShapeDtypeStruct((8, 128), f32), jax.ShapeDtypeStruct((CHUNKS, rows, wide), bf16)],
        in_specs=[hbm] * 9,
        out_specs=[vmem] * 5 + [hbm],
        scratch_shapes=[
            pltpu.VMEM((rows, dim), bf16),
            pltpu.VMEM((rows, dim), bf16),
            pltpu.VMEM((CHUNKS, dim, wide), bf16),
            pltpu.VMEM((CHUNKS, dim, wide), bf16),
            pltpu.VMEM((rows // 2, wide), bf16),
            pltpu.VMEM((rows // 2, wide), bf16),
            pltpu.VMEM((SLOTS, TILE, wide), f32),
            pltpu.VMEM((2, 2, 2, 2, down_rows, dim // 2), f32),
            pltpu.VMEM((2, 2, 2, 2, up_rows, wide // 2), f32),
            *stages(down_rows, dim),
            *stages(up_rows, wide),
            pltpu.VMEM((8, 128), f32),
            pltpu.VMEM((group_size, 8, 128), f32),
            pltpu.SemaphoreType.DMA((3, 2)),
            pltpu.SemaphoreType.DMA((2, CHUNKS)),
            pltpu.SemaphoreType.DMA((1,)),
            pltpu.SemaphoreType.DMA((SLOTS,)),
            pltpu.SemaphoreType.DMA((2, CHUNKS, 5)),
            pltpu.SemaphoreType.DMA((2, CHUNKS, 5)),
            pltpu.SemaphoreType.REGULAR((CHUNKS,)),
            pltpu.SemaphoreType.DMA((group_size,)),
            pltpu.SemaphoreType.DMA((group_size,)),
        ],
        compiler_params=pltpu.CompilerParams(collective_id=2, has_side_effects=True, vmem_limit_bytes=FULL_VMEM),
        name="backward_blocks",
    )(act_in, grad_out, hidden, act_one, slope_one, w_up, down_t_one, down_t_two, up_t.reshape(ff, dim))[:5]


def moments_kernel(clip_ref, norm_ref, g_one, g_two, g_three, g_four, m_up, m_down, v_up, v_down, m_up_out, m_down_out, v_up_out, v_down_out, u_up, u_down, stats):
    inv_one = 1.0 / (1.0 - BETA_ONE ** STEP)
    inv_two = 1.0 / (1.0 - BETA_TWO ** STEP)
    scale = jnp.minimum(1.0, clip_ref[0] / (jnp.sqrt(norm_ref[0:1, 0:1]) + NORM_EPS))
    row_id = lax.broadcasted_iota(jnp.int32, (8, 128), 0)
    sums = jnp.zeros((8, 128), jnp.float32)
    for family, (grads, m, v, m_out, v_out, u) in enumerate([((g_one, g_three), m_up, v_up, m_up_out, v_up_out, u_up), ((g_two, g_four), m_down, v_down, m_down_out, v_down_out, u_down)]):
        for layer in range(2):
            grad = grads[layer][...]
            avg_new = BETA_ONE * m[layer] + (1.0 - BETA_ONE) * scale * grad
            sq_new = BETA_TWO * v[layer] + (1.0 - BETA_TWO) * (scale * scale) * (grad * grad)
            direction = (avg_new * inv_one) / (jnp.sqrt(sq_new * inv_two) + ADAM_EPS)
            m_out[layer] = avg_new
            v_out[layer] = sq_new
            u[layer] = direction
            sums = sums + jnp.where(row_id == 4 + 2 * family + layer, jnp.sum(direction * direction), 0.0)

    @pl.when(pl.program_id(0) == 0)
    def _():
        stats[...] = jnp.zeros_like(stats)

    stats[...] += sums


def moments(clip_norm, norm_tile, grads, m_up, m_down, v_up, v_down, steps=4):
    up, down = m_up.shape, m_down.shape
    up_spec = pl.BlockSpec((2, up[1] // steps, up[2]), lambda i: (0, i, 0))
    down_spec = pl.BlockSpec((2, down[1] // steps, down[2]), lambda i: (0, i, 0))
    up_grad = pl.BlockSpec((up[1] // steps, up[2]), lambda i: (i, 0))
    down_grad = pl.BlockSpec((down[1] // steps, down[2]), lambda i: (i, 0))
    tile = pl.BlockSpec((8, 128), lambda i: (0, 0))
    pair = [up_spec, down_spec]
    up_shape, down_shape = jax.ShapeDtypeStruct(up, jnp.float32), jax.ShapeDtypeStruct(down, jnp.float32)
    return pl.pallas_call(
        moments_kernel,
        grid=(steps,),
        out_shape=[up_shape, down_shape] * 3 + [jax.ShapeDtypeStruct((8, 128), jnp.float32)],
        in_specs=[pl.BlockSpec(memory_space=pltpu.SMEM), tile] + [up_grad, down_grad] * 2 + pair * 2,
        out_specs=pair * 3 + [tile],
        compiler_params=pltpu.CompilerParams(dimension_semantics=("arbitrary",), vmem_limit_bytes=FULL_VMEM),
        name="moments",
    )(clip_norm.reshape(1), norm_tile, *grads, m_up, m_down, v_up, v_down)


PIECES = ((0, 0), (0, 1), (1, 0), (1, 1))


def update_kernel(group_size, rate_ref, stats_ref, u_up_hbm, u_down_hbm, p_up_hbm, p_down_hbm, all_up, all_down, p_up_out, p_down_out,
                  slots, u_up, u_down, p_up, p_down, w_up, w_down, stat_send, stat_recv, send_sem, recv_sem, local_sem, in_sem, out_sem):
    me, partner, near_x, near_y = coords()
    loads = []
    for src, dst in ((p_up_hbm, p_up), (p_down_hbm, p_down), (u_up_hbm, u_up), (u_down_hbm, u_down)):
        for layer in range(2):
            copy = pltpu.make_async_copy(src.at[layer], dst.at[layer], in_sem.at[len(loads)])
            copy.start()
            loads.append(copy)
    meet_all(me, group_size)
    row_id = lax.broadcasted_iota(jnp.int32, (8, 128), 0)
    stats = stats_ref[...]
    for index in range(4):
        loads[index].wait()
        master = (p_up, p_down)[index // 2][index % 2]
        stats = stats + jnp.where(row_id == index, jnp.sum(master * master), 0.0)
    slots[me] = stats
    for copy in exchange_start(me, group_size, slots, stat_send, stat_recv):
        copy.wait()
    total = slots[0]
    for index in range(1, group_size):
        total = total + slots[index]
    ratio = jnp.sqrt(total[0:4]) / jnp.sqrt(total[4:8])
    rate = rate_ref[0]
    params = ((u_up, p_up, p_up_out, w_up, all_up), (u_down, p_down, p_down_out, w_down, all_down))

    def place(piece, owner):
        family, layer = PIECES[piece]
        full = params[family][4]
        rows = params[family][3].shape[1]
        return full.at[layer, pl.ds(pl.multiple_of(owner * rows, rows), rows), :]

    sends = []
    count = [0]

    def forward(src, piece, owner, device, rel):
        copy = remote(src, place(piece, owner), send_sem.at[count[0]], recv_sem.at[rel, piece], device)
        count[0] += 1
        copy.start()
        sends.append(copy)

    def arrival(piece, rel, owner):
        spot = place(piece, owner)
        remote(spot, spot, send_sem.at[0], recv_sem.at[rel, piece], me).wait_recv()
        return spot

    own = {}
    local = []
    for piece in (0, 2, 1, 3):
        family, layer = PIECES[piece]
        u, p, p_out, w, full = params[family]
        index = 2 * family + layer
        loads[4 + index].wait()
        new = p[layer] - rate * ratio[index:index + 1, 0:1] * u[layer]
        w[layer] = new.astype(jnp.bfloat16)
        own[piece] = w.at[layer]
        if family == 0:
            forward(own[piece], piece, me, near_x, 2)
        else:
            forward(own[piece], piece, me, near_y, 4)
        forward(own[piece], piece, me, partner, 1)
        copy = pltpu.make_async_copy(own[piece], place(piece, me), local_sem.at[piece])
        copy.start()
        local.append(copy)
        p[layer] = new
        copy = pltpu.make_async_copy(p.at[layer], p_out.at[layer], out_sem.at[piece])
        copy.start()
        local.append(copy)
    for piece in (2, 3):
        forward(own[piece], piece, me, near_x, 2)
    for piece in (0, 1):
        forward(own[piece], piece, me, near_y, 4)
    diag = near_x + near_y - me
    for k in range(2):
        spot = arrival(k, 2, near_x)
        forward(spot, k, near_x, near_y, 6)
        forward(spot, k, near_x, partner, 3)
        spot = arrival(2 + k, 4, near_y)
        forward(spot, 2 + k, near_y, near_x, 6)
        forward(spot, 2 + k, near_y, partner, 5)
    for k in range(2):
        spot = arrival(2 + k, 2, near_x)
        forward(spot, 2 + k, near_x, partner, 3)
        spot = arrival(k, 4, near_y)
        forward(spot, k, near_y, partner, 5)
    for k in range(2):
        for piece in (2 + k, k):
            spot = arrival(piece, 6, diag)
            forward(spot, piece, diag, partner, 7)
    for rel, owner in ((1, partner), (3, near_x + partner - me), (5, near_y + partner - me), (7, diag + partner - me)):
        for piece in range(4):
            arrival(piece, rel, owner)
    for copy in sends:
        copy.wait_send()
    for copy in local:
        copy.wait()


def update_and_gather(group_size, learn_rate, stats, u_up, u_down, p_up, p_down):
    up, down = p_up.shape, p_down.shape
    vmem = pl.BlockSpec(memory_space=pltpu.VMEM)
    hbm = pl.BlockSpec(memory_space=pl.ANY)
    return pl.pallas_call(
        functools.partial(update_kernel, group_size),
        out_shape=[
            pltpu.VMEM((up[0], up[1] * group_size, up[2]), jnp.bfloat16),
            pltpu.VMEM((down[0], down[1] * group_size, down[2]), jnp.bfloat16),
            jax.ShapeDtypeStruct(up, jnp.float32),
            jax.ShapeDtypeStruct(down, jnp.float32),
        ],
        in_specs=[pl.BlockSpec(memory_space=pltpu.SMEM), vmem] + [hbm] * 4,
        out_specs=[vmem] * 2 + [hbm] * 2,
        scratch_shapes=[
            pltpu.VMEM((group_size, 8, 128), jnp.float32),
            pltpu.VMEM(up, jnp.float32),
            pltpu.VMEM(down, jnp.float32),
            pltpu.VMEM(up, jnp.float32),
            pltpu.VMEM(down, jnp.float32),
            pltpu.VMEM(up, jnp.bfloat16),
            pltpu.VMEM(down, jnp.bfloat16),
            pltpu.SemaphoreType.DMA((group_size,)),
            pltpu.SemaphoreType.DMA((group_size,)),
            pltpu.SemaphoreType.DMA((32,)),
            pltpu.SemaphoreType.DMA((group_size, 4)),
            pltpu.SemaphoreType.DMA((4,)),
            pltpu.SemaphoreType.DMA((8,)),
            pltpu.SemaphoreType.DMA((4,)),
        ],
        compiler_params=pltpu.CompilerParams(collective_id=1, has_side_effects=True, vmem_limit_bytes=FULL_VMEM - 2 * group_size * (up[0] * up[1] * up[2] + down[0] * down[1] * down[2]) - 256 * 1024),
        name="update_and_gather",
    )(learn_rate.reshape(1), stats, u_up, u_down, p_up, p_down)


def solution(mesh):
    group_size = mesh.shape["data"]
    batch_rows = P("data", None)
    state_rows = P(None, "data", None)
    replicated = P()

    def device_step(act_in, grad_out, w_up, w_down, master_up, master_down, exp_avg_up, exp_avg_down, exp_sq_up, exp_sq_down, learn_rate, clip_norm):
        act_one, slope_one, hidden, *turned = forward_block(act_in, w_up, w_down)
        *grads, norm_tile = backward_blocks(group_size, act_in, grad_out, hidden, act_one, slope_one, w_up, *turned)
        grad_norm = jnp.sqrt(norm_tile[0, 0])
        avg_up, avg_down, sq_up, sq_down, dir_up, dir_down, stats = moments(clip_norm, norm_tile, grads, exp_avg_up, exp_avg_down, exp_sq_up, exp_sq_down)
        new_w_up, new_w_down, master_up_out, master_down_out = update_and_gather(group_size, learn_rate, stats, dir_up, dir_down, master_up, master_down)
        return (new_w_up, new_w_down, master_up_out, master_down_out, avg_up, avg_down, sq_up, sq_down, grad_norm)

    return jax.shard_map(device_step, mesh=mesh, in_specs=(batch_rows, batch_rows, replicated, replicated, state_rows, state_rows, state_rows, state_rows, state_rows, state_rows, replicated, replicated), out_specs=(replicated, replicated, state_rows, state_rows, state_rows, state_rows, state_rows, state_rows, replicated), check_vma=False)
```

```python
import functools

import jax
import jax.numpy as jnp
from jax import lax
from jax.experimental import pallas as pl
from jax.experimental.pallas import tpu as pltpu
from jax.sharding import PartitionSpec as P

STEP = 10
BETA_ONE = 0.9
BETA_TWO = 0.95
ADAM_EPS = 1e-8
NORM_EPS = 1e-6
INV_SQRT_TWO = 0.7071067811865476
INV_SQRT_TWO_PI = 0.3989422804014327


def gelu_parts(pre_act):
    normal_cdf = 0.5 * (1.0 + lax.erf(pre_act * INV_SQRT_TWO))
    normal_pdf = jnp.exp(-0.5 * pre_act * pre_act) * INV_SQRT_TWO_PI
    return pre_act * normal_cdf, normal_cdf + pre_act * normal_pdf


MESH = pl.DeviceIdType.MESH


def coords():
    me = lax.axis_index("data")
    core, col, row = me % 2, (me // 2) % 2, me // 4
    return me, me + 1 - 2 * core, me + 2 - 4 * col, me + 4 - 8 * row


def remote(src, dst, send_sem, recv_sem, device):
    return pltpu.make_async_remote_copy(src_ref=src, dst_ref=dst, send_sem=send_sem, recv_sem=recv_sem, device_id=(device,), device_id_type=MESH)


def meet_all(me, group_size):
    barrier = pltpu.get_barrier_semaphore()
    for step in range(1, group_size):
        pl.semaphore_signal(barrier, inc=1, device_id=((me + step) % group_size,), device_id_type=MESH)
    pl.semaphore_wait(barrier, group_size - 1)


def exchange_start(me, group_size, slots, send_sem, recv_sem):
    copies = []
    for step in range(1, group_size):
        copies.append(remote(slots.at[me], slots.at[me], send_sem.at[step], recv_sem.at[step], (me + step) % group_size))
        copies[-1].start()
    return copies


CHUNKS = 3
HALVES = range(2)
DOWN, UP = HALVES
FIRST, SECOND, THIRD = range(CHUNKS)
ZERO = 0.0
LANES = 128
TILE = 256
SLOTS = 4
OWNERS = tuple(chip * 2 + core for core in HALVES for chip in range(4))
FULL_VMEM = 67043328


def dot_nn(lhs, rhs):
    return jnp.dot(lhs, rhs, preferred_element_type=jnp.float32)


def dot_tn(lhs, rhs):
    return lax.dot_general(lhs, rhs, (((0,), (0,)), ((), ())), preferred_element_type=jnp.float32)


def chunk_blocks(chunk, width):
    return [owner * width + chunk * LANES for owner in OWNERS]


def forward_kernel(x_ref, w_up_ref, w_down_ref, up_block, down_block_one, down_block_two, a_out, s_out, h_out, down_t_one, down_t_two, up_t):
    for block, out in ((down_block_one, down_t_one), (down_block_two, down_t_two)):
        for chunk in range(CHUNKS):
            out[chunk] = block[0, chunk * LANES:(chunk + 1) * LANES, :].T
    for chunk in range(CHUNKS):
        up_t[chunk, 0] = up_block[0, :, chunk * LANES:(chunk + 1) * LANES].T
    x = x_ref[...]
    width = w_up_ref.shape[2] // len(OWNERS)
    total = None
    for chunk in range(CHUNKS):
        starts = chunk_blocks(chunk, width)
        w_in = jnp.concatenate([w_up_ref[0, :, s:s + LANES] for s in starts], axis=1)
        gelu, slope = gelu_parts(dot_nn(x, w_in))
        act = gelu.astype(jnp.bfloat16)
        a_out[chunk] = act
        s_out[chunk] = slope
        w_out = jnp.concatenate([w_down_ref[0, s:s + LANES, :] for s in starts], axis=0)
        part = dot_nn(act, w_out)
        total = part if total is None else total + part
    h_out[...] = total.astype(jnp.bfloat16)


def forward_block(act_in, w_up, w_down, tile=512):
    rows, dim = act_in.shape
    ff = w_up.shape[2]
    wide = ff // CHUNKS
    owners = len(OWNERS)
    width = ff // owners
    assert rows // tile == owners

    def slot(i):
        return (i % 2) * (owners // 2) + i // 2

    return pl.pallas_call(
        forward_kernel,
        grid=(rows // tile,),
        out_shape=[
            jax.ShapeDtypeStruct((CHUNKS, rows, wide), jnp.bfloat16),
            jax.ShapeDtypeStruct((CHUNKS, rows, wide), jnp.float32),
            jax.ShapeDtypeStruct((rows, dim), jnp.bfloat16),
            jax.ShapeDtypeStruct((CHUNKS, dim, wide), jnp.bfloat16),
            jax.ShapeDtypeStruct((CHUNKS, dim, wide), jnp.bfloat16),
            jax.ShapeDtypeStruct((CHUNKS, owners, LANES, dim), jnp.bfloat16),
        ],
        in_specs=[
            pl.BlockSpec((tile, dim), lambda i: (i, 0)),
            pl.BlockSpec((1, dim, ff), lambda i: (0, 0, 0)),
            pl.BlockSpec((1, ff, dim), lambda i: (0, 0, 0)),
            pl.BlockSpec((1, dim, width), lambda i: (1, 0, i)),
            pl.BlockSpec((1, width, dim), lambda i: (0, i, 0)),
            pl.BlockSpec((1, width, dim), lambda i: (1, i, 0)),
        ],
        out_specs=[
            pl.BlockSpec((CHUNKS, tile, wide), lambda i: (0, i, 0)),
            pl.BlockSpec((CHUNKS, tile, wide), lambda i: (0, i, 0)),
            pl.BlockSpec((tile, dim), lambda i: (i, 0)),
            pl.BlockSpec((CHUNKS, dim, LANES), lambda i: (0, 0, slot(i))),
            pl.BlockSpec((CHUNKS, dim, LANES), lambda i: (0, 0, slot(i))),
            pl.BlockSpec((CHUNKS, 1, LANES, dim), lambda i: (0, slot(i), 0, 0)),
        ],
        compiler_params=pltpu.CompilerParams(dimension_semantics=("arbitrary",), vmem_limit_bytes=FULL_VMEM),
        name="forward_block",
    )(act_in, w_up, w_down, w_up, w_down, w_down)


def backward_kernel(group_size, x_hbm, e_hbm, h_hbm, a_hbm, s_hbm, w_up_hbm, down_t_one, down_t_two, up_t,
                    g1_hbm, g2_hbm, g3_hbm, g4_hbm, norm_out, q_hbm,
                    g1_out, g2_out, g3_out, g4_out, h_v, e_v, wu_v, wd_v, a_v, q_v, s_v, t_d, t_u,
                    d0, d1a, d1b, d2a, d2b, u0, u1a, u1b, u2a, u2b,
                    sq_v, slots_v, load_sem, w_sem, q_sem, s_sem, send_sem, recv_sem, free_sem, stat_send, stat_recv, out_sem):
    me, partner, near_x, near_y = coords()
    core, col, row = me % 2, (me // 2) % 2, me // 4
    rows, dim = h_v.shape
    half_rows = rows // 2
    wide = wu_v.shape[2]
    width = wide * CHUNKS // len(OWNERS)
    tiles = half_rows // TILE
    slots = s_v.shape[0]

    def at_rows(start, size):
        return pl.ds(pl.multiple_of(start, size), size)

    def half_copy(src, dst, half, sem):
        span = pl.ds(half * half_rows, half_rows)
        return pltpu.make_async_copy(src.at[span], dst.at[span], load_sem.at[sem, half])

    def start_up(chunk):
        for j, start in enumerate(chunk_blocks(chunk, width)):
            pltpu.make_async_copy(w_up_hbm.at[1, :, pl.ds(start, LANES)], wu_v.at[chunk, :, pl.ds(j * LANES, LANES)], w_sem.at[0, chunk]).start()

    def start_down(src, chunk):
        pltpu.make_async_copy(src.at[chunk], wd_v.at[chunk], w_sem.at[1, chunk]).start()

    def up_t_copy(part):
        span = (pl.ds(0, half_rows), pl.ds(half_rows, CHUNKS * wide - half_rows))[part]
        return pltpu.make_async_copy(up_t.at[span], e_v.at[span], load_sem.at[1, part])

    def wait_weight(which, chunk):
        ref = (wu_v, wd_v)[which]
        pltpu.make_async_copy(ref.at[chunk], ref.at[chunk], w_sem.at[which, chunk]).wait()

    half_copy(h_hbm, h_v, 0, 0).start()
    start_up(0)
    half_copy(e_hbm, e_v, 0, 1).start()
    start_down(down_t_two, 0)
    sq_v[...] = jnp.zeros_like(sq_v)
    meet_all(me, group_size)

    def hop(src, dst, kind, chunk, stage, device):
        return remote(src, dst, send_sem.at[kind, chunk, stage], recv_sem.at[kind, chunk, stage], device)

    def hop0(kind, i):
        if kind == DOWN:
            return hop(t_d.at[:, 1 - core], d0.at[i], 0, i, 0, partner)
        return hop(t_u.at[:, :, :, 1 - core], u0.at[i], 1, i, 0, partner)

    def bufs(kind):
        return (d0, d1a, d1b, d2a, d2b) if kind == DOWN else (u0, u1a, u1b, u2a, u2b)

    def hop1(kind, i):
        b0, b1a, b1b, _, _ = bufs(kind)
        return (hop(b0.at[i, 0, :, 1 - col], b1a.at[i], kind, i, 1, near_x),
                hop(b0.at[i, 1, 1 - row], b1b.at[i], kind, i, 2, near_y))

    def hop2(kind, i):
        _, b1a, b1b, b2a, b2b = bufs(kind)
        return (hop(b1a.at[i, 1 - row], b2a.at[i], kind, i, 3, near_y),
                hop(b1b.at[i, 1 - col], b2b.at[i], kind, i, 4, near_x))

    def rs0(kind, i):
        hop0(kind, i).start()

    def rs1(kind, i):
        hop0(kind, i).wait()
        b0 = bufs(kind)[0]
        for side in HALVES:
            for y in HALVES:
                for x in HALVES:
                    own = t_d[side, core, y, x] if kind == DOWN else t_u[side, y, x, core]
                    b0[i, side, y, x] = b0[i, side, y, x] + own
        for copy in hop1(kind, i):
            copy.start()

    def rs2(kind, i):
        b0, b1a, b1b, _, _ = bufs(kind)
        first, second = hop1(kind, i)
        out_a, out_b = hop2(kind, i)
        first.wait()
        for y in HALVES:
            b1a[i, y] = b1a[i, y] + b0[i, 0, y, col]
        out_a.start()
        second.wait()
        for x in HALVES:
            b1b[i, x] = b1b[i, x] + b0[i, 1, row, x]
        out_b.start()

    def rs3(kind, i, out):
        _, b1a, b1b, b2a, b2b = bufs(kind)
        cut = b1a.shape[3]
        for copy in hop2(kind, i):
            copy.wait()
        left = (b1a[i, row] + b2a[i]) / group_size
        right = (b1b[i, col] + b2b[i]) / group_size
        square = (left * left + right * right).reshape(left.shape[0] // 8, 8, cut).sum(axis=0)
        for lane in range(0, cut, LANES):
            sq_v[...] += square[:, lane:lane + LANES]
        if kind == DOWN:
            span = at_rows(i * LANES, LANES)
            out[span, 0:cut] = left
            out[span, cut:2 * cut] = right
        else:
            for j, owner in enumerate(OWNERS):
                part = (left, right)[j // 4]
                lane = (j % 4) * LANES
                out[:, pl.ds(pl.multiple_of(owner * width + i * LANES, LANES), LANES)] = part[:, lane:lane + LANES]

    results = tuple(pltpu.make_async_copy(src, dst, out_sem.at[k]) for k, (src, dst) in enumerate(((g1_out, g1_hbm), (g2_out, g2_hbm), (g3_out, g3_hbm), (g4_out, g4_hbm))))
    g1_copy, g2_copy, g3_copy, g4_copy = results

    def give_free(i):
        for device in (partner, near_x, near_y):
            pl.semaphore_signal(free_sem.at[i], inc=1, device_id=(device,), device_id_type=MESH)

    def grad_down(lhs_ref, rhs_ref, half):
        def part(m, carry):
            acc = dot_tn(lhs_ref[:, at_rows(m * (wide // 2), wide // 2)], rhs_ref[at_rows(half * half_rows, half_rows), :])
            cut = dim // 2
            for side in HALVES:
                piece = acc[:, side * cut:(side + 1) * cut].reshape(t_d.shape[2:])
                t_d[side, m] = piece + jnp.where(half == FIRST, ZERO, t_d[side, m])
            return carry
        lax.fori_loop(0, 2, part, 0)

    def grad_up(lhs_ref, rhs_ref, half):
        def part(m, carry):
            acc = dot_tn(lhs_ref[at_rows(half * half_rows, half_rows), at_rows(m * (dim // 2), dim // 2)], rhs_ref[...])
            cut = wide // 2
            for side in HALVES:
                piece = acc[:, side * cut:(side + 1) * cut].reshape(t_u.shape[2:])
                t_u[side, m] = piece + jnp.where(half == FIRST, ZERO, t_u[side, m])
            return carry
        lax.fori_loop(0, 2, part, 0)

    def q_copy(i, half):
        return pltpu.make_async_copy(q_v, q_hbm.at[i, at_rows(half * half_rows, half_rows), :], q_sem.at[0])

    def second_chunk(i, carry):
        wait_weight(0, i)
        wait_weight(1, i)

        @pl.when(i == FIRST)
        def _():
            half_copy(h_hbm, h_v, 0, 0).wait()
            half_copy(e_hbm, e_v, 0, 1).wait()
            half_copy(h_hbm, h_v, 1, 0).start()
            half_copy(e_hbm, e_v, 1, 1).start()
            for chunk in range(1, CHUNKS):
                start_up(chunk)
                start_down(down_t_two, chunk)

        def second_half(half, carry):
            @pl.when((i == FIRST) & (half == SECOND))
            def _():
                half_copy(h_hbm, h_v, 1, 0).wait()
                half_copy(e_hbm, e_v, 1, 1).wait()

            @pl.when((i > FIRST) | (half > 0))
            def _():
                q_copy(i, half).wait()

            def second_tile(t, carry):
                span = at_rows(half * half_rows + t * TILE, TILE)
                z = dot_nn(h_v[span, :], wu_v[i])
                p = dot_nn(e_v[span, :], wd_v[i])
                gelu, slope = gelu_parts(z)
                here = at_rows(t * TILE, TILE)
                a_v[here, :] = gelu.astype(jnp.bfloat16)
                q_v[here, :] = (p * slope).astype(jnp.bfloat16)

                @pl.when((t == 0) & (half == FIRST) & (i > SECOND))
                def _():
                    rs3(UP, i - 2, g3_out)
                    give_free(i - 2)

                @pl.when((t == 1) & (half == FIRST) & (i > FIRST))
                def _():
                    rs1(DOWN, i - 1)

                @pl.when((t == 5) & (half == FIRST) & (i > FIRST))
                def _():
                    rs1(UP, i - 1)

                @pl.when((t == 0) & (half == SECOND) & (i > FIRST))
                def _():
                    rs2(DOWN, i - 1)

                @pl.when((t == 6) & (half == SECOND) & (i > FIRST))
                def _():
                    rs2(UP, i - 1)
                return carry

            lax.fori_loop(0, tiles, second_tile, 0)
            q_copy(i, half).start()

            grad_down(a_v, e_v, half)

            @pl.when(i == THIRD)
            def _():
                @pl.when(half == FIRST)
                def _():
                    up_t_copy(0).start()

                @pl.when(half == SECOND)
                def _():
                    up_t_copy(1).start()

            @pl.when(half == SECOND)
            def _():
                rs0(DOWN, i)

                @pl.when(i > FIRST)
                def _():
                    rs3(DOWN, i - 1, g4_out)

            grad_up(h_v, q_v, half)

            @pl.when(half == SECOND)
            def _():
                rs0(UP, i)
            return carry

        lax.fori_loop(0, 2, second_half, 0)
        return carry

    lax.fori_loop(0, CHUNKS, second_chunk, 0)

    q_copy(THIRD, 1).wait()
    for chunk in range(CHUNKS):
        start_down(down_t_one, chunk)
    r_rows = half_rows // 4
    staging = (a_v, q_v)

    def r_load(slot, t):
        for k in range(CHUNKS):
            pltpu.make_async_copy(q_hbm.at[k, at_rows(t * r_rows, r_rows), :], staging[slot].at[pl.ds(k * r_rows, r_rows), :], load_sem.at[2, slot]).start()

    def a_load(i, half):
        return pltpu.make_async_copy(a_hbm.at[i, pl.ds(half * half_rows, half_rows), :], staging[half], load_sem.at[0, half])

    for slot in HALVES:
        r_load(slot, slot)
    r_steps = rows // r_rows // 2

    def r_pair(t, carry):
        for slot in HALVES:
            whole = staging[slot].at[pl.ds(0, CHUNKS * r_rows), :]
            pltpu.make_async_copy(whole, whole, load_sem.at[2, slot]).wait()
            for part in HALVES:
                m = part * (r_rows // 2)
                acc = dot_nn(staging[slot][m:m + r_rows // 2, :], e_v[0:wide, :])
                for k in range(1, CHUNKS):
                    acc = acc + dot_nn(staging[slot][k * r_rows + m:k * r_rows + m + r_rows // 2, :], e_v[k * wide:(k + 1) * wide, :])
                h_v[at_rows((2 * t + slot) * r_rows + m, r_rows // 2), :] = acc.astype(jnp.bfloat16)

            @pl.when(t < r_steps - 1)
            def _():
                r_load(slot, 2 * t + 2 + slot)

        @pl.when(t == 0)
        def _():
            rs1(DOWN, THIRD)
            rs1(UP, THIRD)

        @pl.when(t == 2)
        def _():
            rs2(DOWN, THIRD)
        return carry

    rs3(UP, SECOND, g3_out)
    give_free(SECOND)
    for part in HALVES:
        up_t_copy(part).wait()
    lax.fori_loop(0, r_steps, r_pair, 0)
    for half in HALVES:
        half_copy(x_hbm, e_v, half, 1).start()
    for half in HALVES:
        a_load(0, half).start()

    def s_load(i, t):
        slot = lax.rem(t, slots)
        return pltpu.make_async_copy(s_hbm.at[i, at_rows(t * TILE, TILE), :], s_v.at[slot], s_sem.at[slot])

    for t in range(slots):
        s_load(0, t).start()

    def first_chunk(i, carry):
        @pl.when(i == SECOND)
        def _():
            rs2(DOWN, FIRST)

        a_load(i, 0).wait()
        grad_down(a_v, h_v, 0)

        @pl.when(i < THIRD)
        def _():
            a_load(i + 1, 0).start()

        @pl.when(i == FIRST)
        def _():
            rs2(UP, THIRD)

        @pl.when(i == THIRD)
        def _():
            rs2(DOWN, SECOND)

        a_load(i, 1).wait()
        grad_down(q_v, h_v, 1)
        pl.semaphore_wait(free_sem.at[i], 3)
        rs0(DOWN, i)
        wait_weight(1, i)

        @pl.when(i == FIRST)
        def _():
            for half in HALVES:
                half_copy(x_hbm, e_v, half, 1).wait()

        def first_half(half, carry):
            def first_tile(t, carry):
                tt = half * tiles + t
                s_load(i, tt).wait()
                p = dot_nn(h_v[at_rows(tt * TILE, TILE), :], wd_v[i])
                q_v[at_rows(t * TILE, TILE), :] = (p * s_v[lax.rem(tt, slots)]).astype(jnp.bfloat16)

                ahead = tt + slots
                @pl.when(ahead < 2 * tiles)
                def _():
                    s_load(i, ahead).start()

                @pl.when((tt == 7) & (i == FIRST))
                def _():
                    rs3(UP, THIRD, g3_out)
                    give_free(THIRD)
                    g3_copy.start()
                    g4_copy.start()

                @pl.when((tt == tiles + 6) & (i == SECOND))
                def _():
                    rs2(UP, FIRST)
                return carry

            @pl.when(half == FIRST)
            def _():
                @pl.when(i > FIRST)
                def _():
                    rs1(UP, i - 1)

                @pl.when(i == FIRST)
                def _():
                    rs3(DOWN, THIRD, g4_out)

                @pl.when(i == SECOND)
                def _():
                    rs3(DOWN, FIRST, g2_out)

                @pl.when(i == THIRD)
                def _():
                    rs3(UP, FIRST, g1_out)

            lax.fori_loop(0, tiles, first_tile, 0)

            @pl.when((half == SECOND) & (i < THIRD))
            def _():
                for t in range(slots):
                    s_load(i + 1, t).start()

            @pl.when(half == FIRST)
            def _():
                rs1(DOWN, i)

                @pl.when(i == THIRD)
                def _():
                    rs3(DOWN, SECOND, g2_out)

            grad_up(e_v, q_v, half)
            return carry

        lax.fori_loop(0, 2, first_half, 0)
        rs0(UP, i)

        @pl.when(i < THIRD)
        def _():
            a_load(i + 1, 1).start()
        return carry

    lax.fori_loop(0, CHUNKS, first_chunk, 0)
    rs2(UP, SECOND)
    rs1(UP, THIRD)
    rs2(DOWN, THIRD)
    rs3(UP, SECOND, g1_out)
    rs2(UP, THIRD)
    rs3(DOWN, THIRD, g2_out)
    g2_copy.start()
    rs3(UP, THIRD, g1_out)
    g1_copy.start()
    slots_v[me] = sq_v[...]
    for copy in exchange_start(me, group_size, slots_v, stat_send, stat_recv):
        copy.wait()
    total = slots_v[0]
    for index in range(1, group_size):
        total = total + slots_v[index]
    norm_out[...] = jnp.full(norm_out.shape, jnp.sum(total))
    for copy in results:
        copy.wait()


def backward_blocks(group_size, act_in, grad_out, hidden, act_one, slope_one, w_up, down_t_one, down_t_two, up_t):
    rows, dim = act_in.shape
    ff = w_up.shape[2]
    wide = ff // CHUNKS
    up_rows, down_rows = dim // group_size, LANES
    hbm = pl.BlockSpec(memory_space=pl.ANY)
    vmem = pl.BlockSpec(memory_space=pltpu.VMEM)
    f32 = jnp.float32
    bf16 = jnp.bfloat16
    up_grad = jax.ShapeDtypeStruct((up_rows, ff), f32)
    down_grad = jax.ShapeDtypeStruct((ff // group_size, dim), f32)

    def stages(height, cols):
        return [
            pltpu.VMEM((CHUNKS, 2, 2, 2, height, cols // 2), f32),
            pltpu.VMEM((CHUNKS, 2, height, cols // 2), f32),
            pltpu.VMEM((CHUNKS, 2, height, cols // 2), f32),
            pltpu.VMEM((CHUNKS, height, cols // 2), f32),
            pltpu.VMEM((CHUNKS, height, cols // 2), f32),
        ]

    return pl.pallas_call(
        functools.partial(backward_kernel, group_size),
        out_shape=[up_grad, down_grad, up_grad, down_grad, jax.ShapeDtypeStruct((8, 128), f32), jax.ShapeDtypeStruct((CHUNKS, rows, wide), bf16)],
        in_specs=[hbm] * 9,
        out_specs=[hbm] * 4 + [vmem, hbm],
        scratch_shapes=[
            *(pltpu.VMEM(g.shape, f32) for g in (up_grad, down_grad, up_grad, down_grad)),
            pltpu.VMEM((rows, dim), bf16),
            pltpu.VMEM((rows, dim), bf16),
            pltpu.VMEM((CHUNKS, dim, wide), bf16),
            pltpu.VMEM((CHUNKS, dim, wide), bf16),
            pltpu.VMEM((rows // 2, wide), bf16),
            pltpu.VMEM((rows // 2, wide), bf16),
            pltpu.VMEM((SLOTS, TILE, wide), f32),
            pltpu.VMEM((2, 2, 2, 2, down_rows, dim // 2), f32),
            pltpu.VMEM((2, 2, 2, 2, up_rows, wide // 2), f32),
            *stages(down_rows, dim),
            *stages(up_rows, wide),
            pltpu.VMEM((8, 128), f32),
            pltpu.VMEM((group_size, 8, 128), f32),
            pltpu.SemaphoreType.DMA((3, 2)),
            pltpu.SemaphoreType.DMA((2, CHUNKS)),
            pltpu.SemaphoreType.DMA((1,)),
            pltpu.SemaphoreType.DMA((SLOTS,)),
            pltpu.SemaphoreType.DMA((2, CHUNKS, 5)),
            pltpu.SemaphoreType.DMA((2, CHUNKS, 5)),
            pltpu.SemaphoreType.REGULAR((CHUNKS,)),
            pltpu.SemaphoreType.DMA((group_size,)),
            pltpu.SemaphoreType.DMA((group_size,)),
            pltpu.SemaphoreType.DMA((4,)),
        ],
        compiler_params=pltpu.CompilerParams(collective_id=2, has_side_effects=True, vmem_limit_bytes=FULL_VMEM),
        name="backward_blocks",
    )(act_in, grad_out, hidden, act_one, slope_one, w_up, down_t_one, down_t_two, up_t.reshape(ff, dim))[:5]


def moments_kernel(clip_ref, norm_ref, g_one, g_two, g_three, g_four, m_up, m_down, v_up, v_down, m_up_out, m_down_out, v_up_out, v_down_out, u_up, u_down, stats, norm_out):
    inv_one = 1.0 / (1.0 - BETA_ONE ** STEP)
    inv_two = 1.0 / (1.0 - BETA_TWO ** STEP)
    norm_out[0] = jnp.sqrt(norm_ref[0, 0])
    scale = jnp.minimum(1.0, clip_ref[0] / (jnp.sqrt(norm_ref[0:1, 0:1]) + NORM_EPS))
    row_id = lax.broadcasted_iota(jnp.int32, (8, 128), 0)
    sums = jnp.zeros((8, 128), jnp.float32)
    for family, (grads, m, v, m_out, v_out, u) in enumerate([((g_one, g_three), m_up, v_up, m_up_out, v_up_out, u_up), ((g_two, g_four), m_down, v_down, m_down_out, v_down_out, u_down)]):
        for layer in HALVES:
            grad = grads[layer][...]
            avg_new = BETA_ONE * m[layer] + (1.0 - BETA_ONE) * scale * grad
            sq_new = BETA_TWO * v[layer] + (1.0 - BETA_TWO) * (scale * scale) * (grad * grad)
            direction = (avg_new * inv_one) / (jnp.sqrt(sq_new * inv_two) + ADAM_EPS)
            m_out[layer] = avg_new
            v_out[layer] = sq_new
            u[layer] = direction
            sums = sums + jnp.where(row_id == 4 + 2 * family + layer, jnp.sum(direction * direction), 0.0)

    @pl.when(pl.program_id(0) == 0)
    def _():
        stats[...] = jnp.zeros_like(stats)

    stats[...] += sums


def moments(clip_norm, norm_tile, grads, m_up, m_down, v_up, v_down, steps=4):
    up, down = m_up.shape, m_down.shape
    up_spec = pl.BlockSpec((2, up[1] // steps, up[2]), lambda i: (0, i, 0))
    down_spec = pl.BlockSpec((2, down[1] // steps, down[2]), lambda i: (0, i, 0))
    up_grad = pl.BlockSpec((up[1] // steps, up[2]), lambda i: (i, 0))
    down_grad = pl.BlockSpec((down[1] // steps, down[2]), lambda i: (i, 0))
    tile = pl.BlockSpec((8, 128), lambda i: (0, 0))
    pair = [up_spec, down_spec]
    up_shape, down_shape = jax.ShapeDtypeStruct(up, jnp.float32), jax.ShapeDtypeStruct(down, jnp.float32)
    return pl.pallas_call(
        moments_kernel,
        grid=(steps,),
        out_shape=[up_shape, down_shape] * 3 + [jax.ShapeDtypeStruct((8, 128), jnp.float32), jax.ShapeDtypeStruct((1,), jnp.float32)],
        in_specs=[pl.BlockSpec(memory_space=pltpu.SMEM), tile] + [up_grad, down_grad] * 2 + pair * 2,
        out_specs=pair * 3 + [tile, pl.BlockSpec(memory_space=pltpu.SMEM)],
        compiler_params=pltpu.CompilerParams(dimension_semantics=("arbitrary",), vmem_limit_bytes=FULL_VMEM),
        name="moments",
    )(clip_norm.reshape(1), norm_tile, *grads, m_up, m_down, v_up, v_down)


PIECES = ((0, 0), (0, 1), (1, 0), (1, 1))


def update_kernel(group_size, rate_ref, stats_ref, u_up_hbm, u_down_hbm, p_up_hbm, p_down_hbm, all_up, all_down, p_up_out, p_down_out,
                  slots, u_up, u_down, p_up, p_down, w_up, w_down, stat_send, stat_recv, send_sem, recv_sem, local_sem, in_sem, out_sem):
    me, partner, near_x, near_y = coords()
    loads = []
    for src, dst in ((p_up_hbm, p_up), (p_down_hbm, p_down), (u_up_hbm, u_up), (u_down_hbm, u_down)):
        for layer in HALVES:
            copy = pltpu.make_async_copy(src.at[layer], dst.at[layer], in_sem.at[len(loads)])
            copy.start()
            loads.append(copy)
    meet_all(me, group_size)
    row_id = lax.broadcasted_iota(jnp.int32, (8, 128), 0)
    stats = stats_ref[...]
    for index in range(4):
        loads[index].wait()
        master = (p_up, p_down)[index // 2][index % 2]
        stats = stats + jnp.where(row_id == index, jnp.sum(master * master), 0.0)
    slots[me] = stats
    for copy in exchange_start(me, group_size, slots, stat_send, stat_recv):
        copy.wait()
    total = slots[0]
    for index in range(1, group_size):
        total = total + slots[index]
    ratio = jnp.sqrt(total[0:4]) / jnp.sqrt(total[4:8])
    rate = rate_ref[0]
    params = ((u_up, p_up, p_up_out, w_up, all_up), (u_down, p_down, p_down_out, w_down, all_down))

    def place(piece, owner):
        family, layer = PIECES[piece]
        full = params[family][4]
        rows = params[family][3].shape[1]
        return full.at[layer, pl.ds(pl.multiple_of(owner * rows, rows), rows), :]

    sends = []
    count = [0]

    def forward(src, piece, owner, device, rel):
        copy = remote(src, place(piece, owner), send_sem.at[count[0]], recv_sem.at[rel, piece], device)
        count[0] += 1
        copy.start()
        sends.append(copy)

    def arrival(piece, rel, owner):
        spot = place(piece, owner)
        remote(spot, spot, send_sem.at[0], recv_sem.at[rel, piece], me).wait_recv()
        return spot

    own = {}
    local = []
    for piece in (0, 2, 1, 3):
        family, layer = PIECES[piece]
        u, p, p_out, w, full = params[family]
        index = 2 * family + layer
        loads[4 + index].wait()
        new = p[layer] - rate * ratio[index:index + 1, 0:1] * u[layer]
        w[layer] = new.astype(jnp.bfloat16)
        own[piece] = w.at[layer]
        if family == 0:
            forward(own[piece], piece, me, near_x, 2)
        else:
            forward(own[piece], piece, me, near_y, 4)
        forward(own[piece], piece, me, partner, 1)
        copy = pltpu.make_async_copy(own[piece], place(piece, me), local_sem.at[piece])
        copy.start()
        local.append(copy)
        p[layer] = new
        copy = pltpu.make_async_copy(p.at[layer], p_out.at[layer], out_sem.at[piece])
        copy.start()
        local.append(copy)
    for piece in (2, 3):
        forward(own[piece], piece, me, near_x, 2)
    for piece in (0, 1):
        forward(own[piece], piece, me, near_y, 4)
    diag = near_x + near_y - me
    for k in HALVES:
        spot = arrival(k, 2, near_x)
        forward(spot, k, near_x, near_y, 6)
        forward(spot, k, near_x, partner, 3)
        spot = arrival(2 + k, 4, near_y)
        forward(spot, 2 + k, near_y, near_x, 6)
        forward(spot, 2 + k, near_y, partner, 5)
    for k in HALVES:
        spot = arrival(2 + k, 2, near_x)
        forward(spot, 2 + k, near_x, partner, 3)
        spot = arrival(k, 4, near_y)
        forward(spot, k, near_y, partner, 5)
    for k in HALVES:
        for piece in (2 + k, k):
            spot = arrival(piece, 6, diag)
            forward(spot, piece, diag, partner, 7)
    for rel, owner in ((1, partner), (3, near_x + partner - me), (5, near_y + partner - me), (7, diag + partner - me)):
        for piece in range(4):
            arrival(piece, rel, owner)
    for copy in sends:
        copy.wait_send()
    for copy in local:
        copy.wait()


def update_and_gather(group_size, learn_rate, stats, u_up, u_down, p_up, p_down):
    up, down = p_up.shape, p_down.shape
    vmem = pl.BlockSpec(memory_space=pltpu.VMEM)
    hbm = pl.BlockSpec(memory_space=pl.ANY)
    return pl.pallas_call(
        functools.partial(update_kernel, group_size),
        out_shape=[
            pltpu.VMEM((up[0], up[1] * group_size, up[2]), jnp.bfloat16),
            pltpu.VMEM((down[0], down[1] * group_size, down[2]), jnp.bfloat16),
            jax.ShapeDtypeStruct(up, jnp.float32),
            jax.ShapeDtypeStruct(down, jnp.float32),
        ],
        in_specs=[pl.BlockSpec(memory_space=pltpu.SMEM), vmem] + [hbm] * 4,
        out_specs=[vmem] * 2 + [hbm] * 2,
        scratch_shapes=[
            pltpu.VMEM((group_size, 8, 128), jnp.float32),
            pltpu.VMEM(up, jnp.float32),
            pltpu.VMEM(down, jnp.float32),
            pltpu.VMEM(up, jnp.float32),
            pltpu.VMEM(down, jnp.float32),
            pltpu.VMEM(up, jnp.bfloat16),
            pltpu.VMEM(down, jnp.bfloat16),
            pltpu.SemaphoreType.DMA((group_size,)),
            pltpu.SemaphoreType.DMA((group_size,)),
            pltpu.SemaphoreType.DMA((32,)),
            pltpu.SemaphoreType.DMA((group_size, 4)),
            pltpu.SemaphoreType.DMA((4,)),
            pltpu.SemaphoreType.DMA((8,)),
            pltpu.SemaphoreType.DMA((4,)),
        ],
        compiler_params=pltpu.CompilerParams(collective_id=1, has_side_effects=True, vmem_limit_bytes=FULL_VMEM - 2 * group_size * (up[0] * up[1] * up[2] + down[0] * down[1] * down[2]) - 256 * 1024),
        name="update_and_gather",
    )(learn_rate.reshape(1), stats, u_up, u_down, p_up, p_down)


def solution(mesh):
    group_size = mesh.shape["data"]
    batch_rows = P("data", None)
    state_rows = P(None, "data", None)
    replicated = P()

    def device_step(act_in, grad_out, w_up, w_down, master_up, master_down, exp_avg_up, exp_avg_down, exp_sq_up, exp_sq_down, learn_rate, clip_norm):
        act_one, slope_one, hidden, *turned = forward_block(act_in, w_up, w_down)
        *grads, norm_tile = backward_blocks(group_size, act_in, grad_out, hidden, act_one, slope_one, w_up, *turned)
        avg_up, avg_down, sq_up, sq_down, dir_up, dir_down, stats, norm_value = moments(clip_norm, norm_tile, grads, exp_avg_up, exp_avg_down, exp_sq_up, exp_sq_down)
        new_w_up, new_w_down, master_up_out, master_down_out = update_and_gather(group_size, learn_rate, stats, dir_up, dir_down, master_up, master_down)
        return (new_w_up, new_w_down, master_up_out, master_down_out, avg_up, avg_down, sq_up, sq_down, norm_value.reshape(()))

    return jax.shard_map(device_step, mesh=mesh, in_specs=(batch_rows, batch_rows, replicated, replicated, state_rows, state_rows, state_rows, state_rows, state_rows, state_rows, replicated, replicated), out_specs=(replicated, replicated, state_rows, state_rows, state_rows, state_rows, state_rows, state_rows, replicated), check_vma=False)
```

```python
import functools

import jax
import jax.numpy as jnp
from jax import lax
from jax.experimental import pallas as pl
from jax.experimental.pallas import tpu as pltpu
from jax.sharding import PartitionSpec as P

STEP = 10
BETA_ONE = 0.9
BETA_TWO = 0.95
ADAM_EPS = 1e-8
NORM_EPS = 1e-6
INV_SQRT_TWO = 0.7071067811865476
INV_SQRT_TWO_PI = 0.3989422804014327


def gelu_parts(pre_act):
    normal_cdf = 0.5 * (1.0 + lax.erf(pre_act * INV_SQRT_TWO))
    normal_pdf = jnp.exp(-0.5 * pre_act * pre_act) * INV_SQRT_TWO_PI
    return pre_act * normal_cdf, normal_cdf + pre_act * normal_pdf


MESH = pl.DeviceIdType.MESH


def coords():
    me = lax.axis_index("data")
    core, col, row = me % 2, (me // 2) % 2, me // 4
    return me, me + 1 - 2 * core, me + 2 - 4 * col, me + 4 - 8 * row


def remote(src, dst, send_sem, recv_sem, device):
    return pltpu.make_async_remote_copy(src_ref=src, dst_ref=dst, send_sem=send_sem, recv_sem=recv_sem, device_id=(device,), device_id_type=MESH)


def meet_all(me, group_size):
    barrier = pltpu.get_barrier_semaphore()
    for step in range(1, group_size):
        pl.semaphore_signal(barrier, inc=1, device_id=((me + step) % group_size,), device_id_type=MESH)
    pl.semaphore_wait(barrier, group_size - 1)


def exchange_start(me, group_size, slots, send_sem, recv_sem):
    copies = []
    for step in range(1, group_size):
        copies.append(remote(slots.at[me], slots.at[me], send_sem.at[step], recv_sem.at[step], (me + step) % group_size))
        copies[-1].start()
    return copies


CHUNKS = 3
HALVES = range(2)
DOWN, UP = HALVES
FIRST, SECOND, THIRD = range(CHUNKS)
ZERO = 0.0
LANES = 128
TILE = 256
SLOTS = 4
OWNERS = tuple(chip * 2 + core for core in HALVES for chip in range(4))
FULL_VMEM = 67043328


def dot_nn(lhs, rhs):
    return jnp.dot(lhs, rhs, preferred_element_type=jnp.float32)


def dot_tn(lhs, rhs):
    return lax.dot_general(lhs, rhs, (((0,), (0,)), ((), ())), preferred_element_type=jnp.float32)


def chunk_blocks(chunk, width):
    return [owner * width + chunk * LANES for owner in OWNERS]


def forward_kernel(x_ref, w_up_ref, w_down_ref, up_block, down_block_one, down_block_two, a_out, s_out, h_out, down_t_one, down_t_two, up_t):
    for block, out in ((down_block_one, down_t_one), (down_block_two, down_t_two)):
        for chunk in range(CHUNKS):
            out[chunk] = block[0, chunk * LANES:(chunk + 1) * LANES, :].T
    for chunk in range(CHUNKS):
        up_t[chunk, 0] = up_block[0, :, chunk * LANES:(chunk + 1) * LANES].T
    x = x_ref[...]
    width = w_up_ref.shape[2] // len(OWNERS)
    total = None
    for chunk in range(CHUNKS):
        starts = chunk_blocks(chunk, width)
        w_in = jnp.concatenate([w_up_ref[0, :, s:s + LANES] for s in starts], axis=1)
        gelu, slope = gelu_parts(dot_nn(x, w_in))
        act = gelu.astype(jnp.bfloat16)
        a_out[chunk] = act
        s_out[chunk] = slope
        w_out = jnp.concatenate([w_down_ref[0, s:s + LANES, :] for s in starts], axis=0)
        part = dot_nn(act, w_out)
        total = part if total is None else total + part
    h_out[...] = total.astype(jnp.bfloat16)


def forward_block(act_in, w_up, w_down, tile=512):
    rows, dim = act_in.shape
    ff = w_up.shape[2]
    wide = ff // CHUNKS
    owners = len(OWNERS)
    width = ff // owners
    assert rows // tile == owners

    def slot(i):
        return (i % 2) * (owners // 2) + i // 2

    return pl.pallas_call(
        forward_kernel,
        grid=(rows // tile,),
        out_shape=[
            jax.ShapeDtypeStruct((CHUNKS, rows, wide), jnp.bfloat16),
            jax.ShapeDtypeStruct((CHUNKS, rows, wide), jnp.float32),
            jax.ShapeDtypeStruct((rows, dim), jnp.bfloat16),
            jax.ShapeDtypeStruct((CHUNKS, dim, wide), jnp.bfloat16),
            jax.ShapeDtypeStruct((CHUNKS, dim, wide), jnp.bfloat16),
            jax.ShapeDtypeStruct((CHUNKS, owners, LANES, dim), jnp.bfloat16),
        ],
        in_specs=[
            pl.BlockSpec((tile, dim), lambda i: (i, 0)),
            pl.BlockSpec((1, dim, ff), lambda i: (0, 0, 0)),
            pl.BlockSpec((1, ff, dim), lambda i: (0, 0, 0)),
            pl.BlockSpec((1, dim, width), lambda i: (1, 0, i)),
            pl.BlockSpec((1, width, dim), lambda i: (0, i, 0)),
            pl.BlockSpec((1, width, dim), lambda i: (1, i, 0)),
        ],
        out_specs=[
            pl.BlockSpec((CHUNKS, tile, wide), lambda i: (0, i, 0)),
            pl.BlockSpec((CHUNKS, tile, wide), lambda i: (0, i, 0)),
            pl.BlockSpec((tile, dim), lambda i: (i, 0)),
            pl.BlockSpec((CHUNKS, dim, LANES), lambda i: (0, 0, slot(i))),
            pl.BlockSpec((CHUNKS, dim, LANES), lambda i: (0, 0, slot(i))),
            pl.BlockSpec((CHUNKS, 1, LANES, dim), lambda i: (0, slot(i), 0, 0)),
        ],
        compiler_params=pltpu.CompilerParams(dimension_semantics=("arbitrary",), vmem_limit_bytes=FULL_VMEM),
        name="forward_block",
    )(act_in, w_up, w_down, w_up, w_down, w_down)


def backward_kernel(group_size, x_hbm, e_hbm, h_hbm, a_hbm, s_hbm, w_up_hbm, down_t_one, down_t_two, up_t,
                    g1_hbm, g2_hbm, g3_hbm, g4_hbm, norm_out, q_hbm,
                    g1_out, g2_out, g3_out, g4_out, h_v, e_v, wu_v, wd_v, a_v, q_v, s_v, t_d, t_u,
                    d0, d1a, d1b, d2a, d2b, u0, u1a, u1b, u2a, u2b,
                    sq_v, slots_v, load_sem, w_sem, q_sem, s_sem, send_sem, recv_sem, free_sem, stat_send, stat_recv, out_sem):
    me, partner, near_x, near_y = coords()
    core, col, row = me % 2, (me // 2) % 2, me // 4
    rows, dim = h_v.shape
    half_rows = rows // 2
    wide = wu_v.shape[2]
    width = wide * CHUNKS // len(OWNERS)
    tiles = half_rows // TILE
    slots = s_v.shape[0]

    def at_rows(start, size):
        return pl.ds(pl.multiple_of(start, size), size)

    def half_copy(src, dst, half, sem):
        span = pl.ds(half * half_rows, half_rows)
        return pltpu.make_async_copy(src.at[span], dst.at[span], load_sem.at[sem, half])

    def start_up(chunk):
        for j, start in enumerate(chunk_blocks(chunk, width)):
            pltpu.make_async_copy(w_up_hbm.at[1, :, pl.ds(start, LANES)], wu_v.at[chunk, :, pl.ds(j * LANES, LANES)], w_sem.at[0, chunk]).start()

    def start_down(src, chunk):
        pltpu.make_async_copy(src.at[chunk], wd_v.at[chunk], w_sem.at[1, chunk]).start()

    def up_t_copy(part):
        span = (pl.ds(0, half_rows), pl.ds(half_rows, CHUNKS * wide - half_rows))[part]
        return pltpu.make_async_copy(up_t.at[span], e_v.at[span], load_sem.at[1, part])

    def wait_weight(which, chunk):
        ref = (wu_v, wd_v)[which]
        pltpu.make_async_copy(ref.at[chunk], ref.at[chunk], w_sem.at[which, chunk]).wait()

    half_copy(h_hbm, h_v, 0, 0).start()
    start_up(0)
    half_copy(e_hbm, e_v, 0, 1).start()
    start_down(down_t_two, 0)
    sq_v[...] = jnp.zeros_like(sq_v)
    meet_all(me, group_size)

    def hop(src, dst, kind, chunk, stage, device):
        return remote(src, dst, send_sem.at[kind, chunk, stage], recv_sem.at[kind, chunk, stage], device)

    def hop0(kind, i):
        if kind == DOWN:
            return hop(t_d.at[:, 1 - core], d0.at[i], 0, i, 0, partner)
        return hop(t_u.at[:, :, :, 1 - core], u0.at[i], 1, i, 0, partner)

    def bufs(kind):
        return (d0, d1a, d1b, d2a, d2b) if kind == DOWN else (u0, u1a, u1b, u2a, u2b)

    def hop1(kind, i):
        b0, b1a, b1b, _, _ = bufs(kind)
        return (hop(b0.at[i, 0, :, 1 - col], b1a.at[i], kind, i, 1, near_x),
                hop(b0.at[i, 1, 1 - row], b1b.at[i], kind, i, 2, near_y))

    def hop2(kind, i):
        _, b1a, b1b, b2a, b2b = bufs(kind)
        return (hop(b1a.at[i, 1 - row], b2a.at[i], kind, i, 3, near_y),
                hop(b1b.at[i, 1 - col], b2b.at[i], kind, i, 4, near_x))

    def rs0(kind, i):
        hop0(kind, i).start()

    def rs1(kind, i):
        hop0(kind, i).wait()
        b0 = bufs(kind)[0]
        for side in HALVES:
            for y in HALVES:
                for x in HALVES:
                    own = t_d[side, core, y, x] if kind == DOWN else t_u[side, y, x, core]
                    b0[i, side, y, x] = b0[i, side, y, x] + own
        for copy in hop1(kind, i):
            copy.start()

    def rs2(kind, i):
        b0, b1a, b1b, _, _ = bufs(kind)
        first, second = hop1(kind, i)
        out_a, out_b = hop2(kind, i)
        first.wait()
        for y in HALVES:
            b1a[i, y] = b1a[i, y] + b0[i, 0, y, col]
        out_a.start()
        second.wait()
        for x in HALVES:
            b1b[i, x] = b1b[i, x] + b0[i, 1, row, x]
        out_b.start()

    def rs3(kind, i, out):
        _, b1a, b1b, b2a, b2b = bufs(kind)
        cut = b1a.shape[3]
        for copy in hop2(kind, i):
            copy.wait()
        left = (b1a[i, row] + b2a[i]) / group_size
        right = (b1b[i, col] + b2b[i]) / group_size
        square = (left * left + right * right).reshape(left.shape[0] // 8, 8, cut).sum(axis=0)
        for lane in range(0, cut, LANES):
            sq_v[...] += square[:, lane:lane + LANES]
        if kind == DOWN:
            span = at_rows(i * LANES, LANES)
            out[span, 0:cut] = left
            out[span, cut:2 * cut] = right
        else:
            for j, owner in enumerate(OWNERS):
                part = (left, right)[j // 4]
                lane = (j % 4) * LANES
                out[:, pl.ds(pl.multiple_of(owner * width + i * LANES, LANES), LANES)] = part[:, lane:lane + LANES]

    results = tuple(pltpu.make_async_copy(src, dst, out_sem.at[k]) for k, (src, dst) in enumerate(((g1_out, g1_hbm), (g2_out, g2_hbm), (g3_out, g3_hbm), (g4_out, g4_hbm))))
    g1_copy, g2_copy, g3_copy, g4_copy = results

    def give_free(i):
        for device in (partner, near_x, near_y):
            pl.semaphore_signal(free_sem.at[i], inc=1, device_id=(device,), device_id_type=MESH)

    def grad_down(lhs_ref, rhs_ref, half):
        def part(m, carry):
            acc = dot_tn(lhs_ref[:, at_rows(m * (wide // 2), wide // 2)], rhs_ref[at_rows(half * half_rows, half_rows), :])
            cut = dim // 2
            for side in HALVES:
                piece = acc[:, side * cut:(side + 1) * cut].reshape(t_d.shape[2:])
                t_d[side, m] = piece + jnp.where(half == FIRST, ZERO, t_d[side, m])
            return carry
        lax.fori_loop(0, 2, part, 0)

    def grad_up(lhs_ref, rhs_ref, half):
        def part(m, carry):
            acc = dot_tn(lhs_ref[at_rows(half * half_rows, half_rows), at_rows(m * (dim // 2), dim // 2)], rhs_ref[...])
            cut = wide // 2
            for side in HALVES:
                piece = acc[:, side * cut:(side + 1) * cut].reshape(t_u.shape[2:])
                t_u[side, m] = piece + jnp.where(half == FIRST, ZERO, t_u[side, m])
            return carry
        lax.fori_loop(0, 2, part, 0)

    def q_copy(i, half):
        return pltpu.make_async_copy(q_v, q_hbm.at[i, at_rows(half * half_rows, half_rows), :], q_sem.at[0])

    def second_chunk(i, carry):
        wait_weight(0, i)
        wait_weight(1, i)

        @pl.when(i == FIRST)
        def _():
            half_copy(h_hbm, h_v, 0, 0).wait()
            half_copy(e_hbm, e_v, 0, 1).wait()
            half_copy(h_hbm, h_v, 1, 0).start()
            half_copy(e_hbm, e_v, 1, 1).start()
            for chunk in range(1, CHUNKS):
                start_up(chunk)
                start_down(down_t_two, chunk)

        def second_half(half, carry):
            @pl.when((i == FIRST) & (half == SECOND))
            def _():
                half_copy(h_hbm, h_v, 1, 0).wait()
                half_copy(e_hbm, e_v, 1, 1).wait()

            @pl.when((i > FIRST) | (half > 0))
            def _():
                q_copy(i, half).wait()

            def second_tile(t, carry):
                span = at_rows(half * half_rows + t * TILE, TILE)
                z = dot_nn(h_v[span, :], wu_v[i])
                p = dot_nn(e_v[span, :], wd_v[i])
                gelu, slope = gelu_parts(z)
                here = at_rows(t * TILE, TILE)
                a_v[here, :] = gelu.astype(jnp.bfloat16)
                q_v[here, :] = (p * slope).astype(jnp.bfloat16)

                @pl.when((t == 0) & (half == FIRST) & (i > SECOND))
                def _():
                    rs3(UP, i - 2, g3_out)
                    give_free(i - 2)

                @pl.when((t == 1) & (half == FIRST) & (i > FIRST))
                def _():
                    rs1(DOWN, i - 1)

                @pl.when((t == 5) & (half == FIRST) & (i > FIRST))
                def _():
                    rs1(UP, i - 1)

                @pl.when((t == 0) & (half == SECOND) & (i > FIRST))
                def _():
                    rs2(DOWN, i - 1)

                @pl.when((t == 6) & (half == SECOND) & (i > FIRST))
                def _():
                    rs2(UP, i - 1)
                return carry

            lax.fori_loop(0, tiles, second_tile, 0)
            q_copy(i, half).start()

            grad_down(a_v, e_v, half)

            @pl.when(i == THIRD)
            def _():
                @pl.when(half == FIRST)
                def _():
                    up_t_copy(0).start()

                @pl.when(half == SECOND)
                def _():
                    up_t_copy(1).start()

            @pl.when(half == SECOND)
            def _():
                rs0(DOWN, i)

                @pl.when(i > FIRST)
                def _():
                    rs3(DOWN, i - 1, g4_out)

            grad_up(h_v, q_v, half)

            @pl.when(half == SECOND)
            def _():
                rs0(UP, i)
            return carry

        lax.fori_loop(0, 2, second_half, 0)
        return carry

    lax.fori_loop(0, CHUNKS, second_chunk, 0)

    q_copy(THIRD, 1).wait()
    for chunk in range(CHUNKS):
        start_down(down_t_one, chunk)
    r_rows = half_rows // 4
    staging = (a_v, q_v)

    def r_load(slot, t):
        for k in range(CHUNKS):
            pltpu.make_async_copy(q_hbm.at[k, at_rows(t * r_rows, r_rows), :], staging[slot].at[pl.ds(k * r_rows, r_rows), :], load_sem.at[2, slot]).start()

    def a_load(i, half):
        return pltpu.make_async_copy(a_hbm.at[i, pl.ds(half * half_rows, half_rows), :], staging[half], load_sem.at[0, half])

    for slot in HALVES:
        r_load(slot, slot)
    r_steps = rows // r_rows // 2

    def r_pair(t, carry):
        for slot in HALVES:
            whole = staging[slot].at[pl.ds(0, CHUNKS * r_rows), :]
            pltpu.make_async_copy(whole, whole, load_sem.at[2, slot]).wait()
            for part in HALVES:
                m = part * (r_rows // 2)
                acc = dot_nn(staging[slot][m:m + r_rows // 2, :], e_v[0:wide, :])
                for k in range(1, CHUNKS):
                    acc = acc + dot_nn(staging[slot][k * r_rows + m:k * r_rows + m + r_rows // 2, :], e_v[k * wide:(k + 1) * wide, :])
                h_v[at_rows((2 * t + slot) * r_rows + m, r_rows // 2), :] = acc.astype(jnp.bfloat16)

            @pl.when(t < r_steps - 1)
            def _():
                r_load(slot, 2 * t + 2 + slot)

        @pl.when(t == 0)
        def _():
            rs1(DOWN, THIRD)
            rs1(UP, THIRD)

        @pl.when(t == 2)
        def _():
            rs2(DOWN, THIRD)
        return carry

    rs3(UP, SECOND, g3_out)
    give_free(SECOND)
    for part in HALVES:
        up_t_copy(part).wait()
    lax.fori_loop(0, r_steps, r_pair, 0)
    for half in HALVES:
        half_copy(x_hbm, e_v, half, 1).start()
    for half in HALVES:
        a_load(0, half).start()

    def s_load(i, t):
        slot = lax.rem(t, slots)
        return pltpu.make_async_copy(s_hbm.at[i, at_rows(t * TILE, TILE), :], s_v.at[slot], s_sem.at[slot])

    for t in range(slots):
        s_load(0, t).start()

    def first_chunk(i, carry):
        @pl.when(i == SECOND)
        def _():
            rs2(DOWN, FIRST)

        a_load(i, 0).wait()
        grad_down(a_v, h_v, 0)

        @pl.when(i < THIRD)
        def _():
            a_load(i + 1, 0).start()

        @pl.when(i == FIRST)
        def _():
            rs2(UP, THIRD)

        @pl.when(i == THIRD)
        def _():
            rs2(DOWN, SECOND)

        a_load(i, 1).wait()
        grad_down(q_v, h_v, 1)
        pl.semaphore_wait(free_sem.at[i], 3)
        rs0(DOWN, i)
        wait_weight(1, i)

        @pl.when(i == FIRST)
        def _():
            for half in HALVES:
                half_copy(x_hbm, e_v, half, 1).wait()

        def first_half(half, carry):
            def first_tile(t, carry):
                tt = half * tiles + t
                s_load(i, tt).wait()
                p = dot_nn(h_v[at_rows(tt * TILE, TILE), :], wd_v[i])
                q_v[at_rows(t * TILE, TILE), :] = (p * s_v[lax.rem(tt, slots)]).astype(jnp.bfloat16)

                ahead = tt + slots
                @pl.when(ahead < 2 * tiles)
                def _():
                    s_load(i, ahead).start()

                @pl.when((tt == 7) & (i == FIRST))
                def _():
                    rs3(UP, THIRD, g3_out)
                    give_free(THIRD)
                    g3_copy.start()
                    g4_copy.start()

                @pl.when((tt == tiles + 6) & (i > FIRST))
                def _():
                    rs2(UP, i - 1)
                return carry

            @pl.when(half == FIRST)
            def _():
                @pl.when(i > FIRST)
                def _():
                    rs1(UP, i - 1)

                @pl.when(i == FIRST)
                def _():
                    rs3(DOWN, THIRD, g4_out)

                @pl.when(i == SECOND)
                def _():
                    rs3(DOWN, FIRST, g2_out)

                @pl.when(i == THIRD)
                def _():
                    rs3(UP, FIRST, g1_out)

            lax.fori_loop(0, tiles, first_tile, 0)

            @pl.when((half == SECOND) & (i < THIRD))
            def _():
                for t in range(slots):
                    s_load(i + 1, t).start()

            @pl.when(half == FIRST)
            def _():
                rs1(DOWN, i)

                @pl.when(i == THIRD)
                def _():
                    rs3(DOWN, SECOND, g2_out)

            grad_up(e_v, q_v, half)
            return carry

        lax.fori_loop(0, 2, first_half, 0)
        rs0(UP, i)

        @pl.when(i < THIRD)
        def _():
            a_load(i + 1, 1).start()
        return carry

    lax.fori_loop(0, CHUNKS, first_chunk, 0)
    rs2(DOWN, THIRD)
    rs1(UP, THIRD)
    rs3(UP, SECOND, g1_out)
    rs2(UP, THIRD)
    rs3(DOWN, THIRD, g2_out)
    g2_copy.start()
    rs3(UP, THIRD, g1_out)
    g1_copy.start()
    slots_v[me] = sq_v[...]
    for copy in exchange_start(me, group_size, slots_v, stat_send, stat_recv):
        copy.wait()
    total = slots_v[0]
    for index in range(1, group_size):
        total = total + slots_v[index]
    norm_out[...] = jnp.full(norm_out.shape, jnp.sum(total))
    for copy in results:
        copy.wait()


def backward_blocks(group_size, act_in, grad_out, hidden, act_one, slope_one, w_up, down_t_one, down_t_two, up_t):
    rows, dim = act_in.shape
    ff = w_up.shape[2]
    wide = ff // CHUNKS
    up_rows, down_rows = dim // group_size, LANES
    hbm = pl.BlockSpec(memory_space=pl.ANY)
    vmem = pl.BlockSpec(memory_space=pltpu.VMEM)
    f32 = jnp.float32
    bf16 = jnp.bfloat16
    up_grad = jax.ShapeDtypeStruct((up_rows, ff), f32)
    down_grad = jax.ShapeDtypeStruct((ff // group_size, dim), f32)

    def stages(height, cols):
        return [
            pltpu.VMEM((CHUNKS, 2, 2, 2, height, cols // 2), f32),
            pltpu.VMEM((CHUNKS, 2, height, cols // 2), f32),
            pltpu.VMEM((CHUNKS, 2, height, cols // 2), f32),
            pltpu.VMEM((CHUNKS, height, cols // 2), f32),
            pltpu.VMEM((CHUNKS, height, cols // 2), f32),
        ]

    return pl.pallas_call(
        functools.partial(backward_kernel, group_size),
        out_shape=[up_grad, down_grad, up_grad, down_grad, jax.ShapeDtypeStruct((8, 128), f32), jax.ShapeDtypeStruct((CHUNKS, rows, wide), bf16)],
        in_specs=[hbm] * 9,
        out_specs=[hbm] * 4 + [vmem, hbm],
        scratch_shapes=[
            *(pltpu.VMEM(g.shape, f32) for g in (up_grad, down_grad, up_grad, down_grad)),
            pltpu.VMEM((rows, dim), bf16),
            pltpu.VMEM((rows, dim), bf16),
            pltpu.VMEM((CHUNKS, dim, wide), bf16),
            pltpu.VMEM((CHUNKS, dim, wide), bf16),
            pltpu.VMEM((rows // 2, wide), bf16),
            pltpu.VMEM((rows // 2, wide), bf16),
            pltpu.VMEM((SLOTS, TILE, wide), f32),
            pltpu.VMEM((2, 2, 2, 2, down_rows, dim // 2), f32),
            pltpu.VMEM((2, 2, 2, 2, up_rows, wide // 2), f32),
            *stages(down_rows, dim),
            *stages(up_rows, wide),
            pltpu.VMEM((8, 128), f32),
            pltpu.VMEM((group_size, 8, 128), f32),
            pltpu.SemaphoreType.DMA((3, 2)),
            pltpu.SemaphoreType.DMA((2, CHUNKS)),
            pltpu.SemaphoreType.DMA((1,)),
            pltpu.SemaphoreType.DMA((SLOTS,)),
            pltpu.SemaphoreType.DMA((2, CHUNKS, 5)),
            pltpu.SemaphoreType.DMA((2, CHUNKS, 5)),
            pltpu.SemaphoreType.REGULAR((CHUNKS,)),
            pltpu.SemaphoreType.DMA((group_size,)),
            pltpu.SemaphoreType.DMA((group_size,)),
            pltpu.SemaphoreType.DMA((4,)),
        ],
        compiler_params=pltpu.CompilerParams(collective_id=2, has_side_effects=True, vmem_limit_bytes=FULL_VMEM),
        name="backward_blocks",
    )(act_in, grad_out, hidden, act_one, slope_one, w_up, down_t_one, down_t_two, up_t.reshape(ff, dim))[:5]


def moments_kernel(clip_ref, norm_ref, g_one, g_two, g_three, g_four, m_up, m_down, v_up, v_down, m_up_out, m_down_out, v_up_out, v_down_out, u_up, u_down, stats, norm_out):
    inv_one = 1.0 / (1.0 - BETA_ONE ** STEP)
    inv_two = 1.0 / (1.0 - BETA_TWO ** STEP)
    norm_out[0] = jnp.sqrt(norm_ref[0, 0])
    scale = jnp.minimum(1.0, clip_ref[0] / (jnp.sqrt(norm_ref[0:1, 0:1]) + NORM_EPS))
    row_id = lax.broadcasted_iota(jnp.int32, (8, 128), 0)
    sums = jnp.zeros((8, 128), jnp.float32)
    for family, (grads, m, v, m_out, v_out, u) in enumerate([((g_one, g_three), m_up, v_up, m_up_out, v_up_out, u_up), ((g_two, g_four), m_down, v_down, m_down_out, v_down_out, u_down)]):
        for layer in HALVES:
            grad = grads[layer][...]
            avg_new = BETA_ONE * m[layer] + (1.0 - BETA_ONE) * scale * grad
            sq_new = BETA_TWO * v[layer] + (1.0 - BETA_TWO) * (scale * scale) * (grad * grad)
            direction = (avg_new * inv_one) / (jnp.sqrt(sq_new * inv_two) + ADAM_EPS)
            m_out[layer] = avg_new
            v_out[layer] = sq_new
            u[layer] = direction
            sums = sums + jnp.where(row_id == 4 + 2 * family + layer, jnp.sum(direction * direction), 0.0)

    @pl.when(pl.program_id(0) == 0)
    def _():
        stats[...] = jnp.zeros_like(stats)

    stats[...] += sums


def moments(clip_norm, norm_tile, grads, m_up, m_down, v_up, v_down, steps=4):
    up, down = m_up.shape, m_down.shape
    up_spec = pl.BlockSpec((2, up[1] // steps, up[2]), lambda i: (0, i, 0))
    down_spec = pl.BlockSpec((2, down[1] // steps, down[2]), lambda i: (0, i, 0))
    up_grad = pl.BlockSpec((up[1] // steps, up[2]), lambda i: (i, 0))
    down_grad = pl.BlockSpec((down[1] // steps, down[2]), lambda i: (i, 0))
    tile = pl.BlockSpec((8, 128), lambda i: (0, 0))
    pair = [up_spec, down_spec]
    up_shape, down_shape = jax.ShapeDtypeStruct(up, jnp.float32), jax.ShapeDtypeStruct(down, jnp.float32)
    return pl.pallas_call(
        moments_kernel,
        grid=(steps,),
        out_shape=[up_shape, down_shape] * 3 + [jax.ShapeDtypeStruct((8, 128), jnp.float32), jax.ShapeDtypeStruct((1,), jnp.float32)],
        in_specs=[pl.BlockSpec(memory_space=pltpu.SMEM), tile] + [up_grad, down_grad] * 2 + pair * 2,
        out_specs=pair * 3 + [tile, pl.BlockSpec(memory_space=pltpu.SMEM)],
        compiler_params=pltpu.CompilerParams(dimension_semantics=("arbitrary",), vmem_limit_bytes=FULL_VMEM),
        name="moments",
    )(clip_norm.reshape(1), norm_tile, *grads, m_up, m_down, v_up, v_down)


PIECES = ((0, 0), (0, 1), (1, 0), (1, 1))


def update_kernel(group_size, rate_ref, stats_ref, u_up_hbm, u_down_hbm, p_up_hbm, p_down_hbm, all_up, all_down, p_up_out, p_down_out,
                  slots, u_up, u_down, p_up, p_down, w_up, w_down, stat_send, stat_recv, send_sem, recv_sem, local_sem, in_sem, out_sem):
    me, partner, near_x, near_y = coords()
    loads = []
    for src, dst in ((p_up_hbm, p_up), (p_down_hbm, p_down), (u_up_hbm, u_up), (u_down_hbm, u_down)):
        for layer in HALVES:
            copy = pltpu.make_async_copy(src.at[layer], dst.at[layer], in_sem.at[len(loads)])
            copy.start()
            loads.append(copy)
    meet_all(me, group_size)
    row_id = lax.broadcasted_iota(jnp.int32, (8, 128), 0)
    stats = stats_ref[...]
    for index in range(4):
        loads[index].wait()
        master = (p_up, p_down)[index // 2][index % 2]
        stats = stats + jnp.where(row_id == index, jnp.sum(master * master), 0.0)
    slots[me] = stats
    for copy in exchange_start(me, group_size, slots, stat_send, stat_recv):
        copy.wait()
    total = slots[0]
    for index in range(1, group_size):
        total = total + slots[index]
    ratio = jnp.sqrt(total[0:4]) / jnp.sqrt(total[4:8])
    rate = rate_ref[0]
    params = ((u_up, p_up, p_up_out, w_up, all_up), (u_down, p_down, p_down_out, w_down, all_down))

    def place(piece, owner):
        family, layer = PIECES[piece]
        full = params[family][4]
        rows = params[family][3].shape[1]
        return full.at[layer, pl.ds(pl.multiple_of(owner * rows, rows), rows), :]

    sends = []
    count = [0]

    def forward(src, piece, owner, device, rel):
        copy = remote(src, place(piece, owner), send_sem.at[count[0]], recv_sem.at[rel, piece], device)
        count[0] += 1
        copy.start()
        sends.append(copy)

    def arrival(piece, rel, owner):
        spot = place(piece, owner)
        remote(spot, spot, send_sem.at[0], recv_sem.at[rel, piece], me).wait_recv()
        return spot

    own = {}
    local = []
    for piece in (0, 2, 1, 3):
        family, layer = PIECES[piece]
        u, p, p_out, w, full = params[family]
        index = 2 * family + layer
        loads[4 + index].wait()
        new = p[layer] - rate * ratio[index:index + 1, 0:1] * u[layer]
        w[layer] = new.astype(jnp.bfloat16)
        own[piece] = w.at[layer]
        if family == 0:
            forward(own[piece], piece, me, near_x, 2)
        else:
            forward(own[piece], piece, me, near_y, 4)
        forward(own[piece], piece, me, partner, 1)
        copy = pltpu.make_async_copy(own[piece], place(piece, me), local_sem.at[piece])
        copy.start()
        local.append(copy)
        p[layer] = new
        copy = pltpu.make_async_copy(p.at[layer], p_out.at[layer], out_sem.at[piece])
        copy.start()
        local.append(copy)
    for piece in (2, 3):
        forward(own[piece], piece, me, near_x, 2)
    for piece in (0, 1):
        forward(own[piece], piece, me, near_y, 4)
    diag = near_x + near_y - me
    for k in HALVES:
        spot = arrival(k, 2, near_x)
        forward(spot, k, near_x, near_y, 6)
        forward(spot, k, near_x, partner, 3)
        spot = arrival(2 + k, 4, near_y)
        forward(spot, 2 + k, near_y, near_x, 6)
        forward(spot, 2 + k, near_y, partner, 5)
    for k in HALVES:
        spot = arrival(2 + k, 2, near_x)
        forward(spot, 2 + k, near_x, partner, 3)
        spot = arrival(k, 4, near_y)
        forward(spot, k, near_y, partner, 5)
    for k in HALVES:
        for piece in (2 + k, k):
            spot = arrival(piece, 6, diag)
            forward(spot, piece, diag, partner, 7)
    for rel, owner in ((1, partner), (3, near_x + partner - me), (5, near_y + partner - me), (7, diag + partner - me)):
        for piece in range(4):
            arrival(piece, rel, owner)
    for copy in sends:
        copy.wait_send()
    for copy in local:
        copy.wait()


def update_and_gather(group_size, learn_rate, stats, u_up, u_down, p_up, p_down):
    up, down = p_up.shape, p_down.shape
    vmem = pl.BlockSpec(memory_space=pltpu.VMEM)
    hbm = pl.BlockSpec(memory_space=pl.ANY)
    return pl.pallas_call(
        functools.partial(update_kernel, group_size),
        out_shape=[
            pltpu.VMEM((up[0], up[1] * group_size, up[2]), jnp.bfloat16),
            pltpu.VMEM((down[0], down[1] * group_size, down[2]), jnp.bfloat16),
            jax.ShapeDtypeStruct(up, jnp.float32),
            jax.ShapeDtypeStruct(down, jnp.float32),
        ],
        in_specs=[pl.BlockSpec(memory_space=pltpu.SMEM), vmem] + [hbm] * 4,
        out_specs=[vmem] * 2 + [hbm] * 2,
        scratch_shapes=[
            pltpu.VMEM((group_size, 8, 128), jnp.float32),
            pltpu.VMEM(up, jnp.float32),
            pltpu.VMEM(down, jnp.float32),
            pltpu.VMEM(up, jnp.float32),
            pltpu.VMEM(down, jnp.float32),
            pltpu.VMEM(up, jnp.bfloat16),
            pltpu.VMEM(down, jnp.bfloat16),
            pltpu.SemaphoreType.DMA((group_size,)),
            pltpu.SemaphoreType.DMA((group_size,)),
            pltpu.SemaphoreType.DMA((32,)),
            pltpu.SemaphoreType.DMA((group_size, 4)),
            pltpu.SemaphoreType.DMA((4,)),
            pltpu.SemaphoreType.DMA((8,)),
            pltpu.SemaphoreType.DMA((4,)),
        ],
        compiler_params=pltpu.CompilerParams(collective_id=1, has_side_effects=True, vmem_limit_bytes=FULL_VMEM - 2 * group_size * (up[0] * up[1] * up[2] + down[0] * down[1] * down[2]) - 256 * 1024),
        name="update_and_gather",
    )(learn_rate.reshape(1), stats, u_up, u_down, p_up, p_down)


def solution(mesh):
    group_size = mesh.shape["data"]
    batch_rows = P("data", None)
    state_rows = P(None, "data", None)
    replicated = P()

    def device_step(act_in, grad_out, w_up, w_down, master_up, master_down, exp_avg_up, exp_avg_down, exp_sq_up, exp_sq_down, learn_rate, clip_norm):
        act_one, slope_one, hidden, *turned = forward_block(act_in, w_up, w_down)
        *grads, norm_tile = backward_blocks(group_size, act_in, grad_out, hidden, act_one, slope_one, w_up, *turned)
        avg_up, avg_down, sq_up, sq_down, dir_up, dir_down, stats, norm_value = moments(clip_norm, norm_tile, grads, exp_avg_up, exp_avg_down, exp_sq_up, exp_sq_down)
        new_w_up, new_w_down, master_up_out, master_down_out = update_and_gather(group_size, learn_rate, stats, dir_up, dir_down, master_up, master_down)
        return (new_w_up, new_w_down, master_up_out, master_down_out, avg_up, avg_down, sq_up, sq_down, norm_value.reshape(()))

    return jax.shard_map(device_step, mesh=mesh, in_specs=(batch_rows, batch_rows, replicated, replicated, state_rows, state_rows, state_rows, state_rows, state_rows, state_rows, replicated, replicated), out_specs=(replicated, replicated, state_rows, state_rows, state_rows, state_rows, state_rows, state_rows, replicated), check_vma=False)
```
